32 devices in a mesh: blk: 4 (over z), sub: 8 (over y, x, core).
Axes of the slice: x: 2, y: 2, z: 4, core: 2. Of those that a mesh axis runs over, the one named last changes fastest.
Arguments:
- fields: float32 [32, 55, 2197], P(('blk', 'sub')), may hold values from -6 to 6
- flux_matrix: float32 [3, 55, 55], replicated, may hold values from -0.875 to 0.875
- inv_jacobian: float32 [32, 3], P(('blk', 'sub')), may hold values from 1 to 4
- neighbour: int32 [32, 6], P(('blk', 'sub')), may hold values from 0 to 31, as said below
- orientation: int32 [32, 6], P(('blk', 'sub')), may hold values from 0 to 7, as said below
- face_order: int32 [32, 6], P(('blk', 'sub')), may hold values from 9 to 13, as said below
Outputs:
- increment: float32 [32, 55, 2197], P(('blk', 'sub'))
The draws below stay inside these ranges and needn't reach their ends.
Inputs may be any that keep to these rules, and one draw needn't show every extreme that they name: Element g belongs to the device with blk index (g) // 8 and sub index (g) % 8. The neighbour across face 0 (face 1) lies on the device one step lower (higher) along blk, cyclically, with the same sub index; across face 2 (face 3) on the device one step lower (higher) along sub, cyclically, with the same blk index; across faces 4 and 5 on the same device. If h = neighbour[g, f] then neighbour[h, f xor 1] = g, and the faces of one direction pair the elements of two devices one to one. `orientation`: the two sides of a face carry mutually inverse codes under orient. `face_order`: the two sides of a face carry the same order.
All inputs are finite; a program needn't handle non-finite values.
Results may differ from the reference program's by a relative error of at most 0.002.
Values may be sent and summed in bfloat16 or wider, within the bound.
A program may use at most 64 MiB of HBM per device.

```python
import math
import jax
import jax.numpy as jnp
from jax import lax

VARS = 55
PTS = 13
LOW_ORDER = 9
E_DEV = 1
ELEMS = 32
N_BLK = 4
N_SUB = 8


def invert_code(face_code):
    turned = 4 + 2 * (face_code % 2) + face_code // 2 % 2
    return jnp.where(face_code >= 4, turned, face_code)


def mesh_tables(key):
    device_count = N_BLK * N_SUB
    column_len = E_DEV
    base_key = jax.random.fold_in(key, 7)
    key_perm, key_code, key_order = jax.random.split(base_key, 3)
    scores = jax.random.randint(key_perm, (device_count, column_len), 0, 1 << 20) * column_len + jnp.arange(column_len, dtype=jnp.int32)[None, :]
    column = jnp.argsort(scores, axis=1).astype(jnp.int32)
    position = jnp.argsort(column, axis=1).astype(jnp.int32)
    plus_code = jax.random.randint(key_code, (device_count, column_len, 3), 0, 8).astype(jnp.int32)
    plus_order = jax.random.randint(key_order, (device_count, column_len, 3), LOW_ORDER, PTS + 1).astype(jnp.int32)
    shape_two = (device_count, column_len)
    device_id = jnp.broadcast_to(jnp.arange(device_count, dtype=jnp.int32)[:, None], shape_two)
    slot_pos = jnp.broadcast_to(jnp.arange(column_len, dtype=jnp.int32)[None, :], shape_two)
    row_id = device_id // N_SUB
    col_id = device_id % N_SUB
    down_x = (row_id - 1) % N_BLK * N_SUB + col_id
    up_x = (row_id + 1) % N_BLK * N_SUB + col_id
    down_y = row_id * N_SUB + (col_id - 1) % N_SUB
    up_y = row_id * N_SUB + (col_id + 1) % N_SUB
    down_z = (slot_pos - 1) % column_len
    up_z = (slot_pos + 1) % column_len
    nb_device = jnp.stack([down_x, up_x, down_y, up_y, device_id, device_id], axis=-1)
    nb_slot = jnp.stack([slot_pos, slot_pos, slot_pos, slot_pos, down_z, up_z], axis=-1)
    ids = nb_device * column_len + column[nb_device, nb_slot]
    codes = jnp.stack([invert_code(plus_code[down_x, slot_pos, 0]), plus_code[device_id, slot_pos, 0], invert_code(plus_code[down_y, slot_pos, 1]), plus_code[device_id, slot_pos, 1], invert_code(plus_code[device_id, down_z, 2]), plus_code[device_id, slot_pos, 2]], axis=-1)
    orders = jnp.stack([plus_order[down_x, slot_pos, 0], plus_order[device_id, slot_pos, 0], plus_order[down_y, slot_pos, 1], plus_order[device_id, slot_pos, 1], plus_order[device_id, down_z, 2], plus_order[device_id, slot_pos, 2]], axis=-1)
    pick = position[:, :, None]
    ids = jnp.take_along_axis(ids, pick, axis=1).reshape(device_count * column_len, 6)
    codes = jnp.take_along_axis(codes, pick, axis=1).reshape(device_count * column_len, 6)
    orders = jnp.take_along_axis(orders, pick, axis=1).reshape(device_count * column_len, 6)
    return (ids.astype(jnp.int32), codes.astype(jnp.int32), orders.astype(jnp.int32))


def draw_neighbour(key, part):
    return mesh_tables(key)[0]


def draw_orientation(key, part):
    return mesh_tables(key)[1]


def draw_face_order(key, part):
    return mesh_tables(key)[2]


def steps_of(own_key, shape, cuts, low, largest):
    level = 1.0
    for dim, parts in cuts:
        heights = jax.random.uniform(jax.random.fold_in(jax.random.fold_in(own_key, 6), dim), (parts,), jnp.float32, low / len(cuts), largest / len(cuts))
        level = level * jnp.repeat(jnp.exp(heights), shape[dim] // parts).reshape((-1,) + (1,) * (len(shape) - 1 - dim))
    return level


def gaussian(stream_key, extent, deviation, bound, cuts=(), held_as=jnp.bfloat16):
    loudness = steps_of(stream_key, extent, cuts, -0.22, 0.18) if cuts else 1.0
    values = jax.random.normal(stream_key, extent, jnp.float32) * deviation * loudness
    return jnp.minimum(jnp.maximum(values, -bound), bound).astype(held_as)


def setup_inputs(seed: int = 0) -> dict:
    key_of = jax.random.split(jax.random.key(seed), 7)
    return {
        "fields": gaussian(key_of[0], (ELEMS, VARS, PTS ** 3), 1.0, 6.0, ((0, 32),), jnp.float32),
        "flux_matrix": gaussian(key_of[1], (3, VARS, VARS), VARS ** -0.5, 0.875, (), jnp.float32),
        "inv_jacobian": jnp.clip(jnp.exp(math.log(4.0) - 1.3862944 * jax.random.uniform(key_of[2], (ELEMS, 3), jnp.float32) ** steps_of(key_of[2], (ELEMS, 3), ((0, 32),), -0.2, 0.2)), 1.0, 4.0),
        "neighbour": draw_neighbour(jax.random.fold_in(key_of[6], 71), 0),
        "orientation": draw_orientation(jax.random.fold_in(key_of[6], 71), 0),
        "face_order": draw_face_order(jax.random.fold_in(key_of[6], 71), 0),
    }


penalty = 1.0
time_step = 0.01
highest = lax.Precision.HIGHEST

def cheb_matrix(point_count):
    last_node = point_count - 1
    node_index = jnp.arange(point_count, dtype=jnp.int32)
    node_values = -jnp.cos(jnp.pi * node_index.astype(jnp.float32) / last_node)
    weights = jnp.where((node_index == 0) | (node_index == last_node), 2.0, 1.0) * jnp.where(node_index % 2 == 0, 1.0, -1.0)
    weights = weights.astype(jnp.float32)
    identity = jnp.eye(point_count, dtype=jnp.float32)
    node_gap = node_values[:, None] - node_values[None, :] + identity
    off_diag = weights[:, None] / weights[None, :] / node_gap * (1.0 - identity)
    return off_diag - jnp.diag(lax.optimization_barrier(jnp.sum(off_diag, axis=1)))

def dct_matrix(point_count):
    row_index = jnp.arange(point_count, dtype=jnp.float32)[:, None]
    col_index = jnp.arange(point_count, dtype=jnp.float32)[None, :]
    dct_basis = jnp.cos(jnp.pi * row_index * (col_index + 0.5) / point_count) * jnp.sqrt(2.0 / point_count)
    return dct_basis * jnp.where(row_index == 0, jnp.sqrt(0.5), 1.0).astype(jnp.float32)

def orient_face(face_trace, face_code):
    shaped = face_code[:, None, None, None]
    flipped = jnp.where(shaped // 2 % 2 == 1, jnp.flip(face_trace, 2), face_trace)
    flipped = jnp.where(shaped % 2 == 1, jnp.flip(flipped, 3), flipped)
    return jnp.where(shaped >= 4, jnp.swapaxes(flipped, 2, 3), flipped)

def project(face_trace, mode_order, dct_basis):
    modes = jnp.einsum('ka,fvab,lb->fvkl', dct_basis, face_trace, dct_basis, precision=highest)
    mode_index = jnp.arange(dct_basis.shape[0], dtype=jnp.int32)
    keep = (mode_index[None, :] < mode_order[:, None]).astype(jnp.float32)
    mask_grid = keep[:, None, :, None] * keep[:, None, None, :]
    return jnp.einsum('ka,fvkl,lb->fvab', dct_basis, modes * mask_grid, dct_basis, precision=highest)

def face_jump(own_trace, remote_trace, face_code, mode_order, dct_basis):
    turned = orient_face(remote_trace.astype(jnp.float32), face_code)
    return project(turned, mode_order, dct_basis) - project(own_trace.astype(jnp.float32), mode_order, dct_basis)

def face_traces(element_cube):
    last_index = element_cube.shape[-1] - 1
    return jnp.stack([element_cube[:, :, 0], element_cube[:, :, last_index], element_cube[:, :, :, 0], element_cube[:, :, :, last_index], element_cube[:, :, :, :, 0], element_cube[:, :, :, :, last_index]], axis=1)

def volume_rate(element_cube, flux_matrix, inv_jacobian, derivative):
    along_x = jnp.einsum('ai,evijk->evajk', derivative, element_cube, precision=highest)
    along_y = jnp.einsum('aj,evijk->eviak', derivative, element_cube, precision=highest)
    along_z = jnp.einsum('ak,evijk->evija', derivative, element_cube, precision=highest)
    summed = jnp.zeros(element_cube.shape, jnp.float32)
    for axis_id, along in enumerate((along_x, along_y, along_z)):
        mixed = jnp.einsum('wv,evijk->ewijk', flux_matrix[axis_id], along, precision=highest)
        summed = summed + inv_jacobian[:, axis_id][:, None, None, None, None] * mixed
    return -summed

def add_faces(tendency, corrections, inv_jacobian, lift):
    last_index = tendency.shape[-1] - 1
    scaled = [corrections[face_id] * (lift * inv_jacobian[:, face_id // 2])[:, None, None, None] for face_id in range(6)]
    tendency = tendency.at[:, :, 0].add(scaled[0])
    tendency = tendency.at[:, :, last_index].add(scaled[1])
    tendency = tendency.at[:, :, :, 0].add(scaled[2])
    tendency = tendency.at[:, :, :, last_index].add(scaled[3])
    tendency = tendency.at[:, :, :, :, 0].add(scaled[4])
    tendency = tendency.at[:, :, :, :, last_index].add(scaled[5])
    return tendency

def reference(fields, flux_matrix, inv_jacobian, neighbour, orientation, face_order):
    element_cube = fields.reshape(ELEMS, VARS, PTS, PTS, PTS)
    derivative = cheb_matrix(PTS)
    dct_basis = dct_matrix(PTS)
    traces = face_traces(element_cube).astype(jnp.bfloat16)
    other_face = jnp.array([1, 0, 3, 2, 5, 4], dtype=jnp.int32)
    normal_sign = jnp.array([-1.0, 1.0, -1.0, 1.0, -1.0, 1.0], dtype=jnp.float32)
    face_axis = jnp.array([0, 0, 1, 1, 2, 2], dtype=jnp.int32)
    signed = flux_matrix[face_axis] * normal_sign[:, None, None]
    lift = 0.5 * (PTS - 1) ** 2

    def one_block(first_row):
        block_cube = lax.dynamic_slice_in_dim(element_cube, first_row, E_DEV, 0)
        block_jac = lax.dynamic_slice_in_dim(inv_jacobian, first_row, E_DEV, 0)
        block_neigh = lax.dynamic_slice_in_dim(neighbour, first_row, E_DEV, 0).astype(jnp.int32)
        block_code = lax.dynamic_slice_in_dim(orientation, first_row, E_DEV, 0)
        block_order = lax.dynamic_slice_in_dim(face_order, first_row, E_DEV, 0)
        own_traces = lax.dynamic_slice_in_dim(traces, first_row, E_DEV, 0)
        remote = traces[block_neigh, other_face[None, :]]
        jump_all = face_jump(own_traces.reshape(E_DEV * 6, VARS, PTS, PTS), remote.reshape(E_DEV * 6, VARS, PTS, PTS), block_code.reshape(E_DEV * 6), block_order.reshape(E_DEV * 6), dct_basis).reshape(E_DEV, 6, VARS, PTS, PTS)
        moved_all = jnp.einsum('fwv,efvab->efwab', signed, jump_all, precision=highest)
        corr_all = 0.5 * (penalty * jump_all - moved_all)
        tendency = volume_rate(block_cube, flux_matrix, block_jac, derivative)
        tendency = add_faces(tendency, [corr_all[:, face_id] for face_id in range(6)], block_jac, lift)
        return (time_step * tendency).reshape(E_DEV, VARS, PTS ** 3)
    starts = jnp.arange(ELEMS // E_DEV, dtype=jnp.int32) * E_DEV
    return lax.map(one_block, starts).reshape(ELEMS, VARS, PTS ** 3)
```

```python
import functools

import jax
import jax.numpy as jnp
import numpy as np
from jax import lax
from jax.experimental import pallas as pl
from jax.experimental.pallas import tpu as pltpu
from jax.sharding import PartitionSpec as P

MESH = pl.DeviceIdType.MESH
BF = jnp.bfloat16
F32 = jnp.float32
ROWS = 64
LANES = 256
ENTRY = (1, 3)
TIME_STEP = 0.01


def cheb_np(n):
    idx = np.arange(n)
    x = -np.cos(np.pi * idx / (n - 1))
    c = np.where((idx == 0) | (idx == n - 1), 2.0, 1.0) * np.where(idx % 2 == 0, 1.0, -1.0)
    eye = np.eye(n)
    off = c[:, None] / c[None, :] / (x[:, None] - x[None, :] + eye) * (1.0 - eye)
    return off - np.diag(off.sum(axis=1))


def dct_np(n):
    k = np.arange(n)[:, None]
    j = np.arange(n)[None, :]
    basis = np.cos(np.pi * k * (j + 0.5) / n) * np.sqrt(2.0 / n)
    return basis * np.where(k == 0, np.sqrt(0.5), 1.0)


def hi_lo(matrix):
    full = matrix.astype(np.float32)
    hi = full.astype(BF)
    lo = (full - hi.astype(np.float32)).astype(BF)
    return np.stack([hi, lo])


def wide(matrix):
    return np.pad(matrix, ((0, 0), (0, LANES - matrix.shape[1])))


def tables(n):
    plane = n * n
    d = cheb_np(n)
    c = dct_np(n)
    eye = np.eye(n)
    along_y = np.kron(d.T, eye)
    along_z = np.kron(eye, d.T)
    deriv = hi_lo(np.concatenate([wide(along_y), wide(along_z)], axis=1))
    forward = np.kron(c.T, c.T)
    swapped = forward.reshape(plane, n, n).transpose(0, 2, 1).reshape(plane, plane)
    fwd = hi_lo(np.concatenate([wide(forward), wide(swapped)], axis=1))
    back = hi_lo(wide(np.kron(c, c)))
    lane = np.arange(LANES)
    first = np.where(lane < plane, lane // n, 999)
    second = np.where(lane < plane, lane % n, 999)
    ends = lambda v: np.where(v == 0, -1.0, np.where(v == n - 1, 1.0, 0.0))
    sign = lambda v: np.where(v % 2 == 0, 1.0, -1.0)
    lanes = np.stack(
        [first, second, ends(first), ends(second), sign(first), sign(second), first * 0, first * 0]
    ).astype(np.float32)
    return deriv, fwd, back, lanes, d


def body(
    n, diff, sizes,
    code_hbm, order_hbm, jac_hbm, fields_hbm, flux_hbm, deriv_hbm, fwd_hbm, back_hbm, lane_hbm,
    out_ref,
    code_ref, order_ref, jac_ref, fields_ref, flux_ref, deriv_ref, fwd_ref, back_ref, lane_ref,
    xf, xs, xl, zs, zl, zyz, zx, own, remote, fc, load_sem, send_sem, recv_sem, ack,
):
    width = fields_ref.shape[0]
    plane = n * n
    last = n - 1
    blk, sub = lax.axis_index("blk"), lax.axis_index("sub")
    n_blk, n_sub = sizes
    across = [
        (lax.rem(blk + n_blk - 1, n_blk), sub),
        (lax.rem(blk + 1, n_blk), sub),
        (blk, lax.rem(sub + n_sub - 1, n_sub)),
        (blk, lax.rem(sub + 1, n_sub)),
    ]
    barrier = pltpu.get_barrier_semaphore()
    for face in ENTRY:
        pl.semaphore_signal(barrier, inc=1, device_id=across[face ^ 1], device_id_type=MESH)
    pairs = [
        (fields_hbm.at[:, 0, :], fields_ref), (lane_hbm, lane_ref), (deriv_hbm, deriv_ref),
        (fwd_hbm, fwd_ref), (flux_hbm, flux_ref), (back_hbm, back_ref),
        (jac_hbm, jac_ref), (code_hbm, code_ref), (order_hbm, order_ref),
    ]
    loads = [pltpu.make_async_copy(a, b, load_sem.at[i]) for i, (a, b) in enumerate(pairs)]
    for load in loads:
        load.start()
    loads[0].wait()
    loads[1].wait()

    first = lane_ref[0:1, :]
    second = lane_ref[1:2, :]

    for i in range(n):
        slab = fields_ref[:, plane * i : plane * (i + 1)]
        slab = jnp.pad(slab, ((0, ROWS - width), (0, LANES - plane)))
        xf[i] = slab
        xs[i] = slab.astype(BF)
        xl[i] = (slab - slab.astype(BF).astype(F32)).astype(BF)
    stack = xs[...].reshape(n * ROWS, LANES)[:, :plane]
    stack_lo = xl[...].reshape(n * ROWS, LANES)[:, :plane]

    own[0] = xs[0]
    own[1] = xs[last]
    row_id = lax.broadcasted_iota(jnp.int32, (plane, LANES), 0).astype(F32)
    starts = [second, second + n * last, second * n, second * n + last]

    def trace(face):
        pick = jnp.where(row_id == starts[face - 2], 1.0, 0.0).astype(BF)
        spread = jnp.dot(stack, pick, preferred_element_type=F32).reshape(n, ROWS, LANES)
        total = jnp.zeros((ROWS, LANES), F32)
        for i in range(n):
            total = jnp.where(first == float(i), spread[i], total)
        own[face] = total.astype(BF)

    copies = [
        pltpu.make_async_remote_copy(
            src_ref=own.at[face],
            dst_ref=remote.at[face ^ 1],
            send_sem=send_sem.at[face],
            recv_sem=recv_sem.at[face ^ 1],
            device_id=across[face],
            device_id_type=MESH,
        )
        for face in range(4)
    ]
    pl.semaphore_wait(barrier, 2)
    copies[1].start()
    for face in ENTRY:
        pl.semaphore_signal(ack.at[face ^ 1], inc=1, device_id=across[face], device_id_type=MESH)
    trace(2)
    trace(3)
    copies[3].start()

    def answer(face):
        pl.semaphore_wait(ack.at[face], 1)
        copies[face].start()

    @pl.when(lax.rem(sub, 2) == 0)
    def _():
        answer(0)
        answer(2)

    @pl.when(lax.rem(sub, 2) == 1)
    def _():
        answer(2)
        answer(0)

    trace(4)
    trace(5)
    for load in loads[2:]:
        load.wait()

    fc[...] = jnp.zeros_like(fc)
    for axis in range(3):
        scaled = flux_ref[axis] * (-TIME_STEP * jac_ref[0, axis])
        fc[axis, 0:width, 0:width] = scaled
    flux = jnp.concatenate([fc[0], fc[1], fc[2]], axis=1)
    flux_hi = flux.astype(BF)
    flux_lo = (flux - flux_hi.astype(F32)).astype(BF)
    flux_both = jnp.concatenate([flux_hi, flux_lo], axis=0)

    zyz[...] = (
        jnp.dot(stack, deriv_ref[0], preferred_element_type=F32)
        + jnp.dot(stack, deriv_ref[1], preferred_element_type=F32)
        + jnp.dot(stack_lo, deriv_ref[0], preferred_element_type=F32)
    ).reshape(n, ROWS, 2 * LANES)

    for r in range(0, ROWS, 16):
        for c in range(0, LANES, 128):
            parts = [xf[a, r : r + 16, c : c + 128] for a in range(n)]
            for i in range(n):
                total = parts[0] * float(diff[i, 0])
                for a in range(1, n):
                    total = total + parts[a] * float(diff[i, a])
                zx[i, r : r + 16, c : c + 128] = total

    own_flat = own[...].reshape(6 * ROWS, LANES)[:, :plane]
    own_modes = (
        jnp.dot(own_flat, fwd_ref[0, :, :LANES], preferred_element_type=F32)
        + jnp.dot(own_flat, fwd_ref[1, :, :LANES], preferred_element_type=F32)
    ).reshape(6, ROWS, LANES)

    for copy in copies:
        copy.wait()

    far = jnp.concatenate([remote[...], own[5:6], own[4:5]], axis=0)
    far = far.reshape(6 * ROWS, LANES)[:, :plane]
    far_modes = (
        jnp.dot(far, fwd_ref[0], preferred_element_type=F32)
        + jnp.dot(far, fwd_ref[1], preferred_element_type=F32)
    ).reshape(6, ROWS, 2 * LANES)
    ones = jnp.ones((1, LANES), F32)
    sign_first = lane_ref[4:5, :]
    sign_second = lane_ref[5:6, :]
    modes = []
    for face in range(6):
        code = code_ref[0, face]
        order = order_ref[0, face].astype(F32)
        swap = code >= 4
        rev_a = lax.rem(lax.div(code, 2), 2)
        rev_b = lax.rem(code, 2)
        use_first = jnp.where(swap, rev_b, rev_a) == 1
        use_second = jnp.where(swap, rev_a, rev_b) == 1
        sign = jnp.where(use_first, sign_first, ones) * jnp.where(use_second, sign_second, ones)
        keep = jnp.where((first < order) & (second < order), 1.0, 0.0)
        turned = jnp.where(swap, far_modes[face, :, LANES:], far_modes[face, :, :LANES])
        modes.append((turned * sign - own_modes[face]) * keep)
    modes = jnp.concatenate(modes, axis=0)[:, :plane]
    modes_hi = modes.astype(BF)
    modes_lo = (modes - modes_hi.astype(F32)).astype(BF)
    modes = modes_hi
    jump = (
        jnp.dot(modes_lo, back_ref[0], preferred_element_type=F32)
        + jnp.dot(modes, back_ref[0], preferred_element_type=F32)
        + jnp.dot(modes, back_ref[1], preferred_element_type=F32)
    ).reshape(6, ROWS, LANES)
    lift = 0.5 * last * last * 0.5
    jump = jump * lift

    row_int = lax.broadcasted_iota(jnp.int32, (plane, LANES), 0)
    row_second = row_int - n * lax.div(row_int, n)
    col = lax.broadcasted_iota(jnp.int32, (plane, LANES), 1)
    places = [row_second, row_second + n * last, row_second * n, row_second * n + last]
    blocks = [[], [], [], []]
    for f in range(4):
        for i in range(n):
            blocks[f].append(jnp.where(first == float(i), jump[f + 2], 0.0).astype(BF))
    scat = []
    for axis in range(2):
        total = None
        for side in range(2):
            f = 2 * axis + side
            put = jnp.where(col == places[f], 1.0 if side else -1.0, 0.0).astype(BF)
            part = jnp.dot(
                jnp.concatenate(blocks[f], axis=0)[:, :plane], put, preferred_element_type=F32
            )
            total = part if total is None else total + part
        scat.append(total.reshape(n, ROWS, LANES))

    gain_y = lane_ref[2:3, :] * (TIME_STEP * jac_ref[0, 1])
    gain_z = lane_ref[3:4, :] * (TIME_STEP * jac_ref[0, 2])
    gain_x = TIME_STEP * jac_ref[0, 0]
    zx[0] = zx[0] - jump[0]
    zx[last] = zx[last] + jump[1]

    def keep_both(i, axis, value):
        hi = value.astype(BF)
        zs[i, axis] = hi
        zl[i, axis] = (value - hi.astype(F32)).astype(BF)

    for i in range(n):
        keep_both(i, 0, zx[i])
        keep_both(i, 1, zyz[i, :, :LANES] + scat[0][i])
        keep_both(i, 2, zyz[i, :, LANES:] + scat[1][i])
        both = jnp.dot(
            flux_both, zs[i].reshape(3 * ROWS, LANES), preferred_element_type=F32
        )
        moved = both[:ROWS] + both[ROWS:] + jnp.dot(
            flux_hi, zl[i].reshape(3 * ROWS, LANES), preferred_element_type=F32
        )
        moved = moved + scat[0][i] * gain_y + scat[1][i] * gain_z
        if i == 0:
            moved = moved + jump[0] * gain_x
        if i == last:
            moved = moved + jump[1] * gain_x
        out_ref[:, plane * i : plane * (i + 1)] = moved[:width, :plane]


def hand_over(part_ref, out_ref, sem):
    copy = pltpu.make_async_copy(part_ref, out_ref.at[:, 0, :], sem)
    copy.start()
    copy.wait()


def solution(mesh):
    sizes = (mesh.shape["blk"], mesh.shape["sub"])

    def on_device(fields, flux_matrix, inv_jacobian, neighbour, orientation, face_order):
        width, points = fields.shape[1:]
        n = round(points ** (1.0 / 3.0))
        deriv, fwd, back, lanes, diff = tables(n)
        rows = jnp.transpose(fields, (1, 0, 2))
        hbm = pl.BlockSpec(memory_space=pltpu.HBM)
        operands = [
            orientation, face_order, inv_jacobian, rows, flux_matrix,
            jnp.asarray(deriv), jnp.asarray(fwd), jnp.asarray(back), jnp.asarray(lanes),
        ]
        smem = lambda a: pltpu.SMEM(a.shape, a.dtype)
        vmem = lambda a: pltpu.VMEM(a.shape, a.dtype)
        part = pl.pallas_call(
            functools.partial(body, n, diff, sizes),
            out_shape=pltpu.VMEM((width, points), F32),
            in_specs=[hbm] * 9,
            out_specs=pl.BlockSpec(memory_space=pltpu.VMEM),
            scratch_shapes=[smem(a) for a in operands[:3]]
            + [pltpu.VMEM((width, points), F32)]
            + [vmem(a) for a in operands[4:]]
            + [
                pltpu.VMEM((n, ROWS, LANES), F32),
                pltpu.VMEM((n, ROWS, LANES), BF),
                pltpu.VMEM((n, ROWS, LANES), BF),
                pltpu.VMEM((n, 3, ROWS, LANES), BF),
                pltpu.VMEM((n, 3, ROWS, LANES), BF),
                pltpu.VMEM((n, ROWS, 2 * LANES), F32),
                pltpu.VMEM((n, ROWS, LANES), F32),
                pltpu.VMEM((6, ROWS, LANES), BF),
                pltpu.VMEM((4, ROWS, LANES), BF),
                pltpu.VMEM((3, ROWS, ROWS), F32),
                pltpu.SemaphoreType.DMA((9,)),
                pltpu.SemaphoreType.DMA((4,)),
                pltpu.SemaphoreType.DMA((4,)),
                pltpu.SemaphoreType.REGULAR((4,)),
            ],
            compiler_params=pltpu.CompilerParams(
                collective_id=0, has_side_effects=True, vmem_limit_bytes=48 * 1024 * 1024
            ),
        )(*[pltpu.with_memory_space_constraint(a, pltpu.HBM) for a in operands])
        out = pl.pallas_call(
            hand_over,
            out_shape=jax.ShapeDtypeStruct(rows.shape, F32),
            in_specs=[pl.BlockSpec(memory_space=pltpu.VMEM)],
            out_specs=hbm,
            scratch_shapes=[pltpu.SemaphoreType.DMA],
            compiler_params=pltpu.CompilerParams(vmem_limit_bytes=16 * 1024 * 1024),
        )(part)
        return jnp.transpose(out, (1, 0, 2))

    return jax.shard_map(
        on_device,
        mesh=mesh,
        in_specs=(
            P(("blk", "sub"), None, None),
            P(),
            P(("blk", "sub"), None),
            P(("blk", "sub"), None),
            P(("blk", "sub"), None),
            P(("blk", "sub"), None),
        ),
        out_specs=P(("blk", "sub"), None, None),
        check_vma=False,
    )
```

```python
import functools

import jax
import jax.numpy as jnp
import numpy as np
from jax import lax
from jax.experimental import pallas as pl
from jax.experimental.pallas import tpu as pltpu
from jax.sharding import PartitionSpec as P

MESH = pl.DeviceIdType.MESH
BF = jnp.bfloat16
F32 = jnp.float32
ROWS = 64
LANES = 256
TIME_STEP = 0.01
ENTRY = (1, 3)


def cheb_np(n):
    idx = np.arange(n)
    x = -np.cos(np.pi * idx / (n - 1))
    c = np.where((idx == 0) | (idx == n - 1), 2.0, 1.0) * np.where(idx % 2 == 0, 1.0, -1.0)
    eye = np.eye(n)
    off = c[:, None] / c[None, :] / (x[:, None] - x[None, :] + eye) * (1.0 - eye)
    return off - np.diag(off.sum(axis=1))


def dct_np(n):
    k = np.arange(n)[:, None]
    j = np.arange(n)[None, :]
    basis = np.cos(np.pi * k * (j + 0.5) / n) * np.sqrt(2.0 / n)
    return basis * np.where(k == 0, np.sqrt(0.5), 1.0)


def hi_lo(matrix):
    full = matrix.astype(np.float32)
    hi = full.astype(BF)
    lo = (full - hi.astype(np.float32)).astype(BF)
    return np.stack([hi, lo])


def wide(matrix, lanes=LANES):
    return np.pad(matrix, ((0, 0), (0, lanes - matrix.shape[1])))


def tables(n):
    plane = n * n
    d = cheb_np(n)
    c = dct_np(n)
    eye = np.eye(n)
    deriv = np.stack([hi_lo(wide(np.kron(d.T, eye))), hi_lo(wide(np.kron(eye, d.T)))])
    forward = np.kron(c.T, c.T)
    swapped = forward.reshape(plane, n, n).transpose(0, 2, 1).reshape(plane, plane)
    fwd = np.stack([hi_lo(wide(forward)), hi_lo(wide(swapped))])
    back = hi_lo(wide(np.kron(c, c)))
    lane = np.arange(LANES)
    first = np.where(lane < plane, lane // n, 999)
    second = np.where(lane < plane, lane % n, 999)
    sign = lambda v: np.where(v % 2 == 0, 1.0, -1.0)
    lanes = np.stack(
        [first, second, sign(first), sign(second)] + [first * 0] * 4
    ).astype(np.float32)
    pick = np.zeros((plane, 2 * n))
    for j in range(n):
        pick[n * j, j] = 1.0
        pick[n * j + n - 1, n + j] = 1.0
    put = np.concatenate([pick.T, pick.T])
    return deriv, fwd, back, lanes, wide(pick, 128).astype(BF), wide(put).astype(BF), d


def split(value):
    hi = value.astype(BF)
    return hi, (value - hi.astype(F32)).astype(BF)


def dot(a, b):
    return jnp.dot(a, b, preferred_element_type=F32)


def body(
    n, diff, sizes,
    code_hbm, order_hbm, jac_hbm, fields_hbm, flux_hbm,
    deriv_hbm, fwd_hbm, back_hbm, lane_hbm, pick_hbm, put_hbm,
    out_ref,
    code_ref, order_ref, jac_ref, fields_ref, flux_ref,
    deriv_ref, fwd_ref, back_ref, lane_ref, pick_ref, put_ref,
    xs, xl, gx, gs, vol, own, remote, raw, mix, lift_lhs, oper, early,
    load_sem, send_sem, recv_sem, ack,
):
    width, points = fields_ref.shape
    plane = n * n
    last = n - 1
    blk, sub = lax.axis_index("blk"), lax.axis_index("sub")
    n_blk, n_sub = sizes
    across = [
        (lax.rem(blk + n_blk - 1, n_blk), sub),
        (lax.rem(blk + 1, n_blk), sub),
        (blk, lax.rem(sub + n_sub - 1, n_sub)),
        (blk, lax.rem(sub + 1, n_sub)),
    ]
    barrier = pltpu.get_barrier_semaphore()
    for face in ENTRY:
        pl.semaphore_signal(barrier, inc=1, device_id=across[face ^ 1], device_id_type=MESH)
    low = -(-plane // 128) * 128
    high = plane * last // 128 * 128
    piece = lambda a, b: (fields_hbm.at[:, 0, a:b], fields_ref.at[:, a:b])
    pairs = [
        piece(0, low), piece(high, points), piece(low, high),
        (pick_hbm, pick_ref), (fwd_hbm, fwd_ref), (lane_hbm, lane_ref), (back_hbm, back_ref),
        (flux_hbm, flux_ref), (deriv_hbm, deriv_ref), (put_hbm, put_ref),
        (jac_hbm, jac_ref), (code_hbm, code_ref), (order_hbm, order_ref),
    ]
    loads = [pltpu.make_async_copy(a, b, load_sem.at[i]) for i, (a, b) in enumerate(pairs)]
    for load in loads:
        load.start()
    copies = [
        pltpu.make_async_remote_copy(
            src_ref=own.at[face],
            dst_ref=remote.at[face ^ 1],
            send_sem=send_sem.at[face],
            recv_sem=recv_sem.at[face ^ 1],
            device_id=across[face],
            device_id_type=MESH,
        )
        for face in range(4)
    ]

    def padded(value):
        return jnp.pad(value, ((0, ROWS - value.shape[0]), (0, LANES - value.shape[1])))

    def slab(i):
        return padded(fields_ref[:, plane * i : plane * (i + 1)])

    loads[0].wait()
    loads[1].wait()
    own[0] = slab(0).astype(BF)
    own[1] = slab(last).astype(BF)
    pl.semaphore_wait(barrier, 2)
    copies[1].start()
    for face in ENTRY:
        pl.semaphore_signal(ack.at[face ^ 1], inc=1, device_id=across[face], device_id_type=MESH)
    loads[2].wait()
    for face in (2, 3):
        at = (face - 2) * (plane - n)
        runs = [fields_ref[:, plane * i + at : plane * i + at + n] for i in range(n)]
        own[face] = padded(jnp.concatenate(runs, axis=1)).astype(BF)
    copies[3].start()

    for i in range(n):
        xs[i], xl[i] = split(slab(i))
    stack = xs[...].reshape(n * ROWS, LANES)[:, :plane]
    loads[3].wait()
    ends = dot(stack, pick_ref[...]).reshape(n, ROWS, 128)
    for face in (4, 5):
        at = (face - 4) * n
        runs = [ends[i, :, at : at + n] for i in range(n)]
        own[face] = padded(jnp.concatenate(runs, axis=1)).astype(BF)

    def answer(face):
        pl.semaphore_wait(ack.at[face], 1)
        copies[face].start()

    y_first = jnp.logical_or(lax.rem(sub, 2) == 1, blk == 0)

    @pl.when(y_first)
    def _():
        answer(2)

    @pl.when(jnp.logical_not(y_first))
    def _():
        answer(0)

    for load in loads[4:]:
        load.wait()

    raw[...] = jnp.zeros_like(raw)
    for axis in range(3):
        scaled = flux_ref[axis] * (-TIME_STEP * jac_ref[0, axis])
        for k in range(3):
            raw[axis, 0:width, ROWS * k : ROWS * k + width] = scaled

    def thirds(value):
        lane = lax.broadcasted_iota(jnp.int32, value.shape, value.ndim - 1)
        hi = value.astype(BF).astype(F32)
        return jnp.where(lane < 2 * ROWS, hi, value - hi).astype(BF)

    mix[...] = thirds(raw[...])
    row = lax.broadcasted_iota(jnp.int32, (ROWS, LANES), 0)
    lane = lax.broadcasted_iota(jnp.int32, (ROWS, LANES), 1)
    diagonal = jnp.logical_and(jnp.bitwise_and(lane, ROWS - 1) == row, lane < 3 * ROWS)
    lift = 0.5 * last * last * 0.5
    for face in range(6):
        side = lift if face % 2 else -lift
        keep = lift * TIME_STEP * jac_ref[0, face // 2]
        lift_lhs[face] = thirds(raw[face // 2] * side + jnp.where(diagonal, keep, 0.0))

    def fluxed(lhs, hi, lo):
        return dot(lhs[:, : 3 * ROWS], jnp.concatenate([hi, lo, hi], axis=0))

    for i in range(n):
        mixed = fluxed(mix[...].reshape(3 * ROWS, LANES), xs[i], xl[i])
        gx[i] = mixed[:ROWS]
        for axis in range(2):
            part = mixed[ROWS * (axis + 1) : ROWS * (axis + 2)]
            gs[axis, 0, i], gs[axis, 1, i] = split(part)

    first = lane_ref[0:1, :]
    second = lane_ref[1:2, :]
    ones = jnp.ones((1, LANES), F32)

    def face_facts(face):
        code = code_ref[0, face]
        order = order_ref[0, face].astype(F32)
        swap = jnp.where(code >= 4, 1, 0)
        rev_a = lax.rem(lax.div(code, 2), 2)
        rev_b = lax.rem(code, 2)
        use_first = jnp.where(swap == 1, rev_b, rev_a) == 1
        use_second = jnp.where(swap == 1, rev_a, rev_b) == 1
        sign = jnp.where(use_first, lane_ref[2:3, :], ones) * jnp.where(
            use_second, lane_ref[3:4, :], ones
        )
        keep = jnp.where((first < order) & (second < order), 1.0, 0.0)
        return swap, sign, keep

    facts = [face_facts(face) for face in range(6)]
    own_flat = own[...].reshape(6 * ROWS, LANES)[:, :plane]
    own_modes = (dot(own_flat, fwd_ref[0, 0]) + dot(own_flat, fwd_ref[0, 1])).reshape(
        6, ROWS, LANES
    )
    modes = []
    for face in range(6):
        swap, sign, keep = facts[face]
        if face < 4:
            modes.append(own_modes[face] * -keep)
        else:
            far = own[face ^ 1][:, :plane]
            turned = dot(far, fwd_ref[swap, 0]) + dot(far, fwd_ref[swap, 1])
            modes.append((turned * sign - own_modes[face]) * keep)
    modes_hi, modes_lo = split(jnp.concatenate(modes, axis=0))
    modes_hi, modes_lo = modes_hi[:, :plane], modes_lo[:, :plane]
    jump = dot(modes_hi, back_ref[0]) + dot(modes_lo, back_ref[0]) + dot(modes_hi, back_ref[1])
    jump_hi, jump_lo = split(jump)
    cut = lambda a, f: a[ROWS * f : ROWS * (f + 1)]
    lifted = [
        fluxed(lift_lhs[face], cut(jump_hi, face), cut(jump_lo, face)) for face in range(6)
    ]
    for face in range(4):
        early[face] = lifted[face]

    @pl.when(y_first)
    def _():
        answer(0)

    @pl.when(jnp.logical_not(y_first))
    def _():
        answer(2)

    for face in range(4):
        swap, sign, keep = facts[face]
        scale = sign * keep
        f_hi = (fwd_ref[swap, 0].astype(F32) * scale).astype(BF)[:, :plane]
        f_lo = (fwd_ref[swap, 1].astype(F32) * scale).astype(BF)[:, :plane]
        whole = dot(f_hi, back_ref[0]) + dot(f_lo, back_ref[0]) + dot(f_hi, back_ref[1])
        oper[face, 0], oper[face, 1] = split(whole)

    runs = []
    for i in range(n):
        both = jnp.concatenate(
            [lifted[4][:, n * i : n * (i + 1)], lifted[5][:, n * i : n * (i + 1)]], axis=1
        )
        hi = both.astype(BF).astype(F32)
        runs.append(jnp.concatenate([hi, both - hi], axis=1).astype(BF))
    total = dot(jnp.concatenate(runs, axis=0), put_ref[...])
    for axis in range(2):
        hi = gs[axis, 0].reshape(n * ROWS, LANES)[:, :plane]
        lo = gs[axis, 1].reshape(n * ROWS, LANES)[:, :plane]
        total = total + dot(hi, deriv_ref[axis, 0])
        total = total + dot(lo, deriv_ref[axis, 0])
        total = total + dot(hi, deriv_ref[axis, 1])
    vol[...] = total.reshape(n, ROWS, LANES)

    half = n // 2
    for r in range(0, -(-width // 8) * 8, 8):
        for c in range(0, LANES, 128):
            at = (slice(r, r + 8), slice(c, c + 128))
            plus, minus = [], []
            for a in range(half):
                one, two = gx[(a,) + at], gx[(last - a,) + at]
                plus.append(one + two)
                minus.append(one - two)
            middle = gx[(half,) + at]
            for i in range(half):
                even = minus[0] * float(0.5 * (diff[i, 0] - diff[i, last]))
                odd = middle * float(diff[i, half])
                for a in range(half):
                    odd = odd + plus[a] * float(0.5 * (diff[i, a] + diff[i, last - a]))
                    if a:
                        even = even + minus[a] * float(0.5 * (diff[i, a] - diff[i, last - a]))
                vol[(i,) + at] += even + odd
                vol[(last - i,) + at] += even - odd
            even = minus[0] * float(diff[half, 0])
            for a in range(1, half):
                even = even + minus[a] * float(diff[half, a])
            vol[(half,) + at] += even
    for i in range(n):
        value = vol[i]
        if i == 0:
            value = value + early[0]
        if i == last:
            value = value + early[1]
        out_ref[:, plane * i : plane * (i + 1)] = value[:width, :plane]

    def arrived(face):
        copies[face ^ 1].wait_recv()
        far = remote[face][:, :plane]
        turned = dot(far, oper[face, 0]) + dot(far, oper[face, 1])
        return fluxed(lift_lhs[face], *split(turned))

    for face in (2, 3):
        total = (arrived(face) + early[face])[:width]
        at = (face - 2) * (plane - n)
        for i in range(n):
            out_ref[:, plane * i + at : plane * i + at + n] += total[:, n * i : n * (i + 1)]
    for face in (0, 1):
        at = face * plane * last
        out_ref[:, at : at + plane] += arrived(face)[:width, :plane]
    for copy in copies:
        copy.wait_send()


def hand_over(part_ref, out_ref, sem):
    copy = pltpu.make_async_copy(part_ref, out_ref.at[:, 0, :], sem)
    copy.start()
    copy.wait()


def solution(mesh):
    sizes = (mesh.shape["blk"], mesh.shape["sub"])

    def on_device(fields, flux_matrix, inv_jacobian, neighbour, orientation, face_order):
        width, points = fields.shape[1:]
        n = round(points ** (1.0 / 3.0))
        plane = n * n
        *constants, diff = tables(n)
        rows = jnp.transpose(fields, (1, 0, 2))
        hbm = pl.BlockSpec(memory_space=pltpu.HBM)
        operands = [orientation, face_order, inv_jacobian, rows, flux_matrix]
        operands += [jnp.asarray(a) for a in constants]
        vmem = lambda a: pltpu.VMEM(a.shape, a.dtype)
        part = pl.pallas_call(
            functools.partial(body, n, diff, sizes),
            out_shape=pltpu.VMEM((width, points), F32),
            in_specs=[hbm] * len(operands),
            out_specs=pl.BlockSpec(memory_space=pltpu.VMEM),
            scratch_shapes=[pltpu.SMEM(a.shape, a.dtype) for a in operands[:3]]
            + [pltpu.VMEM((width, points), F32)]
            + [vmem(a) for a in operands[4:]]
            + [
                pltpu.VMEM((n, ROWS, LANES), BF),
                pltpu.VMEM((n, ROWS, LANES), BF),
                pltpu.VMEM((n, ROWS, LANES), F32),
                pltpu.VMEM((2, 2, n, ROWS, LANES), BF),
                pltpu.VMEM((n, ROWS, LANES), F32),
                pltpu.VMEM((6, ROWS, LANES), BF),
                pltpu.VMEM((4, ROWS, LANES), BF),
                pltpu.VMEM((3, ROWS, LANES), F32),
                pltpu.VMEM((3, ROWS, LANES), BF),
                pltpu.VMEM((6, ROWS, LANES), BF),
                pltpu.VMEM((4, 2, plane, LANES), BF),
                pltpu.VMEM((4, ROWS, LANES), F32),
                pltpu.SemaphoreType.DMA((13,)),
                pltpu.SemaphoreType.DMA((4,)),
                pltpu.SemaphoreType.DMA((4,)),
                pltpu.SemaphoreType.REGULAR((4,)),
            ],
            compiler_params=pltpu.CompilerParams(
                collective_id=0, has_side_effects=True, vmem_limit_bytes=48 * 1024 * 1024
            ),
        )(*[pltpu.with_memory_space_constraint(a, pltpu.HBM) for a in operands])
        out = pl.pallas_call(
            hand_over,
            out_shape=jax.ShapeDtypeStruct(rows.shape, F32),
            in_specs=[pl.BlockSpec(memory_space=pltpu.VMEM)],
            out_specs=hbm,
            scratch_shapes=[pltpu.SemaphoreType.DMA],
            compiler_params=pltpu.CompilerParams(vmem_limit_bytes=16 * 1024 * 1024),
        )(part)
        return jnp.transpose(out, (1, 0, 2))

    return jax.shard_map(
        on_device,
        mesh=mesh,
        in_specs=(
            P(("blk", "sub"), None, None),
            P(),
            P(("blk", "sub"), None),
            P(("blk", "sub"), None),
            P(("blk", "sub"), None),
            P(("blk", "sub"), None),
        ),
        out_specs=P(("blk", "sub"), None, None),
        check_vma=False,
    )
```

```python
import functools

import jax
import jax.numpy as jnp
import numpy as np
from jax import lax
from jax.experimental import pallas as pl
from jax.experimental.pallas import tpu as pltpu
from jax.sharding import PartitionSpec as P

MESH = pl.DeviceIdType.MESH
BF = jnp.bfloat16
F32 = jnp.float32
ROWS = 64
LANES = 256
TIME_STEP = 0.01
ENTRY = (1, 3)
FIRST = 13


def cheb_np(n):
    idx = np.arange(n)
    x = -np.cos(np.pi * idx / (n - 1))
    c = np.where((idx == 0) | (idx == n - 1), 2.0, 1.0) * np.where(idx % 2 == 0, 1.0, -1.0)
    eye = np.eye(n)
    off = c[:, None] / c[None, :] / (x[:, None] - x[None, :] + eye) * (1.0 - eye)
    return off - np.diag(off.sum(axis=1))


def dct_np(n):
    k = np.arange(n)[:, None]
    j = np.arange(n)[None, :]
    basis = np.cos(np.pi * k * (j + 0.5) / n) * np.sqrt(2.0 / n)
    return basis * np.where(k == 0, np.sqrt(0.5), 1.0)


def hi_lo(matrix):
    full = matrix.astype(np.float32)
    hi = full.astype(BF)
    lo = (full - hi.astype(np.float32)).astype(BF)
    return np.stack([hi, lo])


def wide(matrix, lanes=LANES):
    return np.pad(matrix, ((0, 0), (0, lanes - matrix.shape[1])))


def tables(n):
    plane = n * n
    d = cheb_np(n)
    c = dct_np(n)
    eye = np.eye(n)
    deriv = np.stack([hi_lo(wide(np.kron(d.T, eye))), hi_lo(wide(np.kron(eye, d.T)))])
    forward = np.kron(c.T, c.T)
    swapped = forward.reshape(plane, n, n).transpose(0, 2, 1).reshape(plane, plane)
    fwd = np.stack([hi_lo(wide(forward)), hi_lo(wide(swapped))])
    back = hi_lo(wide(np.kron(c, c)))
    lane = np.arange(LANES)
    first = np.where(lane < plane, lane // n, 999)
    second = np.where(lane < plane, lane % n, 999)
    sign = lambda v: np.where(v % 2 == 0, 1.0, -1.0)
    lanes = np.stack(
        [first, second, sign(first), sign(second)] + [first * 0] * 4
    ).astype(np.float32)
    pick = np.zeros((plane, 2 * n))
    for j in range(n):
        pick[n * j, j] = 1.0
        pick[n * j + n - 1, n + j] = 1.0
    put = np.concatenate([pick.T, pick.T])
    return deriv, fwd, back, lanes, wide(pick, 128).astype(BF), wide(put).astype(BF), d


def split(value):
    hi = value.astype(BF)
    return hi, (value - hi.astype(F32)).astype(BF)


def dot(a, b):
    return jnp.dot(a, b, preferred_element_type=F32)


def fluxed(lhs, hi, lo):
    return dot(lhs[:, : 3 * ROWS], jnp.concatenate([hi, lo, hi], axis=0))


def far_terms(pair, far, oper, lift_lhs):
    plane = oper.shape[2]
    turned = [
        dot(far[f][:, :plane], oper[f, 0]) + dot(far[f][:, :plane], oper[f, 1]) for f in pair
    ]
    return [fluxed(lift_lhs[f], *split(t)) for f, t in zip(pair, turned)]


def body(
    n, diff, sizes,
    code_hbm, order_hbm, jac_hbm, fields_hbm, flux_hbm,
    deriv_hbm, fwd_hbm, back_hbm, lane_hbm, pick_hbm, put_hbm,
    out_ref, far_ref, oper, lift_lhs,
    code_ref, order_ref, jac_ref, fields_ref, flux_ref,
    deriv_ref, fwd_ref, back_ref, lane_ref, pick_ref, put_ref,
    xs, xl, gx, gs, vol, own, remote, raw, mix, early,
    load_sem, send_sem, recv_sem, ack,
):
    width, points = fields_ref.shape
    plane = n * n
    last = n - 1
    blk, sub = lax.axis_index("blk"), lax.axis_index("sub")
    n_blk, n_sub = sizes
    across = [
        (lax.rem(blk + n_blk - 1, n_blk), sub),
        (lax.rem(blk + 1, n_blk), sub),
        (blk, lax.rem(sub + n_sub - 1, n_sub)),
        (blk, lax.rem(sub + 1, n_sub)),
    ]
    barrier = pltpu.get_barrier_semaphore()
    for face in ENTRY:
        pl.semaphore_signal(barrier, inc=1, device_id=across[face ^ 1], device_id_type=MESH)
    low = -(-plane // 128) * 128
    high = plane * last // 128 * 128
    piece = lambda a, b: (fields_hbm.at[:, 0, a:b], fields_ref.at[:, a:b])
    pairs = [
        piece(0, low), piece(high, points), piece(low, high),
        (pick_hbm, pick_ref), (fwd_hbm, fwd_ref), (lane_hbm, lane_ref), (back_hbm, back_ref),
        (flux_hbm, flux_ref), (deriv_hbm, deriv_ref), (put_hbm, put_ref),
        (jac_hbm, jac_ref), (code_hbm, code_ref), (order_hbm, order_ref),
    ]
    loads = [pltpu.make_async_copy(a, b, load_sem.at[i]) for i, (a, b) in enumerate(pairs)]
    for load in loads[:FIRST]:
        load.start()
    copies = [
        pltpu.make_async_remote_copy(
            src_ref=own.at[face],
            dst_ref=remote.at[face ^ 1],
            send_sem=send_sem.at[face],
            recv_sem=recv_sem.at[face ^ 1],
            device_id=across[face],
            device_id_type=MESH,
        )
        for face in range(4)
    ]

    def padded(value):
        return jnp.pad(value, ((0, ROWS - value.shape[0]), (0, LANES - value.shape[1])))

    def slab(i):
        return padded(fields_ref[:, plane * i : plane * (i + 1)])

    lift = 0.5 * last * last * 0.5

    def traces():
        loads[2].wait()
        for face in (2, 3):
            at = (face - 2) * (plane - n)
            runs = [fields_ref[:, plane * i + at : plane * i + at + n] for i in range(n)]
            own[face] = padded(jnp.concatenate(runs, axis=1)).astype(BF)
        for i in range(n):
            xs[i], xl[i] = split(slab(i))
        loads[3].wait()
        stack = xs[...].reshape(n * ROWS, LANES)[:, :plane]
        ends = dot(stack, pick_ref[...]).reshape(n, ROWS, 128)
        for face in (4, 5):
            at = (face - 4) * n
            runs = [ends[i, :, at : at + n] for i in range(n)]
            own[face] = padded(jnp.concatenate(runs, axis=1)).astype(BF)

    def thirds(value):
        lane = lax.broadcasted_iota(jnp.int32, value.shape, value.ndim - 1)
        hi = value.astype(BF).astype(F32)
        return jnp.where(lane < 2 * ROWS, hi, value - hi).astype(BF)

    def volume_flux():
        for load in loads[4:]:
            load.wait()
        raw[...] = jnp.zeros_like(raw)
        for axis in range(3):
            scaled = flux_ref[axis] * (-TIME_STEP * jac_ref[0, axis])
            for k in range(3):
                raw[axis, 0:width, ROWS * k : ROWS * k + width] = scaled
        mix[...] = thirds(raw[...])
        row = lax.broadcasted_iota(jnp.int32, (ROWS, LANES), 0)
        lane = lax.broadcasted_iota(jnp.int32, (ROWS, LANES), 1)
        diagonal = jnp.logical_and(jnp.bitwise_and(lane, ROWS - 1) == row, lane < 3 * ROWS)
        for face in range(6):
            side = lift if face % 2 else -lift
            keep = lift * TIME_STEP * jac_ref[0, face // 2]
            lift_lhs[face] = thirds(raw[face // 2] * side + jnp.where(diagonal, keep, 0.0))
        for i in range(n):
            mixed = fluxed(mix[...].reshape(3 * ROWS, LANES), xs[i], xl[i])
            gx[i] = mixed[:ROWS]
            for axis in range(2):
                part = mixed[ROWS * (axis + 1) : ROWS * (axis + 2)]
                gs[axis, 0, i], gs[axis, 1, i] = split(part)

    def face_facts(face):
        first, second = lane_ref[0:1, :], lane_ref[1:2, :]
        ones = jnp.ones((1, LANES), F32)
        code = code_ref[0, face]
        order = order_ref[0, face].astype(F32)
        swap = jnp.where(code >= 4, 1, 0)
        rev_a = lax.rem(lax.div(code, 2), 2)
        rev_b = lax.rem(code, 2)
        use_first = jnp.where(swap == 1, rev_b, rev_a) == 1
        use_second = jnp.where(swap == 1, rev_a, rev_b) == 1
        sign = jnp.where(use_first, lane_ref[2:3, :], ones) * jnp.where(
            use_second, lane_ref[3:4, :], ones
        )
        keep = jnp.where((first < order) & (second < order), 1.0, 0.0)
        return swap, sign, keep

    def own_faces():
        own_flat = own[...].reshape(6 * ROWS, LANES)[:, :plane]
        own_modes = (dot(own_flat, fwd_ref[0, 0]) + dot(own_flat, fwd_ref[0, 1])).reshape(
            6, ROWS, LANES
        )
        modes = []
        for face in range(6):
            swap, sign, keep = face_facts(face)
            if face < 4:
                modes.append(own_modes[face] * -keep)
            else:
                far = own[face ^ 1][:, :plane]
                turned = dot(far, fwd_ref[swap, 0]) + dot(far, fwd_ref[swap, 1])
                modes.append((turned * sign - own_modes[face]) * keep)
        modes_hi, modes_lo = split(jnp.concatenate(modes, axis=0))
        modes_hi, modes_lo = modes_hi[:, :plane], modes_lo[:, :plane]
        jump = dot(modes_hi, back_ref[0]) + dot(modes_lo, back_ref[0]) + dot(modes_hi, back_ref[1])
        jump_hi, jump_lo = split(jump)
        cut = lambda a, f: a[ROWS * f : ROWS * (f + 1)]
        for face in range(6):
            early[face] = fluxed(lift_lhs[face], cut(jump_hi, face), cut(jump_lo, face))

    def answer(face):
        pl.semaphore_wait(ack.at[face], 1)
        copies[face].start()

    def when(condition, *steps):
        @pl.when(condition)
        def _():
            for step in steps:
                step()

    odd = lax.rem(sub, 2) == 1
    corner = (blk == 0) & (sub < 2)
    even = jnp.logical_not(odd)
    rest = jnp.logical_not(corner)
    y_first = odd | (blk == 0)
    before = odd | corner
    inner = (blk != 0) & (sub != 0)

    loads[0].wait()
    loads[1].wait()
    own[0] = slab(0).astype(BF)
    own[1] = slab(last).astype(BF)
    for load in loads[FIRST:]:
        load.start()
    when(before, traces)
    when(corner, volume_flux, own_faces)
    pl.semaphore_wait(barrier, 2)
    copies[1].start()
    for face in ENTRY:
        pl.semaphore_signal(ack.at[face ^ 1], inc=1, device_id=across[face], device_id_type=MESH)
    when(jnp.logical_not(before), traces)
    copies[3].start()
    when(rest & y_first, lambda: answer(2))
    when(rest & jnp.logical_not(y_first), lambda: answer(0))
    when(rest, volume_flux)
    when(inner & odd, lambda: answer(0))
    when(inner & even, lambda: answer(2))
    when(rest, own_faces)

    for face in range(4):
        swap, sign, keep = face_facts(face)
        scale = sign * keep
        f_hi = (fwd_ref[swap, 0].astype(F32) * scale).astype(BF)[:, :plane]
        f_lo = (fwd_ref[swap, 1].astype(F32) * scale).astype(BF)[:, :plane]
        whole = dot(f_hi, back_ref[0]) + dot(f_lo, back_ref[0]) + dot(f_hi, back_ref[1])
        oper[face, 0], oper[face, 1] = split(whole)

    runs = []
    for i in range(n):
        both = jnp.concatenate([early[f, :, n * i : n * (i + 1)] for f in (4, 5)], axis=1)
        hi = both.astype(BF).astype(F32)
        runs.append(jnp.concatenate([hi, both - hi], axis=1).astype(BF))
    total = dot(jnp.concatenate(runs, axis=0), put_ref[...])
    for axis in range(2):
        hi = gs[axis, 0].reshape(n * ROWS, LANES)[:, :plane]
        lo = gs[axis, 1].reshape(n * ROWS, LANES)[:, :plane]
        total = total + dot(hi, deriv_ref[axis, 0])
        total = total + dot(lo, deriv_ref[axis, 0])
        total = total + dot(hi, deriv_ref[axis, 1])
    vol[...] = total.reshape(n, ROWS, LANES)
    when(corner | ((blk != 0) & (sub == 0)), lambda: answer(2))

    half = n // 2
    for r in range(0, -(-width // 8) * 8, 8):
        for c in range(0, LANES, 128):
            at = (slice(r, r + 8), slice(c, c + 128))
            plus, minus = [], []
            for a in range(half):
                one, two = gx[(a,) + at], gx[(last - a,) + at]
                plus.append(one + two)
                minus.append(one - two)
            middle = gx[(half,) + at]
            for i in range(half):
                even = minus[0] * float(0.5 * (diff[i, 0] - diff[i, last]))
                uneven = middle * float(diff[i, half])
                for a in range(half):
                    uneven = uneven + plus[a] * float(0.5 * (diff[i, a] + diff[i, last - a]))
                    if a:
                        even = even + minus[a] * float(0.5 * (diff[i, a] - diff[i, last - a]))
                vol[(i,) + at] += even + uneven
                vol[(last - i,) + at] += even - uneven
            even = minus[0] * float(diff[half, 0])
            for a in range(1, half):
                even = even + minus[a] * float(diff[half, a])
            vol[(half,) + at] += even
    for i in range(n):
        value = vol[i]
        if i == 0:
            value = value + early[0]
        if i == last:
            value = value + early[1]
        out_ref[:, plane * i : plane * (i + 1)] = value[:width, :plane]
    when(blk == 0, lambda: answer(0))

    def arrived(pair):
        for face in pair:
            copies[face ^ 1].wait_recv()
        return far_terms(pair, remote, oper, lift_lhs)

    for face, part in zip((2, 3), arrived((2, 3))):
        total = (part + early[face])[:width]
        at = (face - 2) * (plane - n)
        for i in range(n):
            out_ref[:, plane * i + at : plane * i + at + n] += total[:, n * i : n * (i + 1)]
    for face in (0, 1):
        copies[face ^ 1].wait_recv()
        far_ref[face] = remote[face]
    for copy in copies:
        copy.wait_send()


def finish(n, part_ref, far_ref, oper, lift_lhs, out_ref, low_ref, high_ref, sem):
    width, points = part_ref.shape
    plane = n * n
    low = low_ref.shape[1]
    high = points - high_ref.shape[1]
    write = lambda a, i, start, stop: pltpu.make_async_copy(
        a, out_ref.at[:, 0, start:stop], sem.at[i]
    )
    inner = write(part_ref.at[:, low:high], 0, low, high)
    inner.start()
    first, second = far_terms((0, 1), far_ref, oper, lift_lhs)
    low_ref[...] = part_ref[:, :low]
    low_ref[:, :plane] += first[:width, :plane]
    high_ref[...] = part_ref[:, high:]
    high_ref[:, points - plane - high :] += second[:width, :plane]
    outer = [write(low_ref, 1, 0, low), write(high_ref, 2, high, points)]
    for copy in outer:
        copy.start()
    for copy in [inner] + outer:
        copy.wait()


def solution(mesh):
    sizes = (mesh.shape["blk"], mesh.shape["sub"])

    def on_device(fields, flux_matrix, inv_jacobian, neighbour, orientation, face_order):
        width, points = fields.shape[1:]
        n = round(points ** (1.0 / 3.0))
        plane = n * n
        *constants, diff = tables(n)
        rows = jnp.transpose(fields, (1, 0, 2))
        hbm = pl.BlockSpec(memory_space=pltpu.HBM)
        operands = [orientation, face_order, inv_jacobian, rows, flux_matrix]
        operands += [jnp.asarray(a) for a in constants]
        vmem = lambda a: pltpu.VMEM(a.shape, a.dtype)
        vmem_spec = pl.BlockSpec(memory_space=pltpu.VMEM)

        def scoped(*refs):
            pl.run_scoped(
                functools.partial(body, n, diff, sizes, *refs),
                pltpu.SemaphoreType.DMA((13,)),
                pltpu.SemaphoreType.DMA((4,)),
                pltpu.SemaphoreType.DMA((4,)),
                pltpu.SemaphoreType.REGULAR((4,)),
            )

        parts = pl.pallas_call(
            scoped,
            out_shape=(
                pltpu.VMEM((width, points), F32),
                pltpu.VMEM((2, ROWS, LANES), BF),
                pltpu.VMEM((4, 2, plane, LANES), BF),
                pltpu.VMEM((6, ROWS, LANES), BF),
            ),
            in_specs=[hbm] * len(operands),
            out_specs=[vmem_spec] * 4,
            scratch_shapes=[pltpu.SMEM(a.shape, a.dtype) for a in operands[:3]]
            + [pltpu.VMEM((width, points), F32)]
            + [vmem(a) for a in operands[4:]]
            + [
                pltpu.VMEM((n, ROWS, LANES), BF),
                pltpu.VMEM((n, ROWS, LANES), BF),
                pltpu.VMEM((n, ROWS, LANES), F32),
                pltpu.VMEM((2, 2, n, ROWS, LANES), BF),
                pltpu.VMEM((n, ROWS, LANES), F32),
                pltpu.VMEM((6, ROWS, LANES), BF),
                pltpu.VMEM((4, ROWS, LANES), BF),
                pltpu.VMEM((3, ROWS, LANES), F32),
                pltpu.VMEM((3, ROWS, LANES), BF),
                pltpu.VMEM((6, ROWS, LANES), F32),
            ],
            compiler_params=pltpu.CompilerParams(
                collective_id=0, has_side_effects=True, vmem_limit_bytes=48 * 1024 * 1024
            ),
        )(*[pltpu.with_memory_space_constraint(a, pltpu.HBM) for a in operands])
        low = -(-plane // 128) * 128
        high = plane * (n - 1) // 128 * 128
        out = pl.pallas_call(
            lambda *refs: pl.run_scoped(
                functools.partial(finish, n, *refs), pltpu.SemaphoreType.DMA((3,))
            ),
            out_shape=jax.ShapeDtypeStruct(rows.shape, F32),
            in_specs=[vmem_spec] * 4,
            out_specs=hbm,
            scratch_shapes=[
                pltpu.VMEM((width, low), F32),
                pltpu.VMEM((width, points - high), F32),
            ],
            compiler_params=pltpu.CompilerParams(vmem_limit_bytes=16 * 1024 * 1024),
        )(*parts)
        return jnp.transpose(out, (1, 0, 2))

    return jax.shard_map(
        on_device,
        mesh=mesh,
        in_specs=(
            P(("blk", "sub"), None, None),
            P(),
            P(("blk", "sub"), None),
            P(("blk", "sub"), None),
            P(("blk", "sub"), None),
            P(("blk", "sub"), None),
        ),
        out_specs=P(("blk", "sub"), None, None),
        check_vma=False,
    )
```

```python
import functools

import jax
import jax.numpy as jnp
import numpy as np
from jax import lax
from jax.experimental import pallas as pl
from jax.experimental.pallas import tpu as pltpu
from jax.sharding import PartitionSpec as P

MESH = pl.DeviceIdType.MESH
BF = jnp.bfloat16
F32 = jnp.float32
ROWS = 64
LANES = 256
TIME_STEP = 0.01
ENTRY = (1, 3)
FIRST = 13


def cheb_np(n):
    idx = np.arange(n)
    x = -np.cos(np.pi * idx / (n - 1))
    c = np.where((idx == 0) | (idx == n - 1), 2.0, 1.0) * np.where(idx % 2 == 0, 1.0, -1.0)
    eye = np.eye(n)
    off = c[:, None] / c[None, :] / (x[:, None] - x[None, :] + eye) * (1.0 - eye)
    return off - np.diag(off.sum(axis=1))


def dct_np(n):
    k = np.arange(n)[:, None]
    j = np.arange(n)[None, :]
    basis = np.cos(np.pi * k * (j + 0.5) / n) * np.sqrt(2.0 / n)
    return basis * np.where(k == 0, np.sqrt(0.5), 1.0)


def hi_lo(matrix):
    full = matrix.astype(np.float32)
    hi = full.astype(BF)
    lo = (full - hi.astype(np.float32)).astype(BF)
    return np.stack([hi, lo])


def wide(matrix, lanes=LANES):
    return np.pad(matrix, ((0, 0), (0, lanes - matrix.shape[1])))


def tables(n):
    plane = n * n
    d = cheb_np(n)
    c = dct_np(n)
    eye = np.eye(n)
    deriv = np.stack([hi_lo(wide(np.kron(d.T, eye))), hi_lo(wide(np.kron(eye, d.T)))])
    forward = np.kron(c.T, c.T)
    swapped = forward.reshape(plane, n, n).transpose(0, 2, 1).reshape(plane, plane)
    fwd = np.stack([hi_lo(wide(forward)), hi_lo(wide(swapped))])
    back = hi_lo(wide(np.kron(c, c)))
    lane = np.arange(LANES)
    first = np.where(lane < plane, lane // n, 999)
    second = np.where(lane < plane, lane % n, 999)
    sign = lambda v: np.where(v % 2 == 0, 1.0, -1.0)
    lanes = np.stack(
        [first, second, sign(first), sign(second)] + [first * 0] * 4
    ).astype(np.float32)
    pick = np.zeros((plane, 2 * n))
    for j in range(n):
        pick[n * j, j] = 1.0
        pick[n * j + n - 1, n + j] = 1.0
    put = np.concatenate([pick.T, pick.T])
    return deriv, fwd, back, lanes, wide(pick, 128).astype(BF), wide(put).astype(BF), d


def split(value):
    hi = value.astype(BF)
    return hi, (value - hi.astype(F32)).astype(BF)


def dot(a, b):
    return jnp.dot(a, b, preferred_element_type=F32)


def fluxed(lhs, hi, lo):
    return dot(lhs[:, : 3 * ROWS], jnp.concatenate([hi, lo, hi], axis=0))


def far_terms(pair, far, oper, lift_lhs):
    plane = oper.shape[2]
    turned = [
        dot(far[f][:, :plane], oper[f, 0]) + dot(far[f][:, :plane], oper[f, 1]) for f in pair
    ]
    return [fluxed(lift_lhs[f], *split(t)) for f, t in zip(pair, turned)]


def body(
    n, diff, sizes,
    code_hbm, order_hbm, jac_hbm, fields_hbm, flux_hbm,
    deriv_hbm, fwd_hbm, back_hbm, lane_hbm, pick_hbm, put_hbm,
    out_ref, far_ref, oper, lift_lhs,
    code_ref, order_ref, jac_ref, fields_ref, flux_ref,
    deriv_ref, fwd_ref, back_ref, lane_ref, pick_ref, put_ref,
    xs, xl, gx, gs, vol, own, remote, raw, mix, early,
    load_sem, send_sem, recv_sem, ack,
):
    width, points = fields_ref.shape
    plane = n * n
    last = n - 1
    blk, sub = lax.axis_index("blk"), lax.axis_index("sub")
    n_blk, n_sub = sizes
    across = [
        (lax.rem(blk + n_blk - 1, n_blk), sub),
        (lax.rem(blk + 1, n_blk), sub),
        (blk, lax.rem(sub + n_sub - 1, n_sub)),
        (blk, lax.rem(sub + 1, n_sub)),
    ]
    barrier = pltpu.get_barrier_semaphore()
    for face in ENTRY:
        pl.semaphore_signal(barrier, inc=1, device_id=across[face ^ 1], device_id_type=MESH)
    low = -(-plane // 128) * 128
    high = plane * last // 128 * 128
    piece = lambda a, b: (fields_hbm.at[:, 0, a:b], fields_ref.at[:, a:b])
    pairs = [
        piece(0, low), piece(high, points), piece(low, high),
        (pick_hbm, pick_ref), (fwd_hbm, fwd_ref), (lane_hbm, lane_ref), (back_hbm, back_ref),
        (flux_hbm, flux_ref), (deriv_hbm, deriv_ref), (put_hbm, put_ref),
        (jac_hbm, jac_ref), (code_hbm, code_ref), (order_hbm, order_ref),
    ]
    loads = [pltpu.make_async_copy(a, b, load_sem.at[i]) for i, (a, b) in enumerate(pairs)]
    for load in loads[:FIRST]:
        load.start()
    used = -(-width // 8) * 8
    for face in range(4):
        remote[face, used:] = jnp.zeros((ROWS - used, LANES), BF)
    copies = [
        pltpu.make_async_remote_copy(
            src_ref=own.at[face, 0:used],
            dst_ref=remote.at[face ^ 1, 0:used],
            send_sem=send_sem.at[face],
            recv_sem=recv_sem.at[face ^ 1],
            device_id=across[face],
            device_id_type=MESH,
        )
        for face in range(4)
    ]

    def padded(value):
        return jnp.pad(value, ((0, ROWS - value.shape[0]), (0, LANES - value.shape[1])))

    def slab(i):
        return padded(fields_ref[:, plane * i : plane * (i + 1)])

    lift = 0.5 * last * last * 0.5

    def traces():
        loads[2].wait()
        for face in (2, 3):
            at = (face - 2) * (plane - n)
            runs = [fields_ref[:, plane * i + at : plane * i + at + n] for i in range(n)]
            own[face] = padded(jnp.concatenate(runs, axis=1)).astype(BF)
        for i in range(n):
            xs[i], xl[i] = split(slab(i))
        loads[3].wait()
        stack = xs[...].reshape(n * ROWS, LANES)[:, :plane]
        ends = dot(stack, pick_ref[...]).reshape(n, ROWS, 128)
        for face in (4, 5):
            at = (face - 4) * n
            runs = [ends[i, :, at : at + n] for i in range(n)]
            own[face] = padded(jnp.concatenate(runs, axis=1)).astype(BF)

    def thirds(value):
        lane = lax.broadcasted_iota(jnp.int32, value.shape, value.ndim - 1)
        hi = value.astype(BF).astype(F32)
        return jnp.where(lane < 2 * ROWS, hi, value - hi).astype(BF)

    def volume_flux():
        for load in loads[4:]:
            load.wait()
        raw[...] = jnp.zeros_like(raw)
        for axis in range(3):
            scaled = flux_ref[axis] * (-TIME_STEP * jac_ref[0, axis])
            for k in range(3):
                raw[axis, 0:width, ROWS * k : ROWS * k + width] = scaled
        mix[...] = thirds(raw[...])
        row = lax.broadcasted_iota(jnp.int32, (ROWS, LANES), 0)
        lane = lax.broadcasted_iota(jnp.int32, (ROWS, LANES), 1)
        diagonal = jnp.logical_and(jnp.bitwise_and(lane, ROWS - 1) == row, lane < 3 * ROWS)
        for face in range(6):
            side = lift if face % 2 else -lift
            keep = lift * TIME_STEP * jac_ref[0, face // 2]
            lift_lhs[face] = thirds(raw[face // 2] * side + jnp.where(diagonal, keep, 0.0))
        for i in range(n):
            mixed = fluxed(mix[...].reshape(3 * ROWS, LANES), xs[i], xl[i])
            gx[i] = mixed[:ROWS]
            for axis in range(2):
                part = mixed[ROWS * (axis + 1) : ROWS * (axis + 2)]
                gs[axis, 0, i], gs[axis, 1, i] = split(part)

    def face_facts(face):
        first, second = lane_ref[0:1, :], lane_ref[1:2, :]
        ones = jnp.ones((1, LANES), F32)
        code = code_ref[0, face]
        order = order_ref[0, face].astype(F32)
        swap = jnp.where(code >= 4, 1, 0)
        rev_a = lax.rem(lax.div(code, 2), 2)
        rev_b = lax.rem(code, 2)
        use_first = jnp.where(swap == 1, rev_b, rev_a) == 1
        use_second = jnp.where(swap == 1, rev_a, rev_b) == 1
        sign = jnp.where(use_first, lane_ref[2:3, :], ones) * jnp.where(
            use_second, lane_ref[3:4, :], ones
        )
        keep = jnp.where((first < order) & (second < order), 1.0, 0.0)
        return swap, sign, keep

    def own_faces():
        own_flat = own[...].reshape(6 * ROWS, LANES)[:, :plane]
        own_modes = (dot(own_flat, fwd_ref[0, 0]) + dot(own_flat, fwd_ref[0, 1])).reshape(
            6, ROWS, LANES
        )
        modes = []
        for face in range(6):
            swap, sign, keep = face_facts(face)
            if face < 4:
                modes.append(own_modes[face] * -keep)
            else:
                far = own[face ^ 1][:, :plane]
                turned = dot(far, fwd_ref[swap, 0]) + dot(far, fwd_ref[swap, 1])
                modes.append((turned * sign - own_modes[face]) * keep)
        modes_hi, modes_lo = split(jnp.concatenate(modes, axis=0))
        modes_hi, modes_lo = modes_hi[:, :plane], modes_lo[:, :plane]
        jump = dot(modes_hi, back_ref[0]) + dot(modes_lo, back_ref[0]) + dot(modes_hi, back_ref[1])
        jump_hi, jump_lo = split(jump)
        cut = lambda a, f: a[ROWS * f : ROWS * (f + 1)]
        for face in range(6):
            early[face] = fluxed(lift_lhs[face], cut(jump_hi, face), cut(jump_lo, face))

    def answer(face):
        pl.semaphore_wait(ack.at[face], 1)
        copies[face].start()

    def when(condition, *steps):
        @pl.when(condition)
        def _():
            for step in steps:
                step()

    odd = lax.rem(sub, 2) == 1
    corner = (blk == 0) & (sub < 2)
    even = jnp.logical_not(odd)
    rest = jnp.logical_not(corner)
    y_first = odd | (blk == 0)
    before = odd | corner
    inner = (blk != 0) & (sub != 0)

    loads[0].wait()
    loads[1].wait()
    own[0] = slab(0).astype(BF)
    own[1] = slab(last).astype(BF)
    for load in loads[FIRST:]:
        load.start()
    when(before, traces)
    when(corner, volume_flux, own_faces)
    pl.semaphore_wait(barrier, 2)
    when(even | corner, copies[1].start)
    for face in ENTRY:
        pl.semaphore_signal(ack.at[face ^ 1], inc=1, device_id=across[face], device_id_type=MESH)
    when(jnp.logical_not(before), traces)
    copies[3].start()
    when(rest & y_first, lambda: answer(2))
    when(rest & jnp.logical_not(y_first), lambda: answer(0))
    when(rest, volume_flux)
    when(odd & rest, copies[1].start)
    when(inner & odd, lambda: answer(0))
    when(inner & even, lambda: answer(2))
    when(rest, own_faces)
    when((blk != 0) & (sub == 0), lambda: answer(2))

    for face in range(4):
        swap, sign, keep = face_facts(face)
        scale = sign * keep
        f_hi = (fwd_ref[swap, 0].astype(F32) * scale).astype(BF)[:, :plane]
        f_lo = (fwd_ref[swap, 1].astype(F32) * scale).astype(BF)[:, :plane]
        whole = dot(f_hi, back_ref[0]) + dot(f_lo, back_ref[0]) + dot(f_hi, back_ref[1])
        oper[face, 0], oper[face, 1] = split(whole)

    runs = []
    for i in range(n):
        both = jnp.concatenate([early[f, :, n * i : n * (i + 1)] for f in (4, 5)], axis=1)
        hi = both.astype(BF).astype(F32)
        runs.append(jnp.concatenate([hi, both - hi], axis=1).astype(BF))
    total = dot(jnp.concatenate(runs, axis=0), put_ref[...])
    for axis in range(2):
        hi = gs[axis, 0].reshape(n * ROWS, LANES)[:, :plane]
        lo = gs[axis, 1].reshape(n * ROWS, LANES)[:, :plane]
        total = total + dot(hi, deriv_ref[axis, 0])
        total = total + dot(lo, deriv_ref[axis, 0])
        total = total + dot(hi, deriv_ref[axis, 1])
    vol[...] = total.reshape(n, ROWS, LANES)
    when(corner, lambda: answer(2))
    when(rest & (blk == 0), lambda: answer(0))

    half = n // 2
    for r in range(0, -(-width // 8) * 8, 8):
        for c in range(0, LANES, 128):
            at = (slice(r, r + 8), slice(c, c + 128))
            plus, minus = [], []
            for a in range(half):
                one, two = gx[(a,) + at], gx[(last - a,) + at]
                plus.append(one + two)
                minus.append(one - two)
            middle = gx[(half,) + at]
            for i in range(half):
                even = minus[0] * float(0.5 * (diff[i, 0] - diff[i, last]))
                uneven = middle * float(diff[i, half])
                for a in range(half):
                    uneven = uneven + plus[a] * float(0.5 * (diff[i, a] + diff[i, last - a]))
                    if a:
                        even = even + minus[a] * float(0.5 * (diff[i, a] - diff[i, last - a]))
                vol[(i,) + at] += even + uneven
                vol[(last - i,) + at] += even - uneven
            even = minus[0] * float(diff[half, 0])
            for a in range(1, half):
                even = even + minus[a] * float(diff[half, a])
            vol[(half,) + at] += even
    for i in range(n):
        value = vol[i]
        if i == 0:
            value = value + early[0]
        if i == last:
            value = value + early[1]
        out_ref[:, plane * i : plane * (i + 1)] = value[:width, :plane]
    when(corner, lambda: answer(0))

    def arrived(pair):
        for face in pair:
            copies[face ^ 1].wait_recv()
        return far_terms(pair, remote, oper, lift_lhs)

    for face, part in zip((2, 3), arrived((2, 3))):
        total = (part + early[face])[:width]
        at = (face - 2) * (plane - n)
        for i in range(n):
            out_ref[:, plane * i + at : plane * i + at + n] += total[:, n * i : n * (i + 1)]
    for face in (0, 1):
        copies[face ^ 1].wait_recv()
        far_ref[face] = remote[face]
    for copy in copies:
        copy.wait_send()


def finish(n, part_ref, far_ref, oper, lift_lhs, out_ref, low_ref, high_ref, sem):
    width, points = part_ref.shape
    plane = n * n
    low = low_ref.shape[1]
    high = points - high_ref.shape[1]
    write = lambda a, i, start, stop: pltpu.make_async_copy(
        a, out_ref.at[:, 0, start:stop], sem.at[i]
    )
    inner = write(part_ref.at[:, low:high], 0, low, high)
    inner.start()
    first, second = far_terms((0, 1), far_ref, oper, lift_lhs)
    low_ref[...] = part_ref[:, :low]
    low_ref[:, :plane] += first[:width, :plane]
    high_ref[...] = part_ref[:, high:]
    high_ref[:, points - plane - high :] += second[:width, :plane]
    outer = [write(low_ref, 1, 0, low), write(high_ref, 2, high, points)]
    for copy in outer:
        copy.start()
    for copy in [inner] + outer:
        copy.wait()


def solution(mesh):
    sizes = (mesh.shape["blk"], mesh.shape["sub"])

    def on_device(fields, flux_matrix, inv_jacobian, neighbour, orientation, face_order):
        width, points = fields.shape[1:]
        n = round(points ** (1.0 / 3.0))
        plane = n * n
        *constants, diff = tables(n)
        rows = jnp.transpose(fields, (1, 0, 2))
        hbm = pl.BlockSpec(memory_space=pltpu.HBM)
        operands = [orientation, face_order, inv_jacobian, rows, flux_matrix]
        operands += [jnp.asarray(a) for a in constants]
        vmem = lambda a: pltpu.VMEM(a.shape, a.dtype)
        vmem_spec = pl.BlockSpec(memory_space=pltpu.VMEM)

        def scoped(*refs):
            pl.run_scoped(
                functools.partial(body, n, diff, sizes, *refs),
                pltpu.SemaphoreType.DMA((13,)),
                pltpu.SemaphoreType.DMA((4,)),
                pltpu.SemaphoreType.DMA((4,)),
                pltpu.SemaphoreType.REGULAR((4,)),
            )

        parts = pl.pallas_call(
            scoped,
            out_shape=(
                pltpu.VMEM((width, points), F32),
                pltpu.VMEM((2, ROWS, LANES), BF),
                pltpu.VMEM((4, 2, plane, LANES), BF),
                pltpu.VMEM((6, ROWS, LANES), BF),
            ),
            in_specs=[hbm] * len(operands),
            out_specs=[vmem_spec] * 4,
            scratch_shapes=[pltpu.SMEM(a.shape, a.dtype) for a in operands[:3]]
            + [pltpu.VMEM((width, points), F32)]
            + [vmem(a) for a in operands[4:]]
            + [
                pltpu.VMEM((n, ROWS, LANES), BF),
                pltpu.VMEM((n, ROWS, LANES), BF),
                pltpu.VMEM((n, ROWS, LANES), F32),
                pltpu.VMEM((2, 2, n, ROWS, LANES), BF),
                pltpu.VMEM((n, ROWS, LANES), F32),
                pltpu.VMEM((6, ROWS, LANES), BF),
                pltpu.VMEM((4, ROWS, LANES), BF),
                pltpu.VMEM((3, ROWS, LANES), F32),
                pltpu.VMEM((3, ROWS, LANES), BF),
                pltpu.VMEM((6, ROWS, LANES), F32),
            ],
            compiler_params=pltpu.CompilerParams(
                collective_id=0, has_side_effects=True, vmem_limit_bytes=48 * 1024 * 1024
            ),
        )(*[pltpu.with_memory_space_constraint(a, pltpu.HBM) for a in operands])
        low = -(-plane // 128) * 128
        high = plane * (n - 1) // 128 * 128
        out = pl.pallas_call(
            lambda *refs: pl.run_scoped(
                functools.partial(finish, n, *refs), pltpu.SemaphoreType.DMA((3,))
            ),
            out_shape=jax.ShapeDtypeStruct(rows.shape, F32),
            in_specs=[vmem_spec] * 4,
            out_specs=hbm,
            scratch_shapes=[
                pltpu.VMEM((width, low), F32),
                pltpu.VMEM((width, points - high), F32),
            ],
            compiler_params=pltpu.CompilerParams(vmem_limit_bytes=16 * 1024 * 1024),
        )(*parts)
        return jnp.transpose(out, (1, 0, 2))

    return jax.shard_map(
        on_device,
        mesh=mesh,
        in_specs=(
            P(("blk", "sub"), None, None),
            P(),
            P(("blk", "sub"), None),
            P(("blk", "sub"), None),
            P(("blk", "sub"), None),
            P(("blk", "sub"), None),
        ),
        out_specs=P(("blk", "sub"), None, None),
        check_vma=False,
    )
```

```python
import functools

import jax
import jax.numpy as jnp
import numpy as np
from jax import lax
from jax.experimental import pallas as pl
from jax.experimental.pallas import tpu as pltpu
from jax.sharding import PartitionSpec as P

MESH = pl.DeviceIdType.MESH
BF = jnp.bfloat16
F32 = jnp.float32
ROWS = 64
LANES = 256
TIME_STEP = 0.01
ENTRY = (1, 3)


def cheb_np(n):
    idx = np.arange(n)
    x = -np.cos(np.pi * idx / (n - 1))
    c = np.where((idx == 0) | (idx == n - 1), 2.0, 1.0) * np.where(idx % 2 == 0, 1.0, -1.0)
    eye = np.eye(n)
    off = c[:, None] / c[None, :] / (x[:, None] - x[None, :] + eye) * (1.0 - eye)
    return off - np.diag(off.sum(axis=1))


def dct_np(n):
    k = np.arange(n)[:, None]
    j = np.arange(n)[None, :]
    basis = np.cos(np.pi * k * (j + 0.5) / n) * np.sqrt(2.0 / n)
    return basis * np.where(k == 0, np.sqrt(0.5), 1.0)


def hi_lo(matrix):
    full = matrix.astype(np.float32)
    hi = full.astype(BF)
    lo = (full - hi.astype(np.float32)).astype(BF)
    return np.stack([hi, lo])


def wide(matrix, lanes=LANES):
    return np.pad(matrix, ((0, 0), (0, lanes - matrix.shape[1])))


def tables(n):
    plane = n * n
    d = cheb_np(n)
    c = dct_np(n)
    eye = np.eye(n)
    deriv = np.stack([hi_lo(wide(np.kron(d.T, eye))), hi_lo(wide(np.kron(eye, d.T)))])
    forward = np.kron(c.T, c.T)
    swapped = forward.reshape(plane, n, n).transpose(0, 2, 1).reshape(plane, plane)
    fwd = np.stack([hi_lo(wide(forward)), hi_lo(wide(swapped))])
    back = hi_lo(wide(np.kron(c, c)))
    lane = np.arange(LANES)
    first = np.where(lane < plane, lane // n, 999)
    second = np.where(lane < plane, lane % n, 999)
    sign = lambda v: np.where(v % 2 == 0, 1.0, -1.0)
    lanes = np.stack(
        [first, second, sign(first), sign(second)] + [first * 0] * 4
    ).astype(np.float32)
    pick = np.zeros((plane, 2 * n))
    for j in range(n):
        pick[n * j, j] = 1.0
        pick[n * j + n - 1, n + j] = 1.0
    put = np.concatenate([pick.T, pick.T])
    return deriv, fwd, back, lanes, wide(pick, 128).astype(BF), wide(put).astype(BF), d


def split(value):
    hi = value.astype(BF)
    return hi, (value - hi.astype(F32)).astype(BF)


def dot(a, b):
    return jnp.dot(a, b, preferred_element_type=F32)


def fluxed(lhs, hi, lo):
    return dot(lhs[:, : 3 * ROWS], jnp.concatenate([hi, hi, lo], axis=0))


def far_terms(pair, far, oper, lift_lhs, plane):
    turned = []
    for f in pair:
        depth = plane if f > 1 else LANES
        one = far[f][:, :depth]
        turned.append(dot(one, oper[f, 0, :depth]) + dot(one, oper[f, 1, :depth]))
    return [fluxed(lift_lhs[f], *split(t)) for f, t in zip(pair, turned)]


def body(
    n, diff, sizes,
    code_hbm, order_hbm, jac_hbm, fields_hbm, flux_hbm,
    deriv_hbm, fwd_hbm, back_hbm, lane_hbm, pick_hbm, put_hbm,
    out_ref, far_ref, oper, lift_lhs,
    code_ref, order_ref, jac_ref, fields_ref, flux_ref,
    deriv_ref, fwd_ref, back_ref, lane_ref, pick_ref, put_ref,
    xs, xl, gx, gs, vol, own, remote, raw, mix, early,
    load_sem, send_sem, recv_sem, ack,
):
    width, points = fields_ref.shape
    plane = n * n
    last = n - 1
    blk, sub = lax.axis_index("blk"), lax.axis_index("sub")
    n_blk, n_sub = sizes
    across = [
        (lax.rem(blk + n_blk - 1, n_blk), sub),
        (lax.rem(blk + 1, n_blk), sub),
        (blk, lax.rem(sub + n_sub - 1, n_sub)),
        (blk, lax.rem(sub + 1, n_sub)),
    ]
    barrier = pltpu.get_barrier_semaphore()
    low = -(-plane // 128) * 128
    high = plane * last // 128 * 128
    piece = lambda a, b: (fields_hbm.at[:, 0, a:b], fields_ref.at[:, a:b])
    pairs = [
        piece(high, points), piece(0, low), piece(low, high),
        (pick_hbm, pick_ref), (fwd_hbm, fwd_ref), (lane_hbm, lane_ref), (back_hbm, back_ref),
        (flux_hbm, flux_ref), (deriv_hbm, deriv_ref), (put_hbm, put_ref),
        (jac_hbm, jac_ref), (code_hbm, code_ref), (order_hbm, order_ref),
    ]
    loads = [pltpu.make_async_copy(a, b, load_sem.at[i]) for i, (a, b) in enumerate(pairs)]
    loads[0].start()
    for face in ENTRY:
        pl.semaphore_signal(barrier, inc=1, device_id=across[face ^ 1], device_id_type=MESH)
    for load in loads[1:]:
        load.start()
    used = -(-width // 8) * 8
    for face in range(4):
        remote[face, used:] = jnp.zeros((ROWS - used, LANES), BF)
    copies = [
        pltpu.make_async_remote_copy(
            src_ref=own.at[face, 0:used],
            dst_ref=remote.at[face ^ 1, 0:used],
            send_sem=send_sem.at[face],
            recv_sem=recv_sem.at[face ^ 1],
            device_id=across[face],
            device_id_type=MESH,
        )
        for face in range(4)
    ]

    def padded(value):
        return jnp.pad(value, ((0, ROWS - value.shape[0]), (0, LANES - value.shape[1])))

    def slab(i):
        return padded(fields_ref[:, plane * i : plane * (i + 1)])

    lift = 0.5 * last * last * 0.5

    def traces():
        loads[1].wait()
        own[0] = slab(0).astype(BF)
        loads[2].wait()
        for face in (2, 3):
            at = (face - 2) * (plane - n)
            runs = [fields_ref[:, plane * i + at : plane * i + at + n] for i in range(n)]
            own[face] = padded(jnp.concatenate(runs, axis=1)).astype(BF)
        for i in range(n):
            xs[i], xl[i] = split(slab(i))
        loads[3].wait()
        stack = xs[...].reshape(n * ROWS, LANES)[:, :plane]
        ends = dot(stack, pick_ref[...]).reshape(n, ROWS, 128)
        for face in (4, 5):
            at = (face - 4) * n
            runs = [ends[i, :, at : at + n] for i in range(n)]
            own[face] = padded(jnp.concatenate(runs, axis=1)).astype(BF)

    def thirds(value):
        lane = lax.broadcasted_iota(jnp.int32, value.shape, value.ndim - 1)
        hi = value.astype(BF).astype(F32)
        return jnp.where(lane < 2 * ROWS, hi, value - hi).astype(BF)

    def thirds(value):
        hi = value.astype(BF).astype(F32)
        lane = lax.broadcasted_iota(jnp.int32, value.shape, value.ndim - 1)
        lows = (lane >= ROWS) & (lane < 2 * ROWS)
        return jnp.where(lows, value - hi, hi).astype(BF)

    def flux_matrices():
        for load in loads[4:]:
            load.wait()
        raw[...] = jnp.zeros_like(raw)
        for axis in range(3):
            scaled = flux_ref[axis] * (-TIME_STEP * jac_ref[0, axis])
            for k in range(3):
                raw[axis, 0:width, ROWS * k : ROWS * k + width] = scaled
        mix[...] = thirds(raw[...])
        row = lax.broadcasted_iota(jnp.int32, (ROWS, LANES), 0)
        lane = lax.broadcasted_iota(jnp.int32, (ROWS, LANES), 1)
        diagonal = (jnp.bitwise_and(lane, ROWS - 1) == row) & (lane < 3 * ROWS)
        for face in range(6):
            side = lift if face % 2 else -lift
            keep = lift * TIME_STEP * jac_ref[0, face // 2]
            lift_lhs[face] = thirds(raw[face // 2] * side + jnp.where(diagonal, keep, 0.0))

    def volume_flux():
        for i in range(n):
            mixed = fluxed(mix[...].reshape(3 * ROWS, LANES), xs[i], xl[i])
            gx[i] = mixed[:ROWS]
            for axis in range(2):
                part = mixed[ROWS * (axis + 1) : ROWS * (axis + 2)]
                gs[axis, 0, i], gs[axis, 1, i] = split(part)

    def face_facts(face):
        first, second = lane_ref[0:1, :], lane_ref[1:2, :]
        ones = jnp.ones((1, LANES), F32)
        code = code_ref[0, face]
        order = order_ref[0, face].astype(F32)
        swap = jnp.where(code >= 4, 1, 0)
        rev_a = lax.rem(lax.div(code, 2), 2)
        rev_b = lax.rem(code, 2)
        use_first = jnp.where(swap == 1, rev_b, rev_a) == 1
        use_second = jnp.where(swap == 1, rev_a, rev_b) == 1
        sign = jnp.where(use_first, lane_ref[2:3, :], ones) * jnp.where(
            use_second, lane_ref[3:4, :], ones
        )
        keep = jnp.where((first < order) & (second < order), 1.0, 0.0)
        return swap, sign, keep

    def own_faces():
        rest_flat = own[2:].reshape(4 * ROWS, LANES)
        own_flat = jnp.concatenate([xs[0], xs[last], rest_flat], axis=0)[:, :plane]
        own_modes = (dot(own_flat, fwd_ref[0, 0]) + dot(own_flat, fwd_ref[0, 1])).reshape(
            6, ROWS, LANES
        )
        modes = []
        for face in range(6):
            swap, sign, keep = face_facts(face)
            if face < 4:
                modes.append(own_modes[face] * -keep)
            else:
                far = own[face ^ 1][:, :plane]
                turned = dot(far, fwd_ref[swap, 0]) + dot(far, fwd_ref[swap, 1])
                modes.append((turned * sign - own_modes[face]) * keep)
        modes_hi, modes_lo = split(jnp.concatenate(modes, axis=0))
        modes_hi, modes_lo = modes_hi[:, :plane], modes_lo[:, :plane]
        jump = dot(modes_hi, back_ref[0]) + dot(modes_lo, back_ref[0]) + dot(modes_hi, back_ref[1])
        jump_hi, jump_lo = split(jump)
        cut = lambda a, f: a[ROWS * f : ROWS * (f + 1)]
        for face in range(6):
            early[face] = fluxed(lift_lhs[face], cut(jump_hi, face), cut(jump_lo, face))

    def answer(face):
        pl.semaphore_wait(ack.at[face], 1)
        copies[face].start()

    def when(condition, *steps):
        @pl.when(condition)
        def _():
            for step in steps:
                step()

    odd = lax.rem(sub, 2) == 1
    corner = (blk == 0) & (sub < 2)
    even = jnp.logical_not(odd)
    rest = jnp.logical_not(corner)
    y_first = odd | (blk == 0)
    before = odd | corner
    inner = (blk != 0) & (sub != 0)

    loads[0].wait()
    offset = plane * last - high
    tail = points - high - LANES
    lane = lax.broadcasted_iota(jnp.int32, (width, 128), 1)
    ahead = jnp.pad(fields_ref[:, high + LANES :], ((0, 0), (0, 128 - tail)))
    merged = jnp.where(lane < tail, ahead, fields_ref[:, high : high + 128])
    turned = jnp.concatenate([merged, fields_ref[:, high + 128 : high + LANES]], axis=1)
    own[1] = padded(turned).astype(BF)
    when(before, traces)
    when(corner, flux_matrices, volume_flux, own_faces)
    pl.semaphore_wait(barrier, 2)
    when(even | corner, copies[1].start)
    for face in ENTRY:
        pl.semaphore_signal(ack.at[face ^ 1], inc=1, device_id=across[face], device_id_type=MESH)
    when(jnp.logical_not(before), traces)
    copies[3].start()
    when(rest & y_first, lambda: answer(2))
    when(rest & jnp.logical_not(y_first), lambda: answer(0))
    when(rest, flux_matrices)
    when(odd & rest, copies[1].start)
    when(rest, volume_flux)
    when(inner & odd, lambda: answer(0))
    when(inner & even, lambda: answer(2))
    when(rest, own_faces)
    when((blk != 0) & (sub == 0), lambda: answer(2))

    for face in range(4):
        swap, sign, keep = face_facts(face)
        scale = sign * keep
        f_hi = (fwd_ref[swap, 0].astype(F32) * scale).astype(BF)[:, :plane]
        f_lo = (fwd_ref[swap, 1].astype(F32) * scale).astype(BF)[:, :plane]
        whole = dot(f_hi, back_ref[0]) + dot(f_lo, back_ref[0]) + dot(f_hi, back_ref[1])
        if face == 1:
            whole = pltpu.roll(whole, offset, 1)
        zeros = jnp.zeros((LANES - plane, LANES), F32)
        if face == 0:
            head = plane - tail
            whole = jnp.concatenate([whole[head:], zeros, whole[:head]], axis=0)
        else:
            whole = jnp.concatenate([whole, zeros], axis=0)
        oper[face, 0], oper[face, 1] = split(whole)

    when(rest & even & (blk == 0), lambda: answer(0))

    runs = []
    for i in range(n):
        both = jnp.concatenate([early[f, :, n * i : n * (i + 1)] for f in (4, 5)], axis=1)
        hi = both.astype(BF).astype(F32)
        runs.append(jnp.concatenate([hi, both - hi], axis=1).astype(BF))
    total = dot(jnp.concatenate(runs, axis=0), put_ref[...])
    for axis in range(2):
        hi = gs[axis, 0].reshape(n * ROWS, LANES)[:, :plane]
        lo = gs[axis, 1].reshape(n * ROWS, LANES)[:, :plane]
        total = total + dot(hi, deriv_ref[axis, 0])
        total = total + dot(lo, deriv_ref[axis, 0])
        total = total + dot(hi, deriv_ref[axis, 1])
    vol[...] = total.reshape(n, ROWS, LANES)
    when(corner, lambda: answer(2))
    when(rest & odd & (blk == 0), lambda: answer(0))

    half = n // 2
    for r in range(0, -(-width // 8) * 8, 8):
        for c in range(0, LANES, 128):
            at = (slice(r, r + 8), slice(c, c + 128))
            plus, minus = [], []
            for a in range(half):
                one, two = gx[(a,) + at], gx[(last - a,) + at]
                plus.append(one + two)
                minus.append(one - two)
            middle = gx[(half,) + at]
            for i in range(half):
                even = minus[0] * float(0.5 * (diff[i, 0] - diff[i, last]))
                uneven = middle * float(diff[i, half])
                for a in range(half):
                    uneven = uneven + plus[a] * float(0.5 * (diff[i, a] + diff[i, last - a]))
                    if a:
                        even = even + minus[a] * float(0.5 * (diff[i, a] - diff[i, last - a]))
                vol[(i,) + at] += even + uneven
                vol[(last - i,) + at] += even - uneven
            even = minus[0] * float(diff[half, 0])
            for a in range(1, half):
                even = even + minus[a] * float(diff[half, a])
            vol[(half,) + at] += even
    for i in range(n):
        value = vol[i]
        if i == 0:
            value = value + early[0]
        if i == last:
            value = value + early[1]
        out_ref[:, plane * i : plane * (i + 1)] = value[:width, :plane]
    when(corner, lambda: answer(0))

    def arrived(pair):
        for face in pair:
            copies[face ^ 1].wait_recv()
        return far_terms(pair, remote, oper, lift_lhs, plane)

    for face, part in zip((2, 3), arrived((2, 3))):
        total = (part + early[face])[:width]
        at = (face - 2) * (plane - n)
        for i in range(n):
            out_ref[:, plane * i + at : plane * i + at + n] += total[:, n * i : n * (i + 1)]
    for face in (0, 1):
        copies[face ^ 1].wait_recv()
        far_ref[face] = remote[face]
    for copy in copies:
        copy.wait_send()


def finish(n, part_ref, far_ref, oper, lift_lhs, out_ref, low_ref, high_ref, sem):
    width, points = part_ref.shape
    plane = n * n
    low = low_ref.shape[1]
    high = points - high_ref.shape[1]
    write = lambda a, i, start, stop: pltpu.make_async_copy(
        a, out_ref.at[:, 0, start:stop], sem.at[i]
    )
    inner = write(part_ref.at[:, low:high], 0, low, high)
    inner.start()
    first, second = (part[:width] for part in far_terms((0, 1), far_ref, oper, lift_lhs, plane))
    low_ref[...] = part_ref[:, :low] + first[:, :low]
    lane = lax.broadcasted_iota(jnp.int32, (width, 128), 1)
    begun = jnp.where(lane >= points - plane - high, second[:, :128], 0.0)
    high_ref[:, :128] = part_ref[:, high : high + 128] + begun
    high_ref[:, 128:LANES] = part_ref[:, high + 128 : high + LANES] + second[:, 128:]
    tail = points - high - LANES
    high_ref[:, LANES:] = part_ref[:, high + LANES :] + second[:, :tail]
    outer = [write(low_ref, 1, 0, low), write(high_ref, 2, high, points)]
    for copy in outer:
        copy.start()
    for copy in [inner] + outer:
        copy.wait()


def solution(mesh):
    sizes = (mesh.shape["blk"], mesh.shape["sub"])

    def on_device(fields, flux_matrix, inv_jacobian, neighbour, orientation, face_order):
        width, points = fields.shape[1:]
        n = round(points ** (1.0 / 3.0))
        plane = n * n
        *constants, diff = tables(n)
        rows = jnp.transpose(fields, (1, 0, 2))
        hbm = pl.BlockSpec(memory_space=pltpu.HBM)
        operands = [orientation, face_order, inv_jacobian, rows, flux_matrix]
        operands += [jnp.asarray(a) for a in constants]
        vmem = lambda a: pltpu.VMEM(a.shape, a.dtype)
        vmem_spec = pl.BlockSpec(memory_space=pltpu.VMEM)

        def scoped(*refs):
            pl.run_scoped(
                functools.partial(body, n, diff, sizes, *refs),
                pltpu.SemaphoreType.DMA((13,)),
                pltpu.SemaphoreType.DMA((4,)),
                pltpu.SemaphoreType.DMA((4,)),
                pltpu.SemaphoreType.REGULAR((4,)),
            )

        parts = pl.pallas_call(
            scoped,
            out_shape=(
                pltpu.VMEM((width, points), F32),
                pltpu.VMEM((2, ROWS, LANES), BF),
                pltpu.VMEM((4, 2, LANES, LANES), BF),
                pltpu.VMEM((6, ROWS, LANES), BF),
            ),
            in_specs=[hbm] * len(operands),
            out_specs=[vmem_spec] * 4,
            scratch_shapes=[pltpu.SMEM(a.shape, a.dtype) for a in operands[:3]]
            + [pltpu.VMEM((width, points), F32)]
            + [vmem(a) for a in operands[4:]]
            + [
                pltpu.VMEM((n, ROWS, LANES), BF),
                pltpu.VMEM((n, ROWS, LANES), BF),
                pltpu.VMEM((n, ROWS, LANES), F32),
                pltpu.VMEM((2, 2, n, ROWS, LANES), BF),
                pltpu.VMEM((n, ROWS, LANES), F32),
                pltpu.VMEM((6, ROWS, LANES), BF),
                pltpu.VMEM((4, ROWS, LANES), BF),
                pltpu.VMEM((3, ROWS, LANES), F32),
                pltpu.VMEM((3, ROWS, LANES), BF),
                pltpu.VMEM((6, ROWS, LANES), F32),
            ],
            compiler_params=pltpu.CompilerParams(
                collective_id=0, has_side_effects=True, vmem_limit_bytes=48 * 1024 * 1024
            ),
        )(*[pltpu.with_memory_space_constraint(a, pltpu.HBM) for a in operands])
        low = -(-plane // 128) * 128
        high = plane * (n - 1) // 128 * 128
        out = pl.pallas_call(
            lambda *refs: pl.run_scoped(
                functools.partial(finish, n, *refs), pltpu.SemaphoreType.DMA((3,))
            ),
            out_shape=jax.ShapeDtypeStruct(rows.shape, F32),
            in_specs=[vmem_spec] * 4,
            out_specs=hbm,
            scratch_shapes=[
                pltpu.VMEM((width, low), F32),
                pltpu.VMEM((width, points - high), F32),
            ],
            compiler_params=pltpu.CompilerParams(vmem_limit_bytes=16 * 1024 * 1024),
        )(*parts)
        return jnp.transpose(out, (1, 0, 2))

    return jax.shard_map(
        on_device,
        mesh=mesh,
        in_specs=(
            P(("blk", "sub"), None, None),
            P(),
            P(("blk", "sub"), None),
            P(("blk", "sub"), None),
            P(("blk", "sub"), None),
            P(("blk", "sub"), None),
        ),
        out_specs=P(("blk", "sub"), None, None),
        check_vma=False,
    )
```

```python
import functools

import jax
import jax.numpy as jnp
import numpy as np
from jax import lax
from jax.experimental import pallas as pl
from jax.experimental.pallas import tpu as pltpu
from jax.sharding import PartitionSpec as P

MESH = pl.DeviceIdType.MESH
BF = jnp.bfloat16
F32 = jnp.float32
ROWS = 64
LANES = 256
TIME_STEP = 0.01
ENTRY = (1, 3)


def cheb_np(n):
    idx = np.arange(n)
    x = -np.cos(np.pi * idx / (n - 1))
    c = np.where((idx == 0) | (idx == n - 1), 2.0, 1.0) * np.where(idx % 2 == 0, 1.0, -1.0)
    eye = np.eye(n)
    off = c[:, None] / c[None, :] / (x[:, None] - x[None, :] + eye) * (1.0 - eye)
    return off - np.diag(off.sum(axis=1))


def dct_np(n):
    k = np.arange(n)[:, None]
    j = np.arange(n)[None, :]
    basis = np.cos(np.pi * k * (j + 0.5) / n) * np.sqrt(2.0 / n)
    return basis * np.where(k == 0, np.sqrt(0.5), 1.0)


def hi_lo(matrix):
    full = matrix.astype(np.float32)
    hi = full.astype(BF)
    lo = (full - hi.astype(np.float32)).astype(BF)
    return np.stack([hi, lo])


def wide(matrix, lanes=LANES):
    return np.pad(matrix, ((0, 0), (0, lanes - matrix.shape[1])))


def tables(n):
    plane = n * n
    d = cheb_np(n)
    c = dct_np(n)
    eye = np.eye(n)
    deriv = np.stack([hi_lo(wide(np.kron(d.T, eye))), hi_lo(wide(np.kron(eye, d.T)))])
    forward = np.kron(c.T, c.T)
    swapped = forward.reshape(plane, n, n).transpose(0, 2, 1).reshape(plane, plane)
    fwd = np.stack([hi_lo(wide(forward)), hi_lo(wide(swapped))])
    back = hi_lo(wide(np.kron(c, c)))
    lane = np.arange(LANES)
    first = np.where(lane < plane, lane // n, 999)
    second = np.where(lane < plane, lane % n, 999)
    sign = lambda v: np.where(v % 2 == 0, 1.0, -1.0)
    lanes = np.stack(
        [first, second, sign(first), sign(second)] + [first * 0] * 4
    ).astype(np.float32)
    pick = np.zeros((plane, 2 * n))
    for j in range(n):
        pick[n * j, j] = 1.0
        pick[n * j + n - 1, n + j] = 1.0
    put = np.concatenate([pick.T, pick.T])
    return deriv, fwd, back, lanes, wide(pick, 128).astype(BF), wide(put).astype(BF), d


def split(value):
    hi = value.astype(BF)
    return hi, (value - hi.astype(F32)).astype(BF)


def dot(a, b):
    return jnp.dot(a, b, preferred_element_type=F32)


def fluxed(lhs, hi, lo):
    return dot(lhs[:, : 3 * ROWS], jnp.concatenate([hi, hi, lo], axis=0))


def far_terms(faces, far, oper, lift_lhs, plane):
    turned = []
    for f in faces:
        depth = plane if f else LANES
        one = far(f)[:, :depth]
        turned.append(dot(one, oper[f, 0, :depth]) + dot(one, oper[f, 1, :depth]))
    return [fluxed(lift_lhs[f], *split(t)) for f, t in zip(faces, turned)]


def body(
    n, diff, sizes,
    code_hbm, order_hbm, jac_hbm, fields_hbm, flux_hbm,
    deriv_hbm, fwd_hbm, back_hbm, lane_hbm, pick_hbm, put_hbm,
    out_ref, far_ref, oper, lift_lhs,
    code_ref, order_ref, jac_ref, fields_ref, flux_ref,
    deriv_ref, fwd_ref, back_ref, lane_ref, pick_ref, put_ref,
    xs, xl, gx, gs, vol, own, remote, raw, mix, early,
    load_sem, send_sem, recv_sem, ack,
):
    width, points = fields_ref.shape
    plane = n * n
    last = n - 1
    blk, sub = lax.axis_index("blk"), lax.axis_index("sub")
    n_blk, n_sub = sizes
    across = [
        (lax.rem(blk + n_blk - 1, n_blk), sub),
        (lax.rem(blk + 1, n_blk), sub),
        (blk, lax.rem(sub + n_sub - 1, n_sub)),
        (blk, lax.rem(sub + 1, n_sub)),
    ]
    barrier = pltpu.get_barrier_semaphore()
    low = -(-plane // 128) * 128
    high = plane * last // 128 * 128
    piece = lambda a, b: (fields_hbm.at[:, 0, a:b], fields_ref.at[:, a:b])
    pairs = [
        piece(high, points), piece(0, low), piece(low, high),
        (pick_hbm, pick_ref), (fwd_hbm, fwd_ref), (lane_hbm, lane_ref), (back_hbm, back_ref),
        (flux_hbm, flux_ref), (deriv_hbm, deriv_ref), (put_hbm, put_ref),
        (jac_hbm, jac_ref), (code_hbm, code_ref), (order_hbm, order_ref),
    ]
    loads = [pltpu.make_async_copy(a, b, load_sem.at[i]) for i, (a, b) in enumerate(pairs)]
    loads[0].start()
    for face in ENTRY:
        pl.semaphore_signal(barrier, inc=1, device_id=across[face ^ 1], device_id_type=MESH)
    for load in loads[1:]:
        load.start()
    used = -(-width // 8) * 8
    far_ref[used:] = jnp.zeros((ROWS - used, LANES), BF)
    for face in range(1, 4):
        remote[face, used:] = jnp.zeros((ROWS - used, LANES), BF)
    copies = [
        pltpu.make_async_remote_copy(
            src_ref=own.at[face, 0:used],
            dst_ref=far_ref.at[0:used] if face == 1 else remote.at[face ^ 1, 0:used],
            send_sem=send_sem.at[face],
            recv_sem=recv_sem.at[face ^ 1],
            device_id=across[face],
            device_id_type=MESH,
        )
        for face in range(4)
    ]

    def padded(value):
        return jnp.pad(value, ((0, ROWS - value.shape[0]), (0, LANES - value.shape[1])))

    def slab(i):
        return padded(fields_ref[:, plane * i : plane * (i + 1)])

    lift = 0.5 * last * last * 0.5

    def traces():
        loads[1].wait()
        own[0] = slab(0).astype(BF)
        loads[2].wait()
        for face in (2, 3):
            at = (face - 2) * (plane - n)
            runs = [fields_ref[:, plane * i + at : plane * i + at + n] for i in range(n)]
            own[face] = padded(jnp.concatenate(runs, axis=1)).astype(BF)
        for i in range(n):
            xs[i], xl[i] = split(slab(i))
        loads[3].wait()
        stack = xs[...].reshape(n * ROWS, LANES)[:, :plane]
        ends = dot(stack, pick_ref[...]).reshape(n, ROWS, 128)
        for face in (4, 5):
            at = (face - 4) * n
            runs = [ends[i, :, at : at + n] for i in range(n)]
            own[face] = padded(jnp.concatenate(runs, axis=1)).astype(BF)

    def thirds(value):
        lane = lax.broadcasted_iota(jnp.int32, value.shape, value.ndim - 1)
        hi = value.astype(BF).astype(F32)
        return jnp.where(lane < 2 * ROWS, hi, value - hi).astype(BF)

    def thirds(value):
        hi = value.astype(BF).astype(F32)
        lane = lax.broadcasted_iota(jnp.int32, value.shape, value.ndim - 1)
        lows = (lane >= ROWS) & (lane < 2 * ROWS)
        return jnp.where(lows, value - hi, hi).astype(BF)

    def flux_matrices():
        for load in loads[4:]:
            load.wait()
        raw[...] = jnp.zeros_like(raw)
        for axis in range(3):
            scaled = flux_ref[axis] * (-TIME_STEP * jac_ref[0, axis])
            for k in range(3):
                raw[axis, 0:width, ROWS * k : ROWS * k + width] = scaled
        mix[...] = thirds(raw[...])
        row = lax.broadcasted_iota(jnp.int32, (ROWS, LANES), 0)
        lane = lax.broadcasted_iota(jnp.int32, (ROWS, LANES), 1)
        diagonal = (jnp.bitwise_and(lane, ROWS - 1) == row) & (lane < 3 * ROWS)
        for face in range(6):
            side = lift if face % 2 else -lift
            keep = lift * TIME_STEP * jac_ref[0, face // 2]
            lift_lhs[face] = thirds(raw[face // 2] * side + jnp.where(diagonal, keep, 0.0))

    def volume_flux():
        for i in range(n):
            mixed = fluxed(mix[...].reshape(3 * ROWS, LANES), xs[i], xl[i])
            gx[i] = mixed[:ROWS]
            for axis in range(2):
                part = mixed[ROWS * (axis + 1) : ROWS * (axis + 2)]
                gs[axis, 0, i], gs[axis, 1, i] = split(part)

    def face_facts(face):
        first, second = lane_ref[0:1, :], lane_ref[1:2, :]
        ones = jnp.ones((1, LANES), F32)
        code = code_ref[0, face]
        order = order_ref[0, face].astype(F32)
        swap = jnp.where(code >= 4, 1, 0)
        rev_a = lax.rem(lax.div(code, 2), 2)
        rev_b = lax.rem(code, 2)
        use_first = jnp.where(swap == 1, rev_b, rev_a) == 1
        use_second = jnp.where(swap == 1, rev_a, rev_b) == 1
        sign = jnp.where(use_first, lane_ref[2:3, :], ones) * jnp.where(
            use_second, lane_ref[3:4, :], ones
        )
        keep = jnp.where((first < order) & (second < order), 1.0, 0.0)
        return swap, sign, keep

    def own_faces():
        rest_flat = own[2:].reshape(4 * ROWS, LANES)
        own_flat = jnp.concatenate([xs[0], xs[last], rest_flat], axis=0)[:, :plane]
        own_modes = (dot(own_flat, fwd_ref[0, 0]) + dot(own_flat, fwd_ref[0, 1])).reshape(
            6, ROWS, LANES
        )
        modes = []
        for face in range(6):
            swap, sign, keep = face_facts(face)
            if face < 4:
                modes.append(own_modes[face] * -keep)
            else:
                far = own[face ^ 1][:, :plane]
                turned = dot(far, fwd_ref[swap, 0]) + dot(far, fwd_ref[swap, 1])
                modes.append((turned * sign - own_modes[face]) * keep)
        modes_hi, modes_lo = split(jnp.concatenate(modes, axis=0))
        modes_hi, modes_lo = modes_hi[:, :plane], modes_lo[:, :plane]
        jump = dot(modes_hi, back_ref[0]) + dot(modes_lo, back_ref[0]) + dot(modes_hi, back_ref[1])
        jump_hi, jump_lo = split(jump)
        cut = lambda a, f: a[ROWS * f : ROWS * (f + 1)]
        for face in range(6):
            early[face] = fluxed(lift_lhs[face], cut(jump_hi, face), cut(jump_lo, face))

    def answer(face):
        pl.semaphore_wait(ack.at[face], 1)
        copies[face].start()

    def when(condition, *steps):
        @pl.when(condition)
        def _():
            for step in steps:
                step()

    odd = lax.rem(sub, 2) == 1
    corner = (blk == 0) & (sub < 2)
    even = jnp.logical_not(odd)
    rest = jnp.logical_not(corner)
    y_first = odd | (blk == 0)
    before = odd | (blk != n_blk - 1)
    inner = (blk != 0) & (sub != 0)

    loads[0].wait()
    offset = plane * last - high
    tail = points - high - LANES
    lane = lax.broadcasted_iota(jnp.int32, (width, 128), 1)
    ahead = jnp.pad(fields_ref[:, high + LANES :], ((0, 0), (0, 128 - tail)))
    merged = jnp.where(lane < tail, ahead, fields_ref[:, high : high + 128])
    turned = jnp.concatenate([merged, fields_ref[:, high + 128 : high + LANES]], axis=1)
    own[1] = padded(turned).astype(BF)
    when(before, traces)
    when(corner, flux_matrices, volume_flux)
    pl.semaphore_wait(barrier, 2)
    when(even | corner, copies[1].start)
    for face in ENTRY:
        pl.semaphore_signal(ack.at[face ^ 1], inc=1, device_id=across[face], device_id_type=MESH)
    when(jnp.logical_not(before), traces)
    copies[3].start()
    when(rest & y_first, lambda: answer(2))
    when(rest & jnp.logical_not(y_first), lambda: answer(0))
    when(rest, flux_matrices)
    when(odd & rest, copies[1].start)
    when(rest, volume_flux)
    when(inner & odd, lambda: answer(0))
    when(inner & even, lambda: answer(2))
    own_faces()
    when((blk != 0) & (sub == 0), lambda: answer(2))

    for face in range(4):
        swap, sign, keep = face_facts(face)
        scale = sign * keep
        f_hi = (fwd_ref[swap, 0].astype(F32) * scale).astype(BF)[:, :plane]
        f_lo = (fwd_ref[swap, 1].astype(F32) * scale).astype(BF)[:, :plane]
        whole = dot(f_hi, back_ref[0]) + dot(f_lo, back_ref[0]) + dot(f_hi, back_ref[1])
        if face == 1:
            whole = pltpu.roll(whole, offset, 1)
        zeros = jnp.zeros((LANES - plane, LANES), F32)
        if face == 0:
            head = plane - tail
            whole = jnp.concatenate([whole[head:], zeros, whole[:head]], axis=0)
        else:
            whole = jnp.concatenate([whole, zeros], axis=0)
        oper[face, 0], oper[face, 1] = split(whole)

    when(rest & even & (blk == 0), lambda: answer(0))

    runs = []
    for i in range(n):
        both = jnp.concatenate([early[f, :, n * i : n * (i + 1)] for f in (4, 5)], axis=1)
        hi = both.astype(BF).astype(F32)
        runs.append(jnp.concatenate([hi, both - hi], axis=1).astype(BF))
    total = dot(jnp.concatenate(runs, axis=0), put_ref[...])
    for axis in range(2):
        hi = gs[axis, 0].reshape(n * ROWS, LANES)[:, :plane]
        lo = gs[axis, 1].reshape(n * ROWS, LANES)[:, :plane]
        total = total + dot(hi, deriv_ref[axis, 0])
        total = total + dot(lo, deriv_ref[axis, 0])
        total = total + dot(hi, deriv_ref[axis, 1])
    vol[...] = total.reshape(n, ROWS, LANES)
    when(corner, lambda: answer(2))
    when(rest & odd & (blk == 0), lambda: answer(0))

    half = n // 2
    for r in range(0, -(-width // 8) * 8, 8):
        for c in range(0, LANES, 128):
            at = (slice(r, r + 8), slice(c, c + 128))
            plus, minus = [], []
            for a in range(half):
                one, two = gx[(a,) + at], gx[(last - a,) + at]
                plus.append(one + two)
                minus.append(one - two)
            middle = gx[(half,) + at]
            for i in range(half):
                even = minus[0] * float(0.5 * (diff[i, 0] - diff[i, last]))
                uneven = middle * float(diff[i, half])
                for a in range(half):
                    uneven = uneven + plus[a] * float(0.5 * (diff[i, a] + diff[i, last - a]))
                    if a:
                        even = even + minus[a] * float(0.5 * (diff[i, a] - diff[i, last - a]))
                vol[(i,) + at] += even + uneven
                vol[(last - i,) + at] += even - uneven
            even = minus[0] * float(diff[half, 0])
            for a in range(1, half):
                even = even + minus[a] * float(diff[half, a])
            vol[(half,) + at] += even
    for i in range(n):
        value = vol[i]
        if i == 0:
            value = value + early[0]
        if i == last:
            value = value + early[1]
        out_ref[:, plane * i : plane * (i + 1)] = value[:width, :plane]
    when(corner, lambda: answer(0))

    def arrived(*faces):
        for face in faces:
            copies[face ^ 1].wait_recv()
        terms = far_terms(faces, lambda f: remote[f], oper, lift_lhs, plane)
        for face, part in zip(faces, terms):
            if face == 1:
                part = part[:width]
                begun = jnp.where(lane >= offset, part[:, :128], 0.0)
                out_ref[:, high : high + 128] += begun
                out_ref[:, high + 128 : high + LANES] += part[:, 128:]
                out_ref[:, high + LANES :] += part[:, :tail]
                continue
            total = (part + early[face])[:width]
            at = (face - 2) * (plane - n)
            for i in range(n):
                out_ref[:, plane * i + at : plane * i + at + n] += total[:, n * i : n * (i + 1)]

    arrived(2, 3)
    arrived(1)
    copies[1].wait_recv()
    for copy in copies:
        copy.wait_send()


def finish(n, part_ref, far_ref, oper, lift_lhs, out_ref, low_ref, sem):
    width, points = part_ref.shape
    low = low_ref.shape[1]
    write = lambda a, i, start, stop: pltpu.make_async_copy(
        a, out_ref.at[:, 0, start:stop], sem.at[i]
    )
    inner = write(part_ref.at[:, low:], 0, low, points)
    inner.start()
    (term,) = far_terms((0,), lambda f: far_ref[...], oper, lift_lhs, n * n)
    low_ref[...] = part_ref[:, :low] + term[:width, :low]
    outer = write(low_ref, 1, 0, low)
    outer.start()
    inner.wait()
    outer.wait()


def solution(mesh):
    sizes = (mesh.shape["blk"], mesh.shape["sub"])

    def on_device(fields, flux_matrix, inv_jacobian, neighbour, orientation, face_order):
        width, points = fields.shape[1:]
        n = round(points ** (1.0 / 3.0))
        plane = n * n
        *constants, diff = tables(n)
        rows = jnp.transpose(fields, (1, 0, 2))
        hbm = pl.BlockSpec(memory_space=pltpu.HBM)
        operands = [orientation, face_order, inv_jacobian, rows, flux_matrix]
        operands += [jnp.asarray(a) for a in constants]
        vmem = lambda a: pltpu.VMEM(a.shape, a.dtype)
        vmem_spec = pl.BlockSpec(memory_space=pltpu.VMEM)

        def scoped(*refs):
            pl.run_scoped(
                functools.partial(body, n, diff, sizes, *refs),
                pltpu.SemaphoreType.DMA((13,)),
                pltpu.SemaphoreType.DMA((4,)),
                pltpu.SemaphoreType.DMA((4,)),
                pltpu.SemaphoreType.REGULAR((4,)),
            )

        parts = pl.pallas_call(
            scoped,
            out_shape=(
                pltpu.VMEM((width, points), F32),
                pltpu.VMEM((ROWS, LANES), BF),
                pltpu.VMEM((4, 2, LANES, LANES), BF),
                pltpu.VMEM((6, ROWS, LANES), BF),
            ),
            in_specs=[hbm] * len(operands),
            out_specs=[vmem_spec] * 4,
            scratch_shapes=[pltpu.SMEM(a.shape, a.dtype) for a in operands[:3]]
            + [pltpu.VMEM((width, points), F32)]
            + [vmem(a) for a in operands[4:]]
            + [
                pltpu.VMEM((n, ROWS, LANES), BF),
                pltpu.VMEM((n, ROWS, LANES), BF),
                pltpu.VMEM((n, ROWS, LANES), F32),
                pltpu.VMEM((2, 2, n, ROWS, LANES), BF),
                pltpu.VMEM((n, ROWS, LANES), F32),
                pltpu.VMEM((6, ROWS, LANES), BF),
                pltpu.VMEM((4, ROWS, LANES), BF),
                pltpu.VMEM((3, ROWS, LANES), F32),
                pltpu.VMEM((3, ROWS, LANES), BF),
                pltpu.VMEM((6, ROWS, LANES), F32),
            ],
            compiler_params=pltpu.CompilerParams(
                collective_id=0, has_side_effects=True, vmem_limit_bytes=48 * 1024 * 1024
            ),
        )(*[pltpu.with_memory_space_constraint(a, pltpu.HBM) for a in operands])
        low = -(-plane // 128) * 128
        out = pl.pallas_call(
            lambda *refs: pl.run_scoped(
                functools.partial(finish, n, *refs), pltpu.SemaphoreType.DMA((2,))
            ),
            out_shape=jax.ShapeDtypeStruct(rows.shape, F32),
            in_specs=[vmem_spec] * 4,
            out_specs=hbm,
            scratch_shapes=[
                pltpu.VMEM((width, low), F32),
            ],
            compiler_params=pltpu.CompilerParams(vmem_limit_bytes=16 * 1024 * 1024),
        )(*parts)
        return jnp.transpose(out, (1, 0, 2))

    return jax.shard_map(
        on_device,
        mesh=mesh,
        in_specs=(
            P(("blk", "sub"), None, None),
            P(),
            P(("blk", "sub"), None),
            P(("blk", "sub"), None),
            P(("blk", "sub"), None),
            P(("blk", "sub"), None),
        ),
        out_specs=P(("blk", "sub"), None, None),
        check_vma=False,
    )
```

```python
import functools

import jax
import jax.numpy as jnp
import numpy as np
from jax import lax
from jax.experimental import pallas as pl
from jax.experimental.pallas import tpu as pltpu
from jax.sharding import PartitionSpec as P

MESH = pl.DeviceIdType.MESH
BF = jnp.bfloat16
F32 = jnp.float32
ROWS = 64
LANES = 256
TIME_STEP = 0.01
ENTRY = (1, 3)


def cheb_np(n):
    idx = np.arange(n)
    x = -np.cos(np.pi * idx / (n - 1))
    c = np.where((idx == 0) | (idx == n - 1), 2.0, 1.0) * np.where(idx % 2 == 0, 1.0, -1.0)
    eye = np.eye(n)
    off = c[:, None] / c[None, :] / (x[:, None] - x[None, :] + eye) * (1.0 - eye)
    return off - np.diag(off.sum(axis=1))


def dct_np(n):
    k = np.arange(n)[:, None]
    j = np.arange(n)[None, :]
    basis = np.cos(np.pi * k * (j + 0.5) / n) * np.sqrt(2.0 / n)
    return basis * np.where(k == 0, np.sqrt(0.5), 1.0)


def hi_lo(matrix):
    full = matrix.astype(np.float32)
    hi = full.astype(BF)
    lo = (full - hi.astype(np.float32)).astype(BF)
    return np.stack([hi, lo])


def wide(matrix, lanes=LANES):
    return np.pad(matrix, ((0, 0), (0, lanes - matrix.shape[1])))


def tables(n):
    plane = n * n
    d = cheb_np(n)
    c = dct_np(n)
    eye = np.eye(n)
    deriv = np.stack([hi_lo(wide(np.kron(d.T, eye))), hi_lo(wide(np.kron(eye, d.T)))])
    forward = np.kron(c.T, c.T)
    swapped = forward.reshape(plane, n, n).transpose(0, 2, 1).reshape(plane, plane)
    fwd = np.stack([hi_lo(wide(forward)), hi_lo(wide(swapped))])
    back = hi_lo(wide(np.kron(c, c)))
    lane = np.arange(LANES)
    first = np.where(lane < plane, lane // n, 999)
    second = np.where(lane < plane, lane % n, 999)
    sign = lambda v: np.where(v % 2 == 0, 1.0, -1.0)
    lanes = np.stack(
        [first, second, sign(first), sign(second)] + [first * 0] * 4
    ).astype(np.float32)
    pick = np.zeros((plane, 2 * n))
    for j in range(n):
        pick[n * j, j] = 1.0
        pick[n * j + n - 1, n + j] = 1.0
    put = np.concatenate([pick.T, pick.T])
    return deriv, fwd, back, lanes, wide(pick, 128).astype(BF), wide(put).astype(BF), d


def split(value):
    hi = value.astype(BF)
    return hi, (value - hi.astype(F32)).astype(BF)


def dot(a, b):
    return jnp.dot(a, b, preferred_element_type=F32)


def fluxed(lhs, hi, lo):
    return dot(lhs[:, : 3 * ROWS], jnp.concatenate([hi, hi, lo], axis=0))


def far_terms(faces, far, oper, lift_lhs, plane):
    turned = []
    for f in faces:
        depth = plane if f else LANES
        one = far(f)[:, :depth]
        turned.append(dot(one, oper[f, 0, :depth]) + dot(one, oper[f, 1, :depth]))
    return [fluxed(lift_lhs[f], *split(t)) for f, t in zip(faces, turned)]


def body(
    n, diff, sizes,
    code_hbm, order_hbm, jac_hbm, fields_hbm, flux_hbm,
    deriv_hbm, fwd_hbm, back_hbm, lane_hbm, pick_hbm, put_hbm,
    out_ref, far_ref, oper, lift_lhs,
    code_ref, order_ref, jac_ref, fields_ref, flux_ref,
    deriv_ref, fwd_ref, back_ref, lane_ref, pick_ref, put_ref,
    xs, xl, gx, gs, vol, own, remote, raw, mix, early,
    load_sem, send_sem, recv_sem, ack,
):
    width, points = fields_ref.shape
    plane = n * n
    last = n - 1
    blk, sub = lax.axis_index("blk"), lax.axis_index("sub")
    n_blk, n_sub = sizes
    across = [
        (lax.rem(blk + n_blk - 1, n_blk), sub),
        (lax.rem(blk + 1, n_blk), sub),
        (blk, lax.rem(sub + n_sub - 1, n_sub)),
        (blk, lax.rem(sub + 1, n_sub)),
    ]
    barrier = pltpu.get_barrier_semaphore()
    low = -(-plane // 128) * 128
    high = plane * last // 128 * 128
    piece = lambda a, b: (fields_hbm.at[:, 0, a:b], fields_ref.at[:, a:b])
    pairs = [
        piece(high, points), piece(0, low), piece(low, high),
        (pick_hbm, pick_ref), (fwd_hbm, fwd_ref), (lane_hbm, lane_ref), (back_hbm, back_ref),
        (flux_hbm, flux_ref), (deriv_hbm, deriv_ref), (put_hbm, put_ref),
        (jac_hbm, jac_ref), (code_hbm, code_ref), (order_hbm, order_ref),
    ]
    loads = [pltpu.make_async_copy(a, b, load_sem.at[i]) for i, (a, b) in enumerate(pairs)]
    loads[0].start()
    for face in ENTRY:
        pl.semaphore_signal(barrier, inc=1, device_id=across[face ^ 1], device_id_type=MESH)
    for load in loads[1:]:
        load.start()
    used = -(-width // 8) * 8
    far_ref[used:] = jnp.zeros((ROWS - used, LANES), BF)
    for face in range(1, 4):
        remote[face, used:] = jnp.zeros((ROWS - used, LANES), BF)
    copies = [
        pltpu.make_async_remote_copy(
            src_ref=own.at[face, 0:used],
            dst_ref=far_ref.at[0:used] if face == 1 else remote.at[face ^ 1, 0:used],
            send_sem=send_sem.at[face],
            recv_sem=recv_sem.at[face ^ 1],
            device_id=across[face],
            device_id_type=MESH,
        )
        for face in range(4)
    ]

    def padded(value):
        return jnp.pad(value, ((0, ROWS - value.shape[0]), (0, LANES - value.shape[1])))

    def slab(i):
        return padded(fields_ref[:, plane * i : plane * (i + 1)])

    lift = 0.5 * last * last * 0.5

    def traces():
        loads[1].wait()
        own[0] = slab(0).astype(BF)
        loads[2].wait()
        for face in (2, 3):
            at = (face - 2) * (plane - n)
            runs = [fields_ref[:, plane * i + at : plane * i + at + n] for i in range(n)]
            own[face] = padded(jnp.concatenate(runs, axis=1)).astype(BF)
        for i in range(n):
            xs[i], xl[i] = split(slab(i))
        loads[3].wait()
        stack = xs[...].reshape(n * ROWS, LANES)[:, :plane]
        ends = dot(stack, pick_ref[...]).reshape(n, ROWS, 128)
        for face in (4, 5):
            at = (face - 4) * n
            runs = [ends[i, :, at : at + n] for i in range(n)]
            own[face] = padded(jnp.concatenate(runs, axis=1)).astype(BF)

    def parts(value):
        hi = value.astype(BF).astype(F32)
        lane = lax.broadcasted_iota(jnp.int32, value.shape, value.ndim - 1)
        return jnp.where(jnp.bitwise_and(lane, ROWS) == 0, hi, value - hi).astype(BF)

    def flux_matrices():
        for load in loads[4:]:
            load.wait()
        raw[...] = jnp.zeros_like(raw)
        for axis in range(3):
            scaled = flux_ref[axis] * (-TIME_STEP * jac_ref[0, axis])
            for k in range(LANES // ROWS):
                raw[axis, 0:width, ROWS * k : ROWS * k + width] = scaled
        mix[...] = parts(raw[...])
        row = lax.broadcasted_iota(jnp.int32, (ROWS, LANES), 0)
        lane = lax.broadcasted_iota(jnp.int32, (ROWS, LANES), 1)
        diagonal = jnp.bitwise_and(lane, ROWS - 1) == row
        for face in range(6):
            side = lift if face % 2 else -lift
            keep = lift * TIME_STEP * jac_ref[0, face // 2]
            lift_lhs[face] = parts(raw[face // 2] * side + jnp.where(diagonal, keep, 0.0))

    def volume_flux():
        for i in range(n):
            both = jnp.concatenate([xs[i], xs[i], xl[i], xl[i]], axis=0)
            mixed = dot(mix[...].reshape(3 * ROWS, LANES), both)
            gx[i] = mixed[:ROWS]
            for axis in range(2):
                part = mixed[ROWS * (axis + 1) : ROWS * (axis + 2)]
                gs[axis, 0, i], gs[axis, 1, i] = split(part)

    def face_facts(face):
        first, second = lane_ref[0:1, :], lane_ref[1:2, :]
        ones = jnp.ones((1, LANES), F32)
        code = code_ref[0, face]
        order = order_ref[0, face].astype(F32)
        swap = jnp.where(code >= 4, 1, 0)
        rev_a = lax.rem(lax.div(code, 2), 2)
        rev_b = lax.rem(code, 2)
        use_first = jnp.where(swap == 1, rev_b, rev_a) == 1
        use_second = jnp.where(swap == 1, rev_a, rev_b) == 1
        sign = jnp.where(use_first, lane_ref[2:3, :], ones) * jnp.where(
            use_second, lane_ref[3:4, :], ones
        )
        keep = jnp.where((first < order) & (second < order), 1.0, 0.0)
        return swap, sign, keep

    def own_faces():
        rest_flat = own[2:].reshape(4 * ROWS, LANES)
        own_flat = jnp.concatenate([xs[0], xs[last], rest_flat], axis=0)[:, :plane]
        own_modes = (dot(own_flat, fwd_ref[0, 0]) + dot(own_flat, fwd_ref[0, 1])).reshape(
            6, ROWS, LANES
        )
        modes = []
        for face in range(6):
            swap, sign, keep = face_facts(face)
            if face < 4:
                modes.append(own_modes[face] * -keep)
            else:
                far = own[face ^ 1][:, :plane]
                turned = dot(far, fwd_ref[swap, 0]) + dot(far, fwd_ref[swap, 1])
                modes.append((turned * sign - own_modes[face]) * keep)
        modes_hi, modes_lo = split(jnp.concatenate(modes, axis=0))
        modes_hi, modes_lo = modes_hi[:, :plane], modes_lo[:, :plane]
        jump = dot(modes_hi, back_ref[0]) + dot(modes_lo, back_ref[0]) + dot(modes_hi, back_ref[1])
        jump_hi, jump_lo = split(jump)
        cut = lambda a, f: a[ROWS * f : ROWS * (f + 1)]
        for face in range(6):
            early[face] = fluxed(lift_lhs[face], cut(jump_hi, face), cut(jump_lo, face))

    def answer(face):
        pl.semaphore_wait(ack.at[face], 1)
        copies[face].start()

    def when(condition, *steps):
        @pl.when(condition)
        def _():
            for step in steps:
                step()

    odd = lax.rem(sub, 2) == 1
    corner = (blk == 0) & (sub < 2)
    even = jnp.logical_not(odd)
    rest = jnp.logical_not(corner)
    y_first = odd | (blk == 0)
    before = odd | (blk != n_blk - 1)
    inner = (blk != 0) & (sub != 0)

    loads[0].wait()
    offset = plane * last - high
    tail = points - high - LANES
    lane = lax.broadcasted_iota(jnp.int32, (width, 128), 1)
    ahead = jnp.pad(fields_ref[:, high + LANES :], ((0, 0), (0, 128 - tail)))
    merged = jnp.where(lane < tail, ahead, fields_ref[:, high : high + 128])
    turned = jnp.concatenate([merged, fields_ref[:, high + 128 : high + LANES]], axis=1)
    own[1] = padded(turned).astype(BF)
    when(before, traces)
    when(corner, flux_matrices, volume_flux)
    pl.semaphore_wait(barrier, 2)
    when(even | corner, copies[1].start)
    for face in ENTRY:
        pl.semaphore_signal(ack.at[face ^ 1], inc=1, device_id=across[face], device_id_type=MESH)
    when(jnp.logical_not(before), traces)
    copies[3].start()
    when(rest & y_first, lambda: answer(2))
    when(rest & jnp.logical_not(y_first), lambda: answer(0))
    when(rest, flux_matrices)
    when(odd & rest, copies[1].start)
    when(rest, volume_flux)
    when(inner & odd, lambda: answer(0))
    when(inner & even, lambda: answer(2))
    own_faces()
    when((blk != 0) & (sub == 0), lambda: answer(2))

    for face in range(4):
        swap, sign, keep = face_facts(face)
        scale = sign * keep
        f_hi = (fwd_ref[swap, 0].astype(F32) * scale).astype(BF)[:, :plane]
        f_lo = (fwd_ref[swap, 1].astype(F32) * scale).astype(BF)[:, :plane]
        whole = dot(f_hi, back_ref[0]) + dot(f_lo, back_ref[0]) + dot(f_hi, back_ref[1])
        whole = whole + dot(f_lo, back_ref[1])
        if face == 1:
            whole = pltpu.roll(whole, offset, 1)
        zeros = jnp.zeros((LANES - plane, LANES), F32)
        if face == 0:
            head = plane - tail
            whole = jnp.concatenate([whole[head:], zeros, whole[:head]], axis=0)
        else:
            whole = jnp.concatenate([whole, zeros], axis=0)
        oper[face, 0], oper[face, 1] = split(whole)

    when(rest & (blk == 0), lambda: answer(0))

    runs = []
    for i in range(n):
        both = jnp.concatenate([early[f, :, n * i : n * (i + 1)] for f in (4, 5)], axis=1)
        hi = both.astype(BF).astype(F32)
        runs.append(jnp.concatenate([hi, both - hi], axis=1).astype(BF))
    total = dot(jnp.concatenate(runs, axis=0), put_ref[...])
    for axis in range(2):
        hi = gs[axis, 0].reshape(n * ROWS, LANES)[:, :plane]
        lo = gs[axis, 1].reshape(n * ROWS, LANES)[:, :plane]
        total = total + dot(hi, deriv_ref[axis, 0])
        total = total + dot(lo, deriv_ref[axis, 0])
        total = total + dot(hi, deriv_ref[axis, 1])
    vol[...] = total.reshape(n, ROWS, LANES)
    when(corner, lambda: answer(2))

    half = n // 2
    for r in range(0, -(-width // 8) * 8, 8):
        for c in range(0, LANES, 128):
            at = (slice(r, r + 8), slice(c, c + 128))
            plus, minus = [], []
            for a in range(half):
                one, two = gx[(a,) + at], gx[(last - a,) + at]
                plus.append(one + two)
                minus.append(one - two)
            middle = gx[(half,) + at]
            for i in range(half):
                even = minus[0] * float(0.5 * (diff[i, 0] - diff[i, last]))
                uneven = middle * float(diff[i, half])
                for a in range(half):
                    uneven = uneven + plus[a] * float(0.5 * (diff[i, a] + diff[i, last - a]))
                    if a:
                        even = even + minus[a] * float(0.5 * (diff[i, a] - diff[i, last - a]))
                vol[(i,) + at] += even + uneven
                vol[(last - i,) + at] += even - uneven
            even = minus[0] * float(diff[half, 0])
            for a in range(1, half):
                even = even + minus[a] * float(diff[half, a])
            vol[(half,) + at] += even
    for i in range(n):
        value = vol[i]
        if i == 0:
            value = value + early[0]
        if i == last:
            value = value + early[1]
        out_ref[:, plane * i : plane * (i + 1)] = value[:width, :plane]
    when(corner, lambda: answer(0))

    def arrived(*faces):
        for face in faces:
            copies[face ^ 1].wait_recv()
        terms = far_terms(faces, lambda f: remote[f], oper, lift_lhs, plane)
        for face, part in zip(faces, terms):
            if face == 1:
                part = part[:width]
                begun = jnp.where(lane >= offset, part[:, :128], 0.0)
                out_ref[:, high : high + 128] += begun
                out_ref[:, high + 128 : high + LANES] += part[:, 128:]
                out_ref[:, high + LANES :] += part[:, :tail]
                continue
            total = (part + early[face])[:width]
            at = (face - 2) * (plane - n)
            for i in range(n):
                out_ref[:, plane * i + at : plane * i + at + n] += total[:, n * i : n * (i + 1)]

    arrived(2, 3)
    arrived(1)
    copies[1].wait_recv()
    for copy in copies:
        copy.wait_send()


def finish(n, part_ref, far_ref, oper, lift_lhs, out_ref, low_ref, sem):
    width, points = part_ref.shape
    low = low_ref.shape[1]
    write = lambda a, i, start, stop: pltpu.make_async_copy(
        a, out_ref.at[:, 0, start:stop], sem.at[i]
    )
    inner = write(part_ref.at[:, low:], 0, low, points)
    inner.start()
    (term,) = far_terms((0,), lambda f: far_ref[...], oper, lift_lhs, n * n)
    low_ref[...] = part_ref[:, :low] + term[:width, :low]
    outer = write(low_ref, 1, 0, low)
    outer.start()
    inner.wait()
    outer.wait()


def solution(mesh):
    sizes = (mesh.shape["blk"], mesh.shape["sub"])

    def on_device(fields, flux_matrix, inv_jacobian, neighbour, orientation, face_order):
        width, points = fields.shape[1:]
        n = round(points ** (1.0 / 3.0))
        plane = n * n
        *constants, diff = tables(n)
        rows = jnp.transpose(fields, (1, 0, 2))
        hbm = pl.BlockSpec(memory_space=pltpu.HBM)
        operands = [orientation, face_order, inv_jacobian, rows, flux_matrix]
        operands += [jnp.asarray(a) for a in constants]
        vmem = lambda a: pltpu.VMEM(a.shape, a.dtype)
        vmem_spec = pl.BlockSpec(memory_space=pltpu.VMEM)

        def scoped(*refs):
            pl.run_scoped(
                functools.partial(body, n, diff, sizes, *refs),
                pltpu.SemaphoreType.DMA((13,)),
                pltpu.SemaphoreType.DMA((4,)),
                pltpu.SemaphoreType.DMA((4,)),
                pltpu.SemaphoreType.REGULAR((4,)),
            )

        parts = pl.pallas_call(
            scoped,
            out_shape=(
                pltpu.VMEM((width, points), F32),
                pltpu.VMEM((ROWS, LANES), BF),
                pltpu.VMEM((4, 2, LANES, LANES), BF),
                pltpu.VMEM((6, ROWS, LANES), BF),
            ),
            in_specs=[hbm] * len(operands),
            out_specs=[vmem_spec] * 4,
            scratch_shapes=[pltpu.SMEM(a.shape, a.dtype) for a in operands[:3]]
            + [pltpu.VMEM((width, points), F32)]
            + [vmem(a) for a in operands[4:]]
            + [
                pltpu.VMEM((n, ROWS, LANES), BF),
                pltpu.VMEM((n, ROWS, LANES), BF),
                pltpu.VMEM((n, ROWS, LANES), F32),
                pltpu.VMEM((2, 2, n, ROWS, LANES), BF),
                pltpu.VMEM((n, ROWS, LANES), F32),
                pltpu.VMEM((6, ROWS, LANES), BF),
                pltpu.VMEM((4, ROWS, LANES), BF),
                pltpu.VMEM((3, ROWS, LANES), F32),
                pltpu.VMEM((3, ROWS, LANES), BF),
                pltpu.VMEM((6, ROWS, LANES), F32),
            ],
            compiler_params=pltpu.CompilerParams(
                collective_id=0, has_side_effects=True, vmem_limit_bytes=48 * 1024 * 1024
            ),
        )(*[pltpu.with_memory_space_constraint(a, pltpu.HBM) for a in operands])
        low = -(-plane // 128) * 128
        out = pl.pallas_call(
            lambda *refs: pl.run_scoped(
                functools.partial(finish, n, *refs), pltpu.SemaphoreType.DMA((2,))
            ),
            out_shape=jax.ShapeDtypeStruct(rows.shape, F32),
            in_specs=[vmem_spec] * 4,
            out_specs=hbm,
            scratch_shapes=[
                pltpu.VMEM((width, low), F32),
            ],
            compiler_params=pltpu.CompilerParams(vmem_limit_bytes=16 * 1024 * 1024),
        )(*parts)
        return jnp.transpose(out, (1, 0, 2))

    return jax.shard_map(
        on_device,
        mesh=mesh,
        in_specs=(
            P(("blk", "sub"), None, None),
            P(),
            P(("blk", "sub"), None),
            P(("blk", "sub"), None),
            P(("blk", "sub"), None),
            P(("blk", "sub"), None),
        ),
        out_specs=P(("blk", "sub"), None, None),
        check_vma=False,
    )
```

```python
import functools

import jax
import jax.numpy as jnp
import numpy as np
from jax import lax
from jax.experimental import pallas as pl
from jax.experimental.pallas import tpu as pltpu
from jax.sharding import PartitionSpec as P

MESH = pl.DeviceIdType.MESH
BF = jnp.bfloat16
F32 = jnp.float32
ROWS = 64
LANES = 256
TIME_STEP = 0.01
ENTRY = (1, 3)
STRIP = 16


def cheb_np(n):
    idx = np.arange(n)
    x = -np.cos(np.pi * idx / (n - 1))
    c = np.where((idx == 0) | (idx == n - 1), 2.0, 1.0) * np.where(idx % 2 == 0, 1.0, -1.0)
    eye = np.eye(n)
    off = c[:, None] / c[None, :] / (x[:, None] - x[None, :] + eye) * (1.0 - eye)
    return off - np.diag(off.sum(axis=1))


def dct_np(n):
    k = np.arange(n)[:, None]
    j = np.arange(n)[None, :]
    basis = np.cos(np.pi * k * (j + 0.5) / n) * np.sqrt(2.0 / n)
    return basis * np.where(k == 0, np.sqrt(0.5), 1.0)


def hi_lo(matrix):
    full = matrix.astype(np.float32)
    hi = full.astype(BF)
    lo = (full - hi.astype(np.float32)).astype(BF)
    return np.stack([hi, lo])


def wide(matrix, lanes=LANES):
    return np.pad(matrix, ((0, 0), (0, lanes - matrix.shape[1])))


def tables(n):
    plane = n * n
    d = cheb_np(n)
    c = dct_np(n)
    eye = np.eye(n)
    deriv = np.stack([hi_lo(wide(np.kron(d.T, eye))), hi_lo(wide(np.kron(eye, d.T)))])
    forward = np.kron(c.T, c.T)
    swapped = forward.reshape(plane, n, n).transpose(0, 2, 1).reshape(plane, plane)
    fwd = np.stack([hi_lo(wide(forward)), hi_lo(wide(swapped))])
    back = hi_lo(wide(np.kron(c, c)))
    lane = np.arange(LANES)
    first = np.where(lane < plane, lane // n, 999)
    second = np.where(lane < plane, lane % n, 999)
    sign = lambda v: np.where(v % 2 == 0, 1.0, -1.0)
    lanes = np.stack(
        [first, second, sign(first), sign(second)] + [first * 0] * 4
    ).astype(np.float32)
    pick = np.zeros((plane, 2 * n))
    for j in range(n):
        pick[n * j, j] = 1.0
        pick[n * j + n - 1, n + j] = 1.0
    put = np.concatenate([pick.T, pick.T])
    return deriv, fwd, back, lanes, wide(pick, 128).astype(BF), wide(put).astype(BF), d


def split(value):
    hi = value.astype(BF)
    return hi, (value - hi.astype(F32)).astype(BF)


def dot(a, b):
    return jnp.dot(a, b, preferred_element_type=F32)


def fluxed(lhs, hi, lo):
    return dot(lhs[:, : 3 * ROWS], jnp.concatenate([hi, hi, lo], axis=0))


def far_terms(faces, far, oper, lift_lhs, plane):
    turned = []
    for f in faces:
        depth = plane if f else LANES
        one = far(f)[:, :depth]
        turned.append(dot(one, oper[f, 0, :depth]) + dot(one, oper[f, 1, :depth]))
    return [fluxed(lift_lhs[f], *split(t)) for f, t in zip(faces, turned)]


def body(
    n, diff, sizes,
    code_hbm, order_hbm, jac_hbm, fields_hbm, flux_hbm,
    deriv_hbm, fwd_hbm, back_hbm, lane_hbm, pick_hbm, put_hbm,
    out_ref, far_ref, oper, lift_lhs,
    code_ref, order_ref, jac_ref, fields_ref, flux_ref,
    deriv_ref, fwd_ref, back_ref, lane_ref, pick_ref, put_ref,
    xs, xl, gx, gs, vol, own, remote, raw, mix, early,
    load_sem, send_sem, recv_sem, ack,
):
    width, points = fields_ref.shape
    plane = n * n
    last = n - 1
    blk, sub = lax.axis_index("blk"), lax.axis_index("sub")
    n_blk, n_sub = sizes
    across = [
        (lax.rem(blk + n_blk - 1, n_blk), sub),
        (lax.rem(blk + 1, n_blk), sub),
        (blk, lax.rem(sub + n_sub - 1, n_sub)),
        (blk, lax.rem(sub + 1, n_sub)),
    ]
    barrier = pltpu.get_barrier_semaphore()
    low = -(-plane // 128) * 128
    high = plane * last // 128 * 128
    piece = lambda a, b: (fields_hbm.at[:, 0, a:b], fields_ref.at[:, a:b])
    pairs = [
        piece(0, low), piece(low, high),
        (pick_hbm, pick_ref), (fwd_hbm, fwd_ref), (lane_hbm, lane_ref), (back_hbm, back_ref),
        (flux_hbm, flux_ref), (deriv_hbm, deriv_ref), (put_hbm, put_ref),
        (jac_hbm, jac_ref), (code_hbm, code_ref), (order_hbm, order_ref),
    ]
    whole_loads = len(pairs)
    for r in range(0, width, STRIP):
        strip = slice(r, min(r + STRIP, width))
        pairs.append((fields_hbm.at[strip, 0, high:], fields_ref.at[strip, high:]))
    loads = [pltpu.make_async_copy(a, b, load_sem.at[i]) for i, (a, b) in enumerate(pairs)]
    for load in loads[whole_loads:]:
        load.start()
    for face in ENTRY:
        pl.semaphore_signal(barrier, inc=1, device_id=across[face ^ 1], device_id_type=MESH)
    for load in loads[:whole_loads]:
        load.start()
    used = -(-width // 8) * 8
    far_ref[used:] = jnp.zeros((ROWS - used, LANES), BF)
    for face in range(1, 4):
        remote[face, used:] = jnp.zeros((ROWS - used, LANES), BF)
    copies = [
        pltpu.make_async_remote_copy(
            src_ref=own.at[face, 0:used],
            dst_ref=far_ref.at[0:used] if face == 1 else remote.at[face ^ 1, 0:used],
            send_sem=send_sem.at[face],
            recv_sem=recv_sem.at[face ^ 1],
            device_id=across[face],
            device_id_type=MESH,
        )
        for face in range(4)
    ]

    def padded(value):
        return jnp.pad(value, ((0, ROWS - value.shape[0]), (0, LANES - value.shape[1])))

    def slab(i):
        return padded(fields_ref[:, plane * i : plane * (i + 1)])

    lift = 0.5 * last * last * 0.5

    def traces():
        loads[0].wait()
        own[0] = slab(0).astype(BF)
        loads[1].wait()
        for face in (2, 3):
            at = (face - 2) * (plane - n)
            runs = [fields_ref[:, plane * i + at : plane * i + at + n] for i in range(n)]
            own[face] = padded(jnp.concatenate(runs, axis=1)).astype(BF)
        for i in range(n):
            xs[i], xl[i] = split(slab(i))
        loads[2].wait()
        stack = xs[...].reshape(n * ROWS, LANES)[:, :plane]
        ends = dot(stack, pick_ref[...]).reshape(n, ROWS, 128)
        for face in (4, 5):
            at = (face - 4) * n
            runs = [ends[i, :, at : at + n] for i in range(n)]
            own[face] = padded(jnp.concatenate(runs, axis=1)).astype(BF)

    def parts(value):
        hi = value.astype(BF).astype(F32)
        lane = lax.broadcasted_iota(jnp.int32, value.shape, value.ndim - 1)
        return jnp.where(jnp.bitwise_and(lane, ROWS) == 0, hi, value - hi).astype(BF)

    def flux_matrices():
        for load in loads[3:whole_loads]:
            load.wait()
        raw[...] = jnp.zeros_like(raw)
        for axis in range(3):
            scaled = flux_ref[axis] * (-TIME_STEP * jac_ref[0, axis])
            for k in range(LANES // ROWS):
                raw[axis, 0:width, ROWS * k : ROWS * k + width] = scaled
        mix[...] = parts(raw[...])
        row = lax.broadcasted_iota(jnp.int32, (ROWS, LANES), 0)
        lane = lax.broadcasted_iota(jnp.int32, (ROWS, LANES), 1)
        diagonal = jnp.bitwise_and(lane, ROWS - 1) == row
        for face in range(6):
            side = lift if face % 2 else -lift
            keep = lift * TIME_STEP * jac_ref[0, face // 2]
            lift_lhs[face] = parts(raw[face // 2] * side + jnp.where(diagonal, keep, 0.0))

    def volume_flux():
        for i in range(n):
            both = jnp.concatenate([xs[i], xs[i], xl[i], xl[i]], axis=0)
            mixed = dot(mix[...].reshape(3 * ROWS, LANES), both)
            gx[i] = mixed[:ROWS]
            for axis in range(2):
                part = mixed[ROWS * (axis + 1) : ROWS * (axis + 2)]
                gs[axis, 0, i], gs[axis, 1, i] = split(part)

    def face_facts(face):
        first, second = lane_ref[0:1, :], lane_ref[1:2, :]
        ones = jnp.ones((1, LANES), F32)
        code = code_ref[0, face]
        order = order_ref[0, face].astype(F32)
        swap = jnp.where(code >= 4, 1, 0)
        rev_a = lax.rem(lax.div(code, 2), 2)
        rev_b = lax.rem(code, 2)
        use_first = jnp.where(swap == 1, rev_b, rev_a) == 1
        use_second = jnp.where(swap == 1, rev_a, rev_b) == 1
        sign = jnp.where(use_first, lane_ref[2:3, :], ones) * jnp.where(
            use_second, lane_ref[3:4, :], ones
        )
        keep = jnp.where((first < order) & (second < order), 1.0, 0.0)
        return swap, sign, keep

    def own_faces():
        rest_flat = own[2:].reshape(4 * ROWS, LANES)
        own_flat = jnp.concatenate([xs[0], xs[last], rest_flat], axis=0)[:, :plane]
        own_modes = (dot(own_flat, fwd_ref[0, 0]) + dot(own_flat, fwd_ref[0, 1])).reshape(
            6, ROWS, LANES
        )
        modes = []
        for face in range(6):
            swap, sign, keep = face_facts(face)
            if face < 4:
                modes.append(own_modes[face] * -keep)
            else:
                far = own[face ^ 1][:, :plane]
                turned = dot(far, fwd_ref[swap, 0]) + dot(far, fwd_ref[swap, 1])
                modes.append((turned * sign - own_modes[face]) * keep)
        modes_hi, modes_lo = split(jnp.concatenate(modes, axis=0))
        modes_hi, modes_lo = modes_hi[:, :plane], modes_lo[:, :plane]
        jump = dot(modes_hi, back_ref[0]) + dot(modes_lo, back_ref[0]) + dot(modes_hi, back_ref[1])
        jump_hi, jump_lo = split(jump)
        cut = lambda a, f: a[ROWS * f : ROWS * (f + 1)]
        for face in range(6):
            early[face] = fluxed(lift_lhs[face], cut(jump_hi, face), cut(jump_lo, face))

    def answer(face):
        pl.semaphore_wait(ack.at[face], 1)
        copies[face].start()

    def when(condition, *steps):
        @pl.when(condition)
        def _():
            for step in steps:
                step()

    odd = lax.rem(sub, 2) == 1
    corner = (blk == 0) & (sub < 2)
    even = jnp.logical_not(odd)
    rest = jnp.logical_not(corner)
    y_first = odd | (blk == 0)
    before = odd | (blk != n_blk - 1)
    inner = (blk != 0) & (sub != 0)

    for load in loads[whole_loads:]:
        load.wait()
    offset = plane * last - high
    tail = points - high - LANES
    lane = lax.broadcasted_iota(jnp.int32, (width, 128), 1)
    ahead = jnp.pad(fields_ref[:, high + LANES :], ((0, 0), (0, 128 - tail)))
    merged = jnp.where(lane < tail, ahead, fields_ref[:, high : high + 128])
    turned = jnp.concatenate([merged, fields_ref[:, high + 128 : high + LANES]], axis=1)
    own[1] = padded(turned).astype(BF)
    when(before, traces)
    when(corner, flux_matrices, volume_flux)
    pl.semaphore_wait(barrier, 2)
    when(even | corner, copies[1].start)
    for face in ENTRY:
        pl.semaphore_signal(ack.at[face ^ 1], inc=1, device_id=across[face], device_id_type=MESH)
    when(jnp.logical_not(before), traces)
    copies[3].start()
    when(rest & y_first, lambda: answer(2))
    when(rest & jnp.logical_not(y_first), lambda: answer(0))
    when(rest, flux_matrices)
    when(odd & rest, copies[1].start)
    when(rest, volume_flux)
    when(inner & odd, lambda: answer(0))
    when(inner & even, lambda: answer(2))
    own_faces()
    when((blk != 0) & (sub == 0), lambda: answer(2))

    for face in range(4):
        swap, sign, keep = face_facts(face)
        scale = sign * keep
        f_hi = (fwd_ref[swap, 0].astype(F32) * scale).astype(BF)[:, :plane]
        f_lo = (fwd_ref[swap, 1].astype(F32) * scale).astype(BF)[:, :plane]
        whole = dot(f_hi, back_ref[0]) + dot(f_lo, back_ref[0]) + dot(f_hi, back_ref[1])
        whole = whole + dot(f_lo, back_ref[1])
        if face == 1:
            whole = pltpu.roll(whole, offset, 1)
        zeros = jnp.zeros((LANES - plane, LANES), F32)
        if face == 0:
            head = plane - tail
            whole = jnp.concatenate([whole[head:], zeros, whole[:head]], axis=0)
        else:
            whole = jnp.concatenate([whole, zeros], axis=0)
        oper[face, 0], oper[face, 1] = split(whole)

    when(rest & (blk == 0), lambda: answer(0))

    runs = []
    for i in range(n):
        both = jnp.concatenate([early[f, :, n * i : n * (i + 1)] for f in (4, 5)], axis=1)
        hi = both.astype(BF).astype(F32)
        runs.append(jnp.concatenate([hi, both - hi], axis=1).astype(BF))
    total = dot(jnp.concatenate(runs, axis=0), put_ref[...])
    for axis in range(2):
        hi = gs[axis, 0].reshape(n * ROWS, LANES)[:, :plane]
        lo = gs[axis, 1].reshape(n * ROWS, LANES)[:, :plane]
        total = total + dot(hi, deriv_ref[axis, 0])
        total = total + dot(lo, deriv_ref[axis, 0])
        total = total + dot(hi, deriv_ref[axis, 1])
    vol[...] = total.reshape(n, ROWS, LANES)
    when(corner, lambda: answer(2))

    half = n // 2
    for r in range(0, -(-width // 8) * 8, 8):
        for c in range(0, LANES, 128):
            at = (slice(r, r + 8), slice(c, c + 128))
            plus, minus = [], []
            for a in range(half):
                one, two = gx[(a,) + at], gx[(last - a,) + at]
                plus.append(one + two)
                minus.append(one - two)
            middle = gx[(half,) + at]
            for i in range(half):
                even = minus[0] * float(0.5 * (diff[i, 0] - diff[i, last]))
                uneven = middle * float(diff[i, half])
                for a in range(half):
                    uneven = uneven + plus[a] * float(0.5 * (diff[i, a] + diff[i, last - a]))
                    if a:
                        even = even + minus[a] * float(0.5 * (diff[i, a] - diff[i, last - a]))
                vol[(i,) + at] += even + uneven
                vol[(last - i,) + at] += even - uneven
            even = minus[0] * float(diff[half, 0])
            for a in range(1, half):
                even = even + minus[a] * float(diff[half, a])
            vol[(half,) + at] += even
    for i in range(n):
        value = vol[i]
        if i == 0:
            value = value + early[0]
        if i == last:
            value = value + early[1]
        out_ref[:, plane * i : plane * (i + 1)] = value[:width, :plane]
    when(corner, lambda: answer(0))

    def arrived(*faces):
        for face in faces:
            copies[face ^ 1].wait_recv()
        terms = far_terms(faces, lambda f: remote[f], oper, lift_lhs, plane)
        for face, part in zip(faces, terms):
            if face == 1:
                part = part[:width]
                begun = jnp.where(lane >= offset, part[:, :128], 0.0)
                out_ref[:, high : high + 128] += begun
                out_ref[:, high + 128 : high + LANES] += part[:, 128:]
                out_ref[:, high + LANES :] += part[:, :tail]
                continue
            total = (part + early[face])[:width]
            at = (face - 2) * (plane - n)
            for i in range(n):
                out_ref[:, plane * i + at : plane * i + at + n] += total[:, n * i : n * (i + 1)]

    arrived(2, 3)
    arrived(1)
    copies[1].wait_recv()
    for copy in copies:
        copy.wait_send()


def finish(n, part_ref, far_ref, oper, lift_lhs, out_ref, low_ref, sem):
    width, points = part_ref.shape
    low = low_ref.shape[1]
    write = lambda a, i, start, stop: pltpu.make_async_copy(
        a, out_ref.at[:, 0, start:stop], sem.at[i]
    )
    inner = write(part_ref.at[:, low:], 0, low, points)
    inner.start()
    (term,) = far_terms((0,), lambda f: far_ref[...], oper, lift_lhs, n * n)
    low_ref[...] = part_ref[:, :low] + term[:width, :low]
    outer = write(low_ref, 1, 0, low)
    outer.start()
    inner.wait()
    outer.wait()


def solution(mesh):
    sizes = (mesh.shape["blk"], mesh.shape["sub"])

    def on_device(fields, flux_matrix, inv_jacobian, neighbour, orientation, face_order):
        width, points = fields.shape[1:]
        n = round(points ** (1.0 / 3.0))
        plane = n * n
        *constants, diff = tables(n)
        rows = jnp.transpose(fields, (1, 0, 2))
        hbm = pl.BlockSpec(memory_space=pltpu.HBM)
        operands = [orientation, face_order, inv_jacobian, rows, flux_matrix]
        operands += [jnp.asarray(a) for a in constants]
        vmem = lambda a: pltpu.VMEM(a.shape, a.dtype)
        vmem_spec = pl.BlockSpec(memory_space=pltpu.VMEM)

        def scoped(*refs):
            pl.run_scoped(
                functools.partial(body, n, diff, sizes, *refs),
                pltpu.SemaphoreType.DMA((len(operands) + 1 + -(-width // STRIP),)),
                pltpu.SemaphoreType.DMA((4,)),
                pltpu.SemaphoreType.DMA((4,)),
                pltpu.SemaphoreType.REGULAR((4,)),
            )

        parts = pl.pallas_call(
            scoped,
            out_shape=(
                pltpu.VMEM((width, points), F32),
                pltpu.VMEM((ROWS, LANES), BF),
                pltpu.VMEM((4, 2, LANES, LANES), BF),
                pltpu.VMEM((6, ROWS, LANES), BF),
            ),
            in_specs=[hbm] * len(operands),
            out_specs=[vmem_spec] * 4,
            scratch_shapes=[pltpu.SMEM(a.shape, a.dtype) for a in operands[:3]]
            + [pltpu.VMEM((width, points), F32)]
            + [vmem(a) for a in operands[4:]]
            + [
                pltpu.VMEM((n, ROWS, LANES), BF),
                pltpu.VMEM((n, ROWS, LANES), BF),
                pltpu.VMEM((n, ROWS, LANES), F32),
                pltpu.VMEM((2, 2, n, ROWS, LANES), BF),
                pltpu.VMEM((n, ROWS, LANES), F32),
                pltpu.VMEM((6, ROWS, LANES), BF),
                pltpu.VMEM((4, ROWS, LANES), BF),
                pltpu.VMEM((3, ROWS, LANES), F32),
                pltpu.VMEM((3, ROWS, LANES), BF),
                pltpu.VMEM((6, ROWS, LANES), F32),
            ],
            compiler_params=pltpu.CompilerParams(
                collective_id=0, has_side_effects=True, vmem_limit_bytes=48 * 1024 * 1024
            ),
        )(*[pltpu.with_memory_space_constraint(a, pltpu.HBM) for a in operands])
        low = -(-plane // 128) * 128
        out = pl.pallas_call(
            lambda *refs: pl.run_scoped(
                functools.partial(finish, n, *refs), pltpu.SemaphoreType.DMA((2,))
            ),
            out_shape=jax.ShapeDtypeStruct(rows.shape, F32),
            in_specs=[vmem_spec] * 4,
            out_specs=hbm,
            scratch_shapes=[
                pltpu.VMEM((width, low), F32),
            ],
            compiler_params=pltpu.CompilerParams(vmem_limit_bytes=16 * 1024 * 1024),
        )(*parts)
        return jnp.transpose(out, (1, 0, 2))

    return jax.shard_map(
        on_device,
        mesh=mesh,
        in_specs=(
            P(("blk", "sub"), None, None),
            P(),
            P(("blk", "sub"), None),
            P(("blk", "sub"), None),
            P(("blk", "sub"), None),
            P(("blk", "sub"), None),
        ),
        out_specs=P(("blk", "sub"), None, None),
        check_vma=False,
    )
```

```python
import functools

import jax
import jax.numpy as jnp
import numpy as np
from jax import lax
from jax.experimental import pallas as pl
from jax.experimental.pallas import tpu as pltpu
from jax.sharding import PartitionSpec as P

MESH = pl.DeviceIdType.MESH
BF = jnp.bfloat16
F32 = jnp.float32
ROWS = 64
LANES = 256
TIME_STEP = 0.01
ENTRY = (1, 3)
STRIP = 16


def cheb_np(n):
    idx = np.arange(n)
    x = -np.cos(np.pi * idx / (n - 1))
    c = np.where((idx == 0) | (idx == n - 1), 2.0, 1.0) * np.where(idx % 2 == 0, 1.0, -1.0)
    eye = np.eye(n)
    off = c[:, None] / c[None, :] / (x[:, None] - x[None, :] + eye) * (1.0 - eye)
    return off - np.diag(off.sum(axis=1))


def dct_np(n):
    k = np.arange(n)[:, None]
    j = np.arange(n)[None, :]
    basis = np.cos(np.pi * k * (j + 0.5) / n) * np.sqrt(2.0 / n)
    return basis * np.where(k == 0, np.sqrt(0.5), 1.0)


def hi_lo(matrix):
    full = matrix.astype(np.float32)
    hi = full.astype(BF)
    lo = (full - hi.astype(np.float32)).astype(BF)
    return np.stack([hi, lo])


def wide(matrix, lanes=LANES):
    return np.pad(matrix, ((0, 0), (0, lanes - matrix.shape[1])))


def tables(n):
    plane = n * n
    d = cheb_np(n)
    c = dct_np(n)
    eye = np.eye(n)
    deriv = np.stack([hi_lo(wide(np.kron(d.T, eye))), hi_lo(wide(np.kron(eye, d.T)))])
    forward = np.kron(c.T, c.T)
    swapped = forward.reshape(plane, n, n).transpose(0, 2, 1).reshape(plane, plane)
    fwd = np.stack([hi_lo(wide(forward)), hi_lo(wide(swapped))])
    back = hi_lo(wide(np.kron(c, c)))
    lane = np.arange(LANES)
    first = np.where(lane < plane, lane // n, 999)
    second = np.where(lane < plane, lane % n, 999)
    sign = lambda v: np.where(v % 2 == 0, 1.0, -1.0)
    lanes = np.stack(
        [first, second, sign(first), sign(second)] + [first * 0] * 4
    ).astype(np.float32)
    pick = np.zeros((plane, 2 * n))
    for j in range(n):
        pick[n * j, j] = 1.0
        pick[n * j + n - 1, n + j] = 1.0
    put = np.concatenate([pick.T, pick.T])
    return deriv, fwd, back, lanes, wide(pick, 128).astype(BF), wide(put).astype(BF), d


def split(value):
    hi = value.astype(BF)
    return hi, (value - hi.astype(F32)).astype(BF)


def dot(a, b):
    return jnp.dot(a, b, preferred_element_type=F32)


def fluxed(lhs, hi, lo):
    return dot(lhs[:, : 3 * ROWS], jnp.concatenate([hi, hi, lo], axis=0))


def far_terms(faces, far, oper, lift_lhs, plane):
    turned = []
    for f in faces:
        depth = plane if f else LANES
        one = far(f)[:, :depth]
        turned.append(dot(one, oper[f, 0, :depth]) + dot(one, oper[f, 1, :depth]))
    return [fluxed(lift_lhs[f], *split(t)) for f, t in zip(faces, turned)]


def body(
    n, diff, sizes,
    code_hbm, order_hbm, jac_hbm, fields_hbm, flux_hbm,
    deriv_hbm, fwd_hbm, back_hbm, lane_hbm, pick_hbm, put_hbm,
    out_ref, far_ref, oper, lift_lhs,
    code_ref, order_ref, jac_ref, fields_ref, flux_ref,
    deriv_ref, fwd_ref, back_ref, lane_ref, pick_ref, put_ref,
    xs, xl, gx, gs, vol, own, remote, raw, mix, early,
    load_sem, send_sem, recv_sem, ack,
):
    width, points = fields_ref.shape
    plane = n * n
    last = n - 1
    blk, sub = lax.axis_index("blk"), lax.axis_index("sub")
    n_blk, n_sub = sizes
    across = [
        (lax.rem(blk + n_blk - 1, n_blk), sub),
        (lax.rem(blk + 1, n_blk), sub),
        (blk, lax.rem(sub + n_sub - 1, n_sub)),
        (blk, lax.rem(sub + 1, n_sub)),
    ]
    barrier = pltpu.get_barrier_semaphore()
    low = -(-plane // 128) * 128
    high = plane * last // 128 * 128
    piece = lambda a, b: (fields_hbm.at[:, 0, a:b], fields_ref.at[:, a:b])
    pairs = [
        piece(0, low), piece(low, high),
        (pick_hbm, pick_ref), (fwd_hbm, fwd_ref), (lane_hbm, lane_ref), (back_hbm, back_ref),
        (flux_hbm, flux_ref), (deriv_hbm, deriv_ref), (put_hbm, put_ref),
        (jac_hbm, jac_ref), (code_hbm, code_ref), (order_hbm, order_ref),
    ]
    whole_loads = len(pairs)
    for r in range(0, width, STRIP):
        strip = slice(r, min(r + STRIP, width))
        pairs.append((fields_hbm.at[strip, 0, high:], fields_ref.at[strip, high:]))
    loads = [pltpu.make_async_copy(a, b, load_sem.at[i]) for i, (a, b) in enumerate(pairs)]
    for load in loads[whole_loads:]:
        load.start()
    for face in ENTRY:
        pl.semaphore_signal(barrier, inc=1, device_id=across[face ^ 1], device_id_type=MESH)
    for load in loads[:whole_loads]:
        load.start()
    used = -(-width // 8) * 8
    far_ref[used:] = jnp.zeros((ROWS - used, LANES), BF)
    for face in range(1, 4):
        remote[face, used:] = jnp.zeros((ROWS - used, LANES), BF)
    copies = [
        pltpu.make_async_remote_copy(
            src_ref=own.at[face, 0:used],
            dst_ref=far_ref.at[0:used] if face == 1 else remote.at[face ^ 1, 0:used],
            send_sem=send_sem.at[face],
            recv_sem=recv_sem.at[face ^ 1],
            device_id=across[face],
            device_id_type=MESH,
        )
        for face in range(4)
    ]

    def padded(value):
        return jnp.pad(value, ((0, ROWS - value.shape[0]), (0, LANES - value.shape[1])))

    def slab(i):
        return padded(fields_ref[:, plane * i : plane * (i + 1)])

    lift = 0.5 * last * last * 0.5

    def traces():
        loads[0].wait()
        own[0] = slab(0).astype(BF)
        loads[1].wait()
        for face in (2, 3):
            at = (face - 2) * (plane - n)
            runs = [fields_ref[:, plane * i + at : plane * i + at + n] for i in range(n)]
            own[face] = padded(jnp.concatenate(runs, axis=1)).astype(BF)
        for i in range(n):
            xs[i], xl[i] = split(slab(i))
        loads[2].wait()
        stack = xs[...].reshape(n * ROWS, LANES)[:, :plane]
        ends = dot(stack, pick_ref[...]).reshape(n, ROWS, 128)
        for face in (4, 5):
            at = (face - 4) * n
            runs = [ends[i, :, at : at + n] for i in range(n)]
            own[face] = padded(jnp.concatenate(runs, axis=1)).astype(BF)

    def parts(value):
        hi = value.astype(BF).astype(F32)
        lane = lax.broadcasted_iota(jnp.int32, value.shape, value.ndim - 1)
        return jnp.where(jnp.bitwise_and(lane, ROWS) == 0, hi, value - hi).astype(BF)

    def flux_matrices():
        for load in loads[3:whole_loads]:
            load.wait()
        raw[...] = jnp.zeros_like(raw)
        for axis in range(3):
            scaled = flux_ref[axis] * (-TIME_STEP * jac_ref[0, axis])
            for k in range(LANES // ROWS):
                raw[axis, 0:width, ROWS * k : ROWS * k + width] = scaled
        mix[...] = parts(raw[...])
        row = lax.broadcasted_iota(jnp.int32, (ROWS, LANES), 0)
        lane = lax.broadcasted_iota(jnp.int32, (ROWS, LANES), 1)
        diagonal = jnp.bitwise_and(lane, ROWS - 1) == row
        for face in range(6):
            side = lift if face % 2 else -lift
            keep = lift * TIME_STEP * jac_ref[0, face // 2]
            lift_lhs[face] = parts(raw[face // 2] * side + jnp.where(diagonal, keep, 0.0))

    def volume_flux():
        for i in range(n):
            both = jnp.concatenate([xs[i], xs[i], xl[i], xl[i]], axis=0)
            mixed = dot(mix[...].reshape(3 * ROWS, LANES), both)
            gx[i] = mixed[:ROWS]
            for axis in range(2):
                part = mixed[ROWS * (axis + 1) : ROWS * (axis + 2)]
                gs[axis, 0, i], gs[axis, 1, i] = split(part)

    def face_facts(face):
        first, second = lane_ref[0:1, :], lane_ref[1:2, :]
        ones = jnp.ones((1, LANES), F32)
        code = code_ref[0, face]
        order = order_ref[0, face].astype(F32)
        swap = jnp.where(code >= 4, 1, 0)
        rev_a = lax.rem(lax.div(code, 2), 2)
        rev_b = lax.rem(code, 2)
        use_first = jnp.where(swap == 1, rev_b, rev_a) == 1
        use_second = jnp.where(swap == 1, rev_a, rev_b) == 1
        sign = jnp.where(use_first, lane_ref[2:3, :], ones) * jnp.where(
            use_second, lane_ref[3:4, :], ones
        )
        keep = jnp.where((first < order) & (second < order), 1.0, 0.0)
        return swap, sign, keep

    def own_faces():
        rest_flat = own[2:].reshape(4 * ROWS, LANES)
        own_flat = jnp.concatenate([xs[0], xs[last], rest_flat], axis=0)[:, :plane]
        own_modes = (dot(own_flat, fwd_ref[0, 0]) + dot(own_flat, fwd_ref[0, 1])).reshape(
            6, ROWS, LANES
        )
        modes = []
        for face in range(6):
            swap, sign, keep = face_facts(face)
            if face < 4:
                modes.append(own_modes[face] * -keep)
            else:
                far = own[face ^ 1][:, :plane]
                turned = dot(far, fwd_ref[swap, 0]) + dot(far, fwd_ref[swap, 1])
                modes.append((turned * sign - own_modes[face]) * keep)
        modes_hi, modes_lo = split(jnp.concatenate(modes, axis=0))
        modes_hi, modes_lo = modes_hi[:, :plane], modes_lo[:, :plane]
        jump = dot(modes_hi, back_ref[0]) + dot(modes_lo, back_ref[0]) + dot(modes_hi, back_ref[1])
        jump_hi, jump_lo = split(jump)
        cut = lambda a, f: a[ROWS * f : ROWS * (f + 1)]
        for face in range(6):
            early[face] = fluxed(lift_lhs[face], cut(jump_hi, face), cut(jump_lo, face))

    def answer(face):
        pl.semaphore_wait(ack.at[face], 1)
        copies[face].start()

    def when(condition, *steps):
        @pl.when(condition)
        def _():
            for step in steps:
                step()

    odd = lax.rem(sub, 2) == 1
    corner = (blk == 0) & (sub < 2)
    even = jnp.logical_not(odd)
    rest = jnp.logical_not(corner)
    y_first = odd | (blk == 0)
    before = odd | (blk != n_blk - 1)
    inner = (blk != 0) & (sub != 0)

    for load in loads[whole_loads:]:
        load.wait()
    offset = plane * last - high
    tail = points - high - LANES
    lane = lax.broadcasted_iota(jnp.int32, (width, 128), 1)
    ahead = jnp.pad(fields_ref[:, high + LANES :], ((0, 0), (0, 128 - tail)))
    merged = jnp.where(lane < tail, ahead, fields_ref[:, high : high + 128])
    turned = jnp.concatenate([merged, fields_ref[:, high + 128 : high + LANES]], axis=1)
    own[1] = padded(turned).astype(BF)
    when(before, traces)
    when(corner, flux_matrices, volume_flux)
    pl.semaphore_wait(barrier, 2)
    when(even | corner, copies[1].start)
    for face in ENTRY:
        pl.semaphore_signal(ack.at[face ^ 1], inc=1, device_id=across[face], device_id_type=MESH)
    when(jnp.logical_not(before), traces)
    copies[3].start()
    when(rest & y_first, lambda: answer(2))
    when(rest & jnp.logical_not(y_first), lambda: answer(0))
    when(rest, flux_matrices)
    when(odd & rest, copies[1].start)
    when(rest, volume_flux)
    when(inner & odd, lambda: answer(0))
    when(inner & even, lambda: answer(2))
    own_faces()
    when((blk != 0) & (sub == 0), lambda: answer(2))

    for face in range(4):
        swap, sign, keep = face_facts(face)
        scale = sign * keep
        f_hi = (fwd_ref[swap, 0].astype(F32) * scale).astype(BF)[:, :plane]
        f_lo = (fwd_ref[swap, 1].astype(F32) * scale).astype(BF)[:, :plane]
        whole = dot(f_hi, back_ref[0]) + dot(f_lo, back_ref[0]) + dot(f_hi, back_ref[1])
        whole = whole + dot(f_lo, back_ref[1])
        if face == 1:
            whole = pltpu.roll(whole, offset, 1)
        zeros = jnp.zeros((LANES - plane, LANES), F32)
        if face == 0:
            head = plane - tail
            whole = jnp.concatenate([whole[head:], zeros, whole[:head]], axis=0)
        else:
            whole = jnp.concatenate([whole, zeros], axis=0)
        oper[face, 0], oper[face, 1] = split(whole)

    when(rest & (blk == 0), lambda: answer(0))

    runs = []
    for i in range(n):
        both = jnp.concatenate([early[f, :, n * i : n * (i + 1)] for f in (4, 5)], axis=1)
        hi = both.astype(BF).astype(F32)
        runs.append(jnp.concatenate([hi, both - hi], axis=1).astype(BF))
    total = dot(jnp.concatenate(runs, axis=0), put_ref[...])
    for axis in range(2):
        hi = gs[axis, 0].reshape(n * ROWS, LANES)[:, :plane]
        lo = gs[axis, 1].reshape(n * ROWS, LANES)[:, :plane]
        total = total + dot(hi, deriv_ref[axis, 0])
        total = total + dot(lo, deriv_ref[axis, 0])
        total = total + dot(hi, deriv_ref[axis, 1])
    vol[...] = total.reshape(n, ROWS, LANES)
    when(corner, lambda: answer(2))

    half = n // 2
    for r in range(0, -(-width // 8) * 8, 8):
        for c in range(0, LANES, 128):
            at = (slice(r, r + 8), slice(c, c + 128))
            plus, minus = [], []
            for a in range(half):
                one, two = gx[(a,) + at], gx[(last - a,) + at]
                plus.append(one + two)
                minus.append(one - two)
            middle = gx[(half,) + at]
            for i in range(half):
                even = minus[0] * float(0.5 * (diff[i, 0] - diff[i, last]))
                uneven = middle * float(diff[i, half])
                for a in range(half):
                    uneven = uneven + plus[a] * float(0.5 * (diff[i, a] + diff[i, last - a]))
                    if a:
                        even = even + minus[a] * float(0.5 * (diff[i, a] - diff[i, last - a]))
                vol[(i,) + at] += even + uneven
                vol[(last - i,) + at] += even - uneven
            even = minus[0] * float(diff[half, 0])
            for a in range(1, half):
                even = even + minus[a] * float(diff[half, a])
            vol[(half,) + at] += even
    for i in range(n):
        value = vol[i]
        if i == 0:
            value = value + early[0]
        if i == last:
            value = value + early[1]
        out_ref[:, plane * i : plane * (i + 1)] = value[:width, :plane]
    when(corner, lambda: answer(0))

    def arrived(*faces):
        for face in faces:
            copies[face ^ 1].wait_recv()
        terms = far_terms(faces, lambda f: remote[f], oper, lift_lhs, plane)
        for face, part in zip(faces, terms):
            if face == 1:
                part = part[:width]
                begun = jnp.where(lane >= offset, part[:, :128], 0.0)
                out_ref[:, high : high + 128] += begun
                out_ref[:, high + 128 : high + LANES] += part[:, 128:]
                out_ref[:, high + LANES :] += part[:, :tail]
                continue
            total = (part + early[face])[:width]
            at = (face - 2) * (plane - n)
            for i in range(n):
                out_ref[:, plane * i + at : plane * i + at + n] += total[:, n * i : n * (i + 1)]

    arrived(2, 3)
    arrived(1)
    copies[1].wait_recv()
    for copy in copies:
        copy.wait_send()


def finish(n, part_ref, far_ref, oper, lift_lhs, out_ref, low_ref, sem):
    width = part_ref.shape[0]
    low = low_ref.shape[1]
    writes = [pltpu.make_async_copy(part_ref.at[:, low:], out_ref.at[:, 0, low:], sem.at[0])]
    writes[0].start()
    (term,) = far_terms((0,), lambda f: far_ref[...], oper, lift_lhs, n * n)
    for i, r in enumerate(range(0, width, STRIP)):
        strip = slice(r, min(r + STRIP, width))
        low_ref[strip] = part_ref[strip, :low] + term[strip, :low]
        writes.append(
            pltpu.make_async_copy(low_ref.at[strip], out_ref.at[strip, 0, :low], sem.at[i + 1])
        )
        writes[-1].start()
    for copy in writes:
        copy.wait()


def solution(mesh):
    sizes = (mesh.shape["blk"], mesh.shape["sub"])

    def on_device(fields, flux_matrix, inv_jacobian, neighbour, orientation, face_order):
        width, points = fields.shape[1:]
        n = round(points ** (1.0 / 3.0))
        plane = n * n
        *constants, diff = tables(n)
        rows = jnp.transpose(fields, (1, 0, 2))
        hbm = pl.BlockSpec(memory_space=pltpu.HBM)
        operands = [orientation, face_order, inv_jacobian, rows, flux_matrix]
        operands += [jnp.asarray(a) for a in constants]
        vmem = lambda a: pltpu.VMEM(a.shape, a.dtype)
        vmem_spec = pl.BlockSpec(memory_space=pltpu.VMEM)

        def scoped(*refs):
            pl.run_scoped(
                functools.partial(body, n, diff, sizes, *refs),
                pltpu.SemaphoreType.DMA((len(operands) + 1 + -(-width // STRIP),)),
                pltpu.SemaphoreType.DMA((4,)),
                pltpu.SemaphoreType.DMA((4,)),
                pltpu.SemaphoreType.REGULAR((4,)),
            )

        parts = pl.pallas_call(
            scoped,
            out_shape=(
                pltpu.VMEM((width, points), F32),
                pltpu.VMEM((ROWS, LANES), BF),
                pltpu.VMEM((4, 2, LANES, LANES), BF),
                pltpu.VMEM((6, ROWS, LANES), BF),
            ),
            in_specs=[hbm] * len(operands),
            out_specs=[vmem_spec] * 4,
            scratch_shapes=[pltpu.SMEM(a.shape, a.dtype) for a in operands[:3]]
            + [pltpu.VMEM((width, points), F32)]
            + [vmem(a) for a in operands[4:]]
            + [
                pltpu.VMEM((n, ROWS, LANES), BF),
                pltpu.VMEM((n, ROWS, LANES), BF),
                pltpu.VMEM((n, ROWS, LANES), F32),
                pltpu.VMEM((2, 2, n, ROWS, LANES), BF),
                pltpu.VMEM((n, ROWS, LANES), F32),
                pltpu.VMEM((6, ROWS, LANES), BF),
                pltpu.VMEM((4, ROWS, LANES), BF),
                pltpu.VMEM((3, ROWS, LANES), F32),
                pltpu.VMEM((3, ROWS, LANES), BF),
                pltpu.VMEM((6, ROWS, LANES), F32),
            ],
            compiler_params=pltpu.CompilerParams(
                collective_id=0, has_side_effects=True, vmem_limit_bytes=48 * 1024 * 1024
            ),
        )(*[pltpu.with_memory_space_constraint(a, pltpu.HBM) for a in operands])
        low = -(-plane // 128) * 128
        out = pl.pallas_call(
            lambda *refs: pl.run_scoped(
                functools.partial(finish, n, *refs),
                pltpu.SemaphoreType.DMA((1 + -(-width // STRIP),)),
            ),
            out_shape=jax.ShapeDtypeStruct(rows.shape, F32),
            in_specs=[vmem_spec] * 4,
            out_specs=hbm,
            scratch_shapes=[
                pltpu.VMEM((width, low), F32),
            ],
            compiler_params=pltpu.CompilerParams(vmem_limit_bytes=16 * 1024 * 1024),
        )(*parts)
        return jnp.transpose(out, (1, 0, 2))

    return jax.shard_map(
        on_device,
        mesh=mesh,
        in_specs=(
            P(("blk", "sub"), None, None),
            P(),
            P(("blk", "sub"), None),
            P(("blk", "sub"), None),
            P(("blk", "sub"), None),
            P(("blk", "sub"), None),
        ),
        out_specs=P(("blk", "sub"), None, None),
        check_vma=False,
    )
```

```python
import functools

import jax
import jax.numpy as jnp
import numpy as np
from jax import lax
from jax.experimental import pallas as pl
from jax.experimental.pallas import tpu as pltpu
from jax.sharding import PartitionSpec as P

MESH = pl.DeviceIdType.MESH
BF = jnp.bfloat16
F32 = jnp.float32
ROWS = 64
LANES = 256
TIME_STEP = 0.01
ENTRY = (1, 3)
STRIP = 16


def cheb_np(n):
    idx = np.arange(n)
    x = -np.cos(np.pi * idx / (n - 1))
    c = np.where((idx == 0) | (idx == n - 1), 2.0, 1.0) * np.where(idx % 2 == 0, 1.0, -1.0)
    eye = np.eye(n)
    off = c[:, None] / c[None, :] / (x[:, None] - x[None, :] + eye) * (1.0 - eye)
    return off - np.diag(off.sum(axis=1))


def dct_np(n):
    k = np.arange(n)[:, None]
    j = np.arange(n)[None, :]
    basis = np.cos(np.pi * k * (j + 0.5) / n) * np.sqrt(2.0 / n)
    return basis * np.where(k == 0, np.sqrt(0.5), 1.0)


def hi_lo(matrix):
    full = matrix.astype(np.float32)
    hi = full.astype(BF)
    lo = (full - hi.astype(np.float32)).astype(BF)
    return np.stack([hi, lo])


def wide(matrix, lanes=LANES):
    return np.pad(matrix, ((0, 0), (0, lanes - matrix.shape[1])))


def tables(n):
    plane = n * n
    d = cheb_np(n)
    c = dct_np(n)
    eye = np.eye(n)
    deriv = np.stack([hi_lo(wide(np.kron(d.T, eye))), hi_lo(wide(np.kron(eye, d.T)))])
    forward = np.kron(c.T, c.T)
    swapped = forward.reshape(plane, n, n).transpose(0, 2, 1).reshape(plane, plane)
    fwd = np.stack([hi_lo(wide(forward)), hi_lo(wide(swapped))])
    back = hi_lo(wide(np.kron(c, c)))
    lane = np.arange(LANES)
    first = np.where(lane < plane, lane // n, 999)
    second = np.where(lane < plane, lane % n, 999)
    sign = lambda v: np.where(v % 2 == 0, 1.0, -1.0)
    lanes = np.stack(
        [first, second, sign(first), sign(second)] + [first * 0] * 4
    ).astype(np.float32)
    pick = np.zeros((plane, 2 * n))
    for j in range(n):
        pick[n * j, j] = 1.0
        pick[n * j + n - 1, n + j] = 1.0
    put = np.concatenate([pick.T, pick.T])
    return deriv, fwd, back, lanes, wide(pick, 128).astype(BF), wide(put).astype(BF), d


def split(value):
    hi = value.astype(BF)
    return hi, (value - hi.astype(F32)).astype(BF)


def dot(a, b):
    return jnp.dot(a, b, preferred_element_type=F32)


def fluxed(lhs, hi, lo):
    return dot(lhs[:, : 3 * ROWS], jnp.concatenate([hi, hi, lo], axis=0))


def far_terms(faces, far, oper, lift_lhs, plane):
    turned = []
    for f in faces:
        depth = plane if f else LANES
        one = far(f)[:, :depth]
        turned.append(dot(one, oper[f, 0, :depth]) + dot(one, oper[f, 1, :depth]))
    return [fluxed(lift_lhs[f], *split(t)) for f, t in zip(faces, turned)]


def body(
    n, diff, sizes,
    code_hbm, order_hbm, jac_hbm, fields_hbm, flux_hbm,
    deriv_hbm, fwd_hbm, back_hbm, lane_hbm, pick_hbm, put_hbm,
    out_ref, far_ref, oper, lift_lhs,
    code_ref, order_ref, jac_ref, fields_ref, flux_ref,
    deriv_ref, fwd_ref, back_ref, lane_ref, pick_ref, put_ref,
    xs, xl, gx, gs, vol, own, remote, raw, mix, early,
    load_sem, send_sem, recv_sem, ack,
):
    width, points = fields_ref.shape
    plane = n * n
    last = n - 1
    blk, sub = lax.axis_index("blk"), lax.axis_index("sub")
    n_blk, n_sub = sizes
    across = [
        (lax.rem(blk + n_blk - 1, n_blk), sub),
        (lax.rem(blk + 1, n_blk), sub),
        (blk, lax.rem(sub + n_sub - 1, n_sub)),
        (blk, lax.rem(sub + 1, n_sub)),
    ]
    barrier = pltpu.get_barrier_semaphore()
    low = -(-plane // 128) * 128
    high = plane * last // 128 * 128
    piece = lambda a, b: (fields_hbm.at[:, 0, a:b], fields_ref.at[:, a:b])
    pairs = [
        piece(0, low), piece(low, high),
        (pick_hbm, pick_ref), (fwd_hbm, fwd_ref), (lane_hbm, lane_ref), (back_hbm, back_ref),
        (flux_hbm, flux_ref), (deriv_hbm, deriv_ref), (put_hbm, put_ref),
        (jac_hbm, jac_ref), (code_hbm, code_ref), (order_hbm, order_ref),
    ]
    whole_loads = len(pairs)
    for r in range(0, width, STRIP):
        strip = slice(r, min(r + STRIP, width))
        pairs.append((fields_hbm.at[strip, 0, high:], fields_ref.at[strip, high:]))
    loads = [pltpu.make_async_copy(a, b, load_sem.at[i]) for i, (a, b) in enumerate(pairs)]
    for load in loads[whole_loads:]:
        load.start()
    for face in ENTRY:
        pl.semaphore_signal(barrier, inc=1, device_id=across[face ^ 1], device_id_type=MESH)
    for load in loads[:whole_loads]:
        load.start()
    used = -(-width // 8) * 8
    far_ref[used:] = jnp.zeros((ROWS - used, LANES), BF)
    for face in range(1, 4):
        remote[face, used:] = jnp.zeros((ROWS - used, LANES), BF)
    copies = [
        pltpu.make_async_remote_copy(
            src_ref=own.at[face, 0:used],
            dst_ref=far_ref.at[0:used] if face == 1 else remote.at[face ^ 1, 0:used],
            send_sem=send_sem.at[face],
            recv_sem=recv_sem.at[face ^ 1],
            device_id=across[face],
            device_id_type=MESH,
        )
        for face in range(4)
    ]

    def padded(value):
        return jnp.pad(value, ((0, ROWS - value.shape[0]), (0, LANES - value.shape[1])))

    def slab(i):
        return padded(fields_ref[:, plane * i : plane * (i + 1)])

    lift = 0.5 * last * last * 0.5

    def traces():
        loads[0].wait()
        own[0] = slab(0).astype(BF)
        loads[1].wait()
        for face in (2, 3):
            at = (face - 2) * (plane - n)
            runs = [fields_ref[:, plane * i + at : plane * i + at + n] for i in range(n)]
            own[face] = padded(jnp.concatenate(runs, axis=1)).astype(BF)
        for i in range(n):
            xs[i], xl[i] = split(slab(i))
        loads[2].wait()
        stack = xs[...].reshape(n * ROWS, LANES)[:, :plane]
        ends = dot(stack, pick_ref[...]).reshape(n, ROWS, 128)
        for face in (4, 5):
            at = (face - 4) * n
            runs = [ends[i, :, at : at + n] for i in range(n)]
            own[face] = padded(jnp.concatenate(runs, axis=1)).astype(BF)

    def parts(value):
        hi = value.astype(BF).astype(F32)
        lane = lax.broadcasted_iota(jnp.int32, value.shape, value.ndim - 1)
        return jnp.where(jnp.bitwise_and(lane, ROWS) == 0, hi, value - hi).astype(BF)

    def flux_matrices():
        for load in loads[3:whole_loads]:
            load.wait()
        raw[...] = jnp.zeros_like(raw)
        for axis in range(3):
            scaled = flux_ref[axis] * (-TIME_STEP * jac_ref[0, axis])
            for k in range(LANES // ROWS):
                raw[axis, 0:width, ROWS * k : ROWS * k + width] = scaled
        mix[...] = parts(raw[...])
        row = lax.broadcasted_iota(jnp.int32, (ROWS, LANES), 0)
        lane = lax.broadcasted_iota(jnp.int32, (ROWS, LANES), 1)
        diagonal = jnp.bitwise_and(lane, ROWS - 1) == row
        for face in range(6):
            side = lift if face % 2 else -lift
            keep = lift * TIME_STEP * jac_ref[0, face // 2]
            lift_lhs[face] = parts(raw[face // 2] * side + jnp.where(diagonal, keep, 0.0))

    def volume_flux():
        for i in range(n):
            both = jnp.concatenate([xs[i], xs[i], xl[i], xl[i]], axis=0)
            mixed = dot(mix[...].reshape(3 * ROWS, LANES), both)
            gx[i] = mixed[:ROWS]
            for axis in range(2):
                part = mixed[ROWS * (axis + 1) : ROWS * (axis + 2)]
                gs[axis, 0, i], gs[axis, 1, i] = split(part)

    def face_facts(face):
        first, second = lane_ref[0:1, :], lane_ref[1:2, :]
        ones = jnp.ones((1, LANES), F32)
        code = code_ref[0, face]
        order = order_ref[0, face].astype(F32)
        swap = jnp.where(code >= 4, 1, 0)
        rev_a = lax.rem(lax.div(code, 2), 2)
        rev_b = lax.rem(code, 2)
        use_first = jnp.where(swap == 1, rev_b, rev_a) == 1
        use_second = jnp.where(swap == 1, rev_a, rev_b) == 1
        sign = jnp.where(use_first, lane_ref[2:3, :], ones) * jnp.where(
            use_second, lane_ref[3:4, :], ones
        )
        keep = jnp.where((first < order) & (second < order), 1.0, 0.0)
        return swap, sign, keep

    def own_faces():
        rest_flat = own[2:].reshape(4 * ROWS, LANES)
        own_flat = jnp.concatenate([xs[0], xs[last], rest_flat], axis=0)[:, :plane]
        own_modes = (dot(own_flat, fwd_ref[0, 0]) + dot(own_flat, fwd_ref[0, 1])).reshape(
            6, ROWS, LANES
        )
        modes = []
        for face in range(6):
            swap, sign, keep = face_facts(face)
            if face < 4:
                modes.append(own_modes[face] * -keep)
            else:
                far = own[face ^ 1][:, :plane]
                turned = dot(far, fwd_ref[swap, 0]) + dot(far, fwd_ref[swap, 1])
                modes.append((turned * sign - own_modes[face]) * keep)
        modes_hi, modes_lo = split(jnp.concatenate(modes, axis=0))
        modes_hi, modes_lo = modes_hi[:, :plane], modes_lo[:, :plane]
        jump = dot(modes_hi, back_ref[0]) + dot(modes_lo, back_ref[0]) + dot(modes_hi, back_ref[1])
        jump_hi, jump_lo = split(jump)
        cut = lambda a, f: a[ROWS * f : ROWS * (f + 1)]
        for face in range(6):
            early[face] = fluxed(lift_lhs[face], cut(jump_hi, face), cut(jump_lo, face))

    def answer(face):
        pl.semaphore_wait(ack.at[face], 1)
        copies[face].start()

    def when(condition, *steps):
        @pl.when(condition)
        def _():
            for step in steps:
                step()

    odd = lax.rem(sub, 2) == 1
    corner = (blk == 0) & (sub < 2)
    even = jnp.logical_not(odd)
    rest = jnp.logical_not(corner)
    y_first = odd | (blk == 0)
    before = odd | (blk != n_blk - 1)
    inner = (blk != 0) & (sub != 0)

    for load in loads[whole_loads:]:
        load.wait()
    offset = plane * last - high
    tail = points - high - LANES
    lane = lax.broadcasted_iota(jnp.int32, (width, 128), 1)
    ahead = jnp.pad(fields_ref[:, high + LANES :], ((0, 0), (0, 128 - tail)))
    merged = jnp.where(lane < tail, ahead, fields_ref[:, high : high + 128])
    turned = jnp.concatenate([merged, fields_ref[:, high + 128 : high + LANES]], axis=1)
    own[1] = padded(turned).astype(BF)
    when(before, traces)
    when(corner, flux_matrices, volume_flux)
    pl.semaphore_wait(barrier, 2)
    when(even | corner, copies[1].start)
    for face in ENTRY:
        pl.semaphore_signal(ack.at[face ^ 1], inc=1, device_id=across[face], device_id_type=MESH)
    when(jnp.logical_not(before), traces)
    copies[3].start()
    when(rest, flux_matrices)
    when(odd & rest, copies[1].start)
    when(rest & y_first, lambda: answer(2))
    when(rest & jnp.logical_not(y_first), lambda: answer(0))
    when(rest, volume_flux)
    when(inner & odd, lambda: answer(0))
    when(inner & even, lambda: answer(2))
    own_faces()
    when((blk != 0) & (sub == 0), lambda: answer(2))

    for face in range(4):
        swap, sign, keep = face_facts(face)
        scale = sign * keep
        f_hi = (fwd_ref[swap, 0].astype(F32) * scale).astype(BF)[:, :plane]
        f_lo = (fwd_ref[swap, 1].astype(F32) * scale).astype(BF)[:, :plane]
        whole = dot(f_hi, back_ref[0]) + dot(f_lo, back_ref[0]) + dot(f_hi, back_ref[1])
        whole = whole + dot(f_lo, back_ref[1])
        if face == 1:
            whole = pltpu.roll(whole, offset, 1)
        zeros = jnp.zeros((LANES - plane, LANES), F32)
        if face == 0:
            head = plane - tail
            whole = jnp.concatenate([whole[head:], zeros, whole[:head]], axis=0)
        else:
            whole = jnp.concatenate([whole, zeros], axis=0)
        oper[face, 0], oper[face, 1] = split(whole)

    when(rest & (blk == 0), lambda: answer(0))

    runs = []
    for i in range(n):
        both = jnp.concatenate([early[f, :, n * i : n * (i + 1)] for f in (4, 5)], axis=1)
        hi = both.astype(BF).astype(F32)
        runs.append(jnp.concatenate([hi, both - hi], axis=1).astype(BF))
    total = dot(jnp.concatenate(runs, axis=0), put_ref[...])
    for axis in range(2):
        hi = gs[axis, 0].reshape(n * ROWS, LANES)[:, :plane]
        lo = gs[axis, 1].reshape(n * ROWS, LANES)[:, :plane]
        total = total + dot(hi, deriv_ref[axis, 0])
        total = total + dot(lo, deriv_ref[axis, 0])
        total = total + dot(hi, deriv_ref[axis, 1])
    vol[...] = total.reshape(n, ROWS, LANES)
    when(corner, lambda: answer(2))

    half = n // 2
    for r in range(0, -(-width // 8) * 8, 8):
        for c in range(0, LANES, 128):
            at = (slice(r, r + 8), slice(c, c + 128))
            plus, minus = [], []
            for a in range(half):
                one, two = gx[(a,) + at], gx[(last - a,) + at]
                plus.append(one + two)
                minus.append(one - two)
            middle = gx[(half,) + at]
            for i in range(half):
                even = minus[0] * float(0.5 * (diff[i, 0] - diff[i, last]))
                uneven = middle * float(diff[i, half])
                for a in range(half):
                    uneven = uneven + plus[a] * float(0.5 * (diff[i, a] + diff[i, last - a]))
                    if a:
                        even = even + minus[a] * float(0.5 * (diff[i, a] - diff[i, last - a]))
                vol[(i,) + at] += even + uneven
                vol[(last - i,) + at] += even - uneven
            even = minus[0] * float(diff[half, 0])
            for a in range(1, half):
                even = even + minus[a] * float(diff[half, a])
            vol[(half,) + at] += even
    for i in range(n):
        value = vol[i]
        if i == 0:
            value = value + early[0]
        if i == last:
            value = value + early[1]
        out_ref[:, plane * i : plane * (i + 1)] = value[:width, :plane]
    when(corner, lambda: answer(0))

    def arrived(*faces):
        for face in faces:
            copies[face ^ 1].wait_recv()
        terms = far_terms(faces, lambda f: remote[f], oper, lift_lhs, plane)
        for face, part in zip(faces, terms):
            if face == 1:
                part = part[:width]
                begun = jnp.where(lane >= offset, part[:, :128], 0.0)
                out_ref[:, high : high + 128] += begun
                out_ref[:, high + 128 : high + LANES] += part[:, 128:]
                out_ref[:, high + LANES :] += part[:, :tail]
                continue
            total = (part + early[face])[:width]
            at = (face - 2) * (plane - n)
            for i in range(n):
                out_ref[:, plane * i + at : plane * i + at + n] += total[:, n * i : n * (i + 1)]

    arrived(2, 3)
    arrived(1)
    copies[1].wait_recv()
    for copy in copies:
        copy.wait_send()


def finish(n, part_ref, far_ref, oper, lift_lhs, out_ref, low_ref, sem):
    width = part_ref.shape[0]
    low = low_ref.shape[1]
    writes = [pltpu.make_async_copy(part_ref.at[:, low:], out_ref.at[:, 0, low:], sem.at[0])]
    writes[0].start()
    (term,) = far_terms((0,), lambda f: far_ref[...], oper, lift_lhs, n * n)
    for i, r in enumerate(range(0, width, STRIP)):
        strip = slice(r, min(r + STRIP, width))
        low_ref[strip] = part_ref[strip, :low] + term[strip, :low]
        writes.append(
            pltpu.make_async_copy(low_ref.at[strip], out_ref.at[strip, 0, :low], sem.at[i + 1])
        )
        writes[-1].start()
    for copy in writes:
        copy.wait()


def solution(mesh):
    sizes = (mesh.shape["blk"], mesh.shape["sub"])

    def on_device(fields, flux_matrix, inv_jacobian, neighbour, orientation, face_order):
        width, points = fields.shape[1:]
        n = round(points ** (1.0 / 3.0))
        plane = n * n
        *constants, diff = tables(n)
        rows = jnp.transpose(fields, (1, 0, 2))
        hbm = pl.BlockSpec(memory_space=pltpu.HBM)
        operands = [orientation, face_order, inv_jacobian, rows, flux_matrix]
        operands += [jnp.asarray(a) for a in constants]
        vmem = lambda a: pltpu.VMEM(a.shape, a.dtype)
        vmem_spec = pl.BlockSpec(memory_space=pltpu.VMEM)

        def scoped(*refs):
            pl.run_scoped(
                functools.partial(body, n, diff, sizes, *refs),
                pltpu.SemaphoreType.DMA((len(operands) + 1 + -(-width // STRIP),)),
                pltpu.SemaphoreType.DMA((4,)),
                pltpu.SemaphoreType.DMA((4,)),
                pltpu.SemaphoreType.REGULAR((4,)),
            )

        parts = pl.pallas_call(
            scoped,
            out_shape=(
                pltpu.VMEM((width, points), F32),
                pltpu.VMEM((ROWS, LANES), BF),
                pltpu.VMEM((4, 2, LANES, LANES), BF),
                pltpu.VMEM((6, ROWS, LANES), BF),
            ),
            in_specs=[hbm] * len(operands),
            out_specs=[vmem_spec] * 4,
            scratch_shapes=[pltpu.SMEM(a.shape, a.dtype) for a in operands[:3]]
            + [pltpu.VMEM((width, points), F32)]
            + [vmem(a) for a in operands[4:]]
            + [
                pltpu.VMEM((n, ROWS, LANES), BF),
                pltpu.VMEM((n, ROWS, LANES), BF),
                pltpu.VMEM((n, ROWS, LANES), F32),
                pltpu.VMEM((2, 2, n, ROWS, LANES), BF),
                pltpu.VMEM((n, ROWS, LANES), F32),
                pltpu.VMEM((6, ROWS, LANES), BF),
                pltpu.VMEM((4, ROWS, LANES), BF),
                pltpu.VMEM((3, ROWS, LANES), F32),
                pltpu.VMEM((3, ROWS, LANES), BF),
                pltpu.VMEM((6, ROWS, LANES), F32),
            ],
            compiler_params=pltpu.CompilerParams(
                collective_id=0, has_side_effects=True, vmem_limit_bytes=48 * 1024 * 1024
            ),
        )(*[pltpu.with_memory_space_constraint(a, pltpu.HBM) for a in operands])
        low = -(-plane // 128) * 128
        out = pl.pallas_call(
            lambda *refs: pl.run_scoped(
                functools.partial(finish, n, *refs),
                pltpu.SemaphoreType.DMA((1 + -(-width // STRIP),)),
            ),
            out_shape=jax.ShapeDtypeStruct(rows.shape, F32),
            in_specs=[vmem_spec] * 4,
            out_specs=hbm,
            scratch_shapes=[
                pltpu.VMEM((width, low), F32),
            ],
            compiler_params=pltpu.CompilerParams(vmem_limit_bytes=16 * 1024 * 1024),
        )(*parts)
        return jnp.transpose(out, (1, 0, 2))

    return jax.shard_map(
        on_device,
        mesh=mesh,
        in_specs=(
            P(("blk", "sub"), None, None),
            P(),
            P(("blk", "sub"), None),
            P(("blk", "sub"), None),
            P(("blk", "sub"), None),
            P(("blk", "sub"), None),
        ),
        out_specs=P(("blk", "sub"), None, None),
        check_vma=False,
    )
```
